32 devices in a mesh: aux: 8 (over y, x, core), pair: 4 (over z).
Axes of the slice: x: 2, y: 2, z: 4, core: 2. Of those that a mesh axis runs over, the one named last changes fastest.
Arguments:
- integrals: bfloat16 [3072, 32768], P('aux', 'pair'), may hold values from -0.15625 to 0.15625
- densities: bfloat16 [16, 32768], P(None, 'pair'), may hold values from -2.390625 to 2.390625
- screen: int32 [24, 256], P('aux', 'pair'), may hold values 0 or 1
- factor: float32 [3072, 3072], P('aux', 'pair'), may hold values from -0.109375 to 0.109375
- diag_inv: float32 [3072, 768], P('aux'), may hold values from -2 to 2, as said below
Outputs:
- coulomb: float32 [16, 32768], P(None, ('pair', 'aux'))
The draws below stay inside these ranges and needn't reach their ends.
Inputs may be any that keep to these rules, and one draw needn't show every extreme that they name: `diag_inv`: each block of 768 rows is an upper triangular matrix with a positive diagonal.
All inputs are finite; a program needn't handle non-finite values. No bound on the sum of `screen` on one device may be relied on, other than what follows from the above.
Results may differ from the reference program's by a relative error of at most 0.0041.
Values may be sent and summed in bfloat16 or wider, within the bound.
No kernel may reach another device: no remote copies, remote signals or barrier semaphores. Data moves between devices by JAX's collectives and lax.ppermute only.
A program may use at most 128 MiB of HBM per device.

```python
import math
import jax
import jax.numpy as jnp
from jax import lax

AUX_DEV = 384
DENS = 16
TILE = 128
SOLVE_BLOCKS = 4
NAUX = 3072
BLOCK = 768
NPAIR = 32768


def draw_diag_inv(key, part):
    off_key = jax.random.fold_in(key, 11)
    diag_key = jax.random.fold_in(key, 12)
    spread = 0.5 / math.sqrt(BLOCK)
    offdiag = jnp.clip(jax.random.normal(off_key, (NAUX, BLOCK), jnp.float32), -4.0, 4.0) * spread
    diagonal = jnp.exp(jax.random.uniform(diag_key, (NAUX, 1), jnp.float32, math.log(0.7), math.log(1.4)))
    within = (jnp.arange(NAUX, dtype=jnp.int32) % BLOCK)[:, None]
    across = jnp.arange(BLOCK, dtype=jnp.int32)[None, :]
    return jnp.where(across == within, diagonal, jnp.where(across > within, offdiag, 0.0)).astype(jnp.float32)


def set_ends(result, own_key, low, largest):
    extent = result.shape
    index_at = [jax.random.randint(jax.random.fold_in(own_key, axis), (), 0, extent[axis]) for axis in range(len(extent))]
    result = result.at[tuple(index_at)].set(low)
    longest = extent.index(max(extent))
    index_at[longest] = (index_at[longest] + 1) % extent[longest]
    return result.at[tuple(index_at)].set(largest)


def spiked(result, rng, source, target, parts, factor):
    owner, partner = [(jnp.arange(result.shape[axis_at]) // (result.shape[axis_at] // parts)).reshape([-1 if axis == axis_at else 1 for axis in range(result.ndim)]) for axis_at in (source, target)]
    chosen = jax.random.permutation(rng, parts)[partner]
    strong = (owner == chosen) | (owner == (partner + parts // 2) % parts)
    return jnp.where(strong, factor * result, result)


def shard_levels(rng, dims, shards, smallest, high):
    gain = 1.0
    for dim, shards_of in shards:
        heights = jax.random.uniform(jax.random.fold_in(jax.random.fold_in(rng, 6), dim), (shards_of,), jnp.float32, smallest / len(shards), high / len(shards))
        gain = gain * jnp.repeat(jnp.exp(heights), dims[dim] // shards_of).reshape((-1,) + (1,) * (len(dims) - 1 - dim))
    return gain


def noise(rng, extent, width, bound, split=(), held_as=jnp.bfloat16):
    level = shard_levels(rng, extent, split, -0.22, 0.18) if split else 1.0
    array = jax.random.normal(rng, extent, jnp.float32) * width * level
    return jnp.minimum(jnp.maximum(array, -bound), bound).astype(held_as)


def heavy_noise(own_key, dims, width, reach, shards, heavy, kind=jnp.bfloat16):
    entries = width * jax.random.normal(own_key, dims, jnp.float32)
    if shards:
        entries = entries * shard_levels(own_key, dims, shards, -0.22, 0.18)
    return jnp.clip(spiked(entries, jax.random.fold_in(own_key, 3), *heavy), -reach, reach).astype(kind)


def setup_inputs(seed: int = 0) -> dict:
    key_list = jax.random.split(jax.random.key(seed), 6)
    integrals = heavy_noise(key_list[0], (NAUX, NPAIR), NAUX ** -0.5, 0.15625, ((0, 8), (1, 4)), (0, 1, 8, 2.0))
    densities = noise(key_list[1], (DENS, NPAIR), 0.4, 2.390625, ((1, 4),))
    screen = set_ends((jax.random.randint(key_list[2], (NAUX // TILE, NPAIR // TILE), 0, 4) < 3).astype(jnp.int32), jax.random.fold_in(key_list[2], 1), 0, 1)
    factor = noise(key_list[3], (NAUX, NAUX), NAUX ** -0.5, 0.109375, ((0, 8), (1, 4)), jnp.float32)
    diag_inv = draw_diag_inv(jax.random.fold_in(key_list[5], 71), 0)
    return dict(integrals=integrals, densities=densities, screen=screen, factor=factor, diag_inv=diag_inv)


def reference(integrals, densities, screen, factor, diag_inv):
    blocks = NAUX // AUX_DEV
    highest = lax.Precision.HIGHEST
    tiles_block = AUX_DEV // TILE

    def masked_rows(index):
        slab_rows = lax.dynamic_slice_in_dim(integrals, index * AUX_DEV, AUX_DEV, 0)
        screen_tiles = lax.dynamic_slice_in_dim(screen, index * tiles_block, tiles_block, 0)
        expanded = jnp.repeat(jnp.repeat(screen_tiles, TILE, axis=0), TILE, axis=1).astype(jnp.bfloat16)
        return slab_rows * expanded

    def fit_block(index):
        return lax.dot_general(densities, masked_rows(index), (((1,), (1,)), ((), ())), preferred_element_type=jnp.float32)

    fitted_blocks = lax.map(fit_block, jnp.arange(blocks, dtype=jnp.int32))
    fitted = jnp.transpose(fitted_blocks, (1, 0, 2)).reshape(DENS, NAUX)

    solved = jnp.zeros((DENS, NAUX), jnp.float32)
    for k in range(SOLVE_BLOCKS):
        offset = k * BLOCK
        upper = offset + BLOCK
        residual = fitted[:, offset:upper]
        if k > 0:
            residual = residual - jnp.dot(solved[:, :offset], factor[offset:upper, :offset].T, precision=highest, preferred_element_type=jnp.float32)
        solved = solved.at[:, offset:upper].set(jnp.dot(residual, diag_inv[offset:upper], precision=highest, preferred_element_type=jnp.float32))

    coefficients = jnp.zeros((DENS, NAUX), jnp.float32)
    for k in reversed(range(SOLVE_BLOCKS)):
        offset = k * BLOCK
        upper = offset + BLOCK
        residual = solved[:, offset:upper]
        if upper < NAUX:
            residual = residual - jnp.dot(coefficients[:, upper:], factor[upper:, offset:upper], precision=highest, preferred_element_type=jnp.float32)
        coefficients = coefficients.at[:, offset:upper].set(jnp.dot(residual, diag_inv[offset:upper].T, precision=highest, preferred_element_type=jnp.float32))

    rounded = coefficients.astype(jnp.bfloat16)

    def add_block(running, index):
        weights = lax.dynamic_slice_in_dim(rounded, index * AUX_DEV, AUX_DEV, 1)
        return running + jnp.dot(weights, masked_rows(index), preferred_element_type=jnp.float32), None

    coulomb, unused = lax.scan(add_block, jnp.zeros((DENS, NPAIR), jnp.float32), jnp.arange(blocks, dtype=jnp.int32))
    return coulomb
```

```python
import jax
import jax.numpy as jnp
from jax import lax
from jax.sharding import PartitionSpec as P

TILE = 128
SOLVE_BLOCKS = 4
AXES = ("aux", "pair")
HIGHEST = lax.Precision.HIGHEST


def mm(a, b):
    return jnp.dot(a, b, precision=HIGHEST, preferred_element_type=jnp.float32)


def mm_t(a, b):
    return lax.dot_general(
        a, b, (((1,), (1,)), ((), ())), precision=HIGHEST, preferred_element_type=jnp.float32
    )


def masked_integrals(integrals, screen):
    expanded = jnp.repeat(jnp.repeat(screen, TILE, axis=0), TILE, axis=1).astype(jnp.bfloat16)
    return integrals * expanded


def fit_partial(densities, masked):
    return lax.dot_general(
        densities, masked, (((1,), (1,)), ((), ())), preferred_element_type=jnp.float32
    )


def scatter_sum(summand):
    members = lax.axis_size("aux")
    count, width = summand.shape
    pieces = summand.astype(jnp.bfloat16).reshape(count, members, width // members)
    arrived = lax.all_to_all(pieces.transpose(1, 0, 2), "aux", 0, 0, tiled=True)
    return jnp.sum(arrived.astype(jnp.float32), axis=0)


def chip_solve(partial_fit, factor, diag_inv):
    count, height = partial_fit.shape
    half = count // 2
    planes = lax.axis_size("pair")
    row = lax.axis_index("aux")
    z = lax.axis_index("pair")
    block = row // 2
    side = row % 2

    def send(value, moves):
        pairs = []
        for (k_from, z_from), (k_to, z_to) in moves:
            for c in range(2):
                pairs.append(
                    ((2 * k_from + c) * planes + z_from, (2 * k_to + c) * planes + z_to)
                )
        return lax.ppermute(value, AXES, pairs)

    def swap(value):
        return lax.ppermute(value, "aux", [(i, i ^ 1) for i in range(2 * SOLVE_BLOCKS)])

    def join(own, other, axis):
        low = jnp.where(side == 0, own, other)
        high = jnp.where(side == 0, other, own)
        return jnp.concatenate([low, high], axis)

    factor = join(factor, swap(factor), 0)
    inverse = join(diag_inv, swap(diag_inv), 0)
    kept = lax.dynamic_slice_in_dim(partial_fit, side * half, half, 0)
    given = lax.dynamic_slice_in_dim(partial_fit, (1 - side) * half, half, 0)
    fit = join(kept, swap(given), 1)

    home = [max(k - 1, 0) for k in range(SOLVE_BLOCKS)]
    parts = fit
    for step in range(1, planes):
        fit = fit + send(
            parts, [((k, (home[k] + step) % planes), (k, home[k])) for k in range(SOLVE_BLOCKS)]
        )
    s_zero = mm(fit, inverse)
    at = lambda k, plane: (block == k) & (z == plane)
    got = send(s_zero, [((0, 0), (1, 0))])
    got = got + send(s_zero, [((0, 0), (2, 0))])
    got = got + send(s_zero, [((0, 0), (3, 0))])
    zero_copy = jnp.where(at(0, 0), s_zero, 0.0)
    for plane in range(1, planes):
        zero_copy = zero_copy + send(s_zero, [((0, 0), (0, plane))])
    term = mm_t(got, factor)
    s_one = mm(fit - term, inverse)
    out = jnp.where(block == 1, s_one, term)
    first = send(out, [((1, 0), (2, 1)), ((3, 0), (3, 1))])
    second = send(out, [((1, 0), (3, 1)), ((2, 0), (2, 1))])
    known = jnp.where(block == 3, second, first)
    behind = jnp.where(block == 3, first, second)
    term = behind + mm_t(known, factor)
    s_two = mm(fit - term, inverse)
    known = send(s_two, [((2, 1), (3, 2))])
    behind = send(term, [((3, 1), (3, 2))])
    s_three = mm(fit - behind - mm_t(known, factor), inverse)
    c_three = mm_t(s_three, inverse)
    back = mm(c_three, factor)
    into_two = send(back, [((3, 2), (2, 1))])
    three = send(c_three, [((3, 2), (3, 1))])
    three = three + send(c_three, [((3, 2), (3, 0))])
    c_two = mm_t(s_two - into_two, inverse)
    back = mm(jnp.where(block == 3, three, c_two), factor)
    into_one = send(back, [((2, 1), (1, 0)), ((3, 0), (2, 0))])
    other = send(jnp.where(block == 3, back, c_two), [((3, 1), (1, 0)), ((2, 1), (2, 0))])
    c_one = mm_t(s_one - into_one - other, inverse)
    back = mm(jnp.where(block == 2, other, c_one), factor) + jnp.where(block == 2, into_one, 0.0)
    into_zero = jnp.zeros_like(back)
    for plane in range(planes):
        into_zero = into_zero + send(
            back, [((1, 0), (0, plane)), ((2, 0), (0, (plane + 1) % planes))]
        )
    c_zero = mm_t(zero_copy - into_zero, inverse)
    have_two = at(2, 1)
    coef = jnp.where(at(1, 0), c_one, jnp.where(have_two, c_two, jnp.where(at(3, 2), c_three, 0.0)))
    spread = coef
    for step in range(1, planes):
        moves = [((1, 0), (1, step))]
        if 1 + step < planes:
            moves.append(((2, 1), (2, 1 + step)))
        if 2 + step < planes:
            moves.append(((3, 2), (3, 2 + step)))
        spread = spread + send(coef, moves)
    spread = spread + jnp.where(at(3, 0) | at(3, 1), three, 0.0) + jnp.where(at(2, 0), other, 0.0)
    final = jnp.where(block == 0, c_zero, spread).astype(jnp.bfloat16)
    own = lax.dynamic_slice_in_dim(final, side * height, height, 1)
    mate = lax.dynamic_slice_in_dim(final, (1 - side) * height, height, 1)
    return join(own, swap(mate), 0)


def chain_solve(partial_fit, factor, diag_inv):
    count, height = partial_fit.shape
    breadth = factor.shape[1]
    block_size = diag_inv.shape[1]
    rows_aux = lax.axis_size("aux")
    total = height * rows_aux
    members = rows_aux // SOLVE_BLOCKS
    my_row = lax.axis_index("aux")
    my_column = lax.axis_index("pair")
    my_block = my_row // members
    column_block = (my_column * breadth + jnp.arange(breadth, dtype=jnp.int32)) // block_size
    factor_low = jnp.where((column_block < my_block)[None, :], factor, 0.0)

    def own_columns(whole):
        return lax.dynamic_slice_in_dim(whole, my_column * breadth, breadth, 1)

    zero_block = jnp.zeros((count, block_size), jnp.float32)
    solved = jnp.zeros((count, total), jnp.float32)
    for k in range(SOLVE_BLOCKS):

        def on_group(current):
            return mm(partial_fit - mm_t(own_columns(current), factor_low), diag_inv)

        def off_group(current):
            return zero_block

        summand = lax.cond(my_block == k, on_group, off_group, solved)
        arrived = lax.psum(summand, AXES)
        solved = lax.dynamic_update_slice_in_dim(solved, arrived, k * block_size, 1)
    own_coef = jnp.zeros((count, height), jnp.float32)
    contrib = jnp.zeros((count, total), jnp.float32)
    for target in reversed(range(SOLVE_BLOCKS)):
        settled = solved[:, target * block_size : (target + 1) * block_size]
        if target < SOLVE_BLOCKS - 1:
            portion = contrib[:, target * block_size : (target + 1) * block_size]
            settled = settled - lax.psum(portion, AXES)

        def on_group(state):
            coef = mm_t(settled, diag_inv)
            if target > 0:
                fresh = lax.dynamic_update_slice_in_dim(
                    jnp.zeros((count, total), jnp.float32),
                    mm(coef, factor_low),
                    my_column * breadth,
                    1,
                )
            else:
                fresh = state[1]
            return (coef, fresh)

        def keep_state(state):
            return state

        own_coef, contrib = lax.cond(my_block == target, on_group, keep_state, (own_coef, contrib))
    return own_coef.astype(jnp.bfloat16)


def shards(integrals, densities, screen, factor, diag_inv):
    block_size = diag_inv.shape[1]
    chip_blocks = (
        lax.axis_size("aux") == 2 * SOLVE_BLOCKS
        and factor.shape[1] == block_size
        and lax.axis_size("pair") == SOLVE_BLOCKS
    )
    solve = chip_solve if chip_blocks else chain_solve
    masked = masked_integrals(integrals, screen)
    rounded = solve(fit_partial(densities, masked), factor, diag_inv)
    summand = jnp.dot(rounded, masked, preferred_element_type=jnp.float32)
    return scatter_sum(summand)


def solution(mesh):
    in_specs = (
        P("aux", "pair"),
        P(None, "pair"),
        P("aux", "pair"),
        P("aux", "pair"),
        P("aux", None),
    )
    out_specs = P(None, ("pair", "aux"))
    return jax.shard_map(shards, mesh=mesh, in_specs=in_specs, out_specs=out_specs, check_vma=False)
```

```python
import functools

import jax
import jax.numpy as jnp
from jax import lax
from jax.experimental import pallas as pl
from jax.experimental.pallas import tpu as pltpu
from jax.sharding import PartitionSpec as P

TILE = 128
SOLVE_BLOCKS = 4
AXES = ("aux", "pair")
HIGHEST = lax.Precision.HIGHEST
F32 = jnp.float32
BF16 = jnp.bfloat16
VMEM = pl.BlockSpec(memory_space=pltpu.VMEM)
SMEM = pl.BlockSpec(memory_space=pltpu.SMEM)
MIB = 1024 * 1024
NN = (((1,), (0,)), ((), ()))
NT = (((1,), (1,)), ((), ()))
TN = (((0,), (0,)), ((), ()))


def chunk_of(width):
    return 1024 if width % 1024 == 0 else width


def fit_kernel(screen, densities, integrals, out):
    step = pl.program_id(0)
    strips = integrals.shape[0] // TILE
    tiles = integrals.shape[1] // TILE

    @pl.when(step == 0)
    def _():
        out[...] = jnp.zeros_like(out)

    for i in range(strips):
        masked = jnp.concatenate(
            [
                jnp.where(
                    screen[i, step * tiles + j] != 0,
                    densities[:, j * TILE : (j + 1) * TILE],
                    jnp.zeros((), BF16),
                )
                for j in range(tiles)
            ],
            axis=1,
        )
        out[:, i * TILE : (i + 1) * TILE] += lax.dot_general(
            masked, integrals[i * TILE : (i + 1) * TILE, :], NT, preferred_element_type=F32
        )


def fit_partial(densities, integrals, screen):
    count = densities.shape[0]
    height, width = integrals.shape
    chunk = chunk_of(width)
    return pl.pallas_call(
        fit_kernel,
        grid=(width // chunk,),
        in_specs=[
            SMEM,
            pl.BlockSpec((count, chunk), lambda j: (0, j)),
            pl.BlockSpec((height, chunk), lambda j: (0, j)),
        ],
        out_specs=pl.BlockSpec((count, height), lambda j: (0, 0)),
        out_shape=jax.ShapeDtypeStruct((count, height), F32),
        compiler_params=pltpu.CompilerParams(vmem_limit_bytes=12 * MIB),
        name="fit",
    )(screen, densities, integrals)


def coulomb_kernel(screen, rounded, integrals, out):
    step = pl.program_id(0)
    strips = integrals.shape[0] // TILE
    tiles = integrals.shape[1] // TILE
    for j in range(tiles):
        masked = jnp.concatenate(
            [
                jnp.where(
                    screen[i, step * tiles + j] != 0,
                    rounded[:, i * TILE : (i + 1) * TILE],
                    jnp.zeros((), BF16),
                )
                for i in range(strips)
            ],
            axis=1,
        )
        part = jnp.dot(
            masked, integrals[:, j * TILE : (j + 1) * TILE], preferred_element_type=F32
        )
        out[:, j * TILE : (j + 1) * TILE] = part.astype(out.dtype)


def coulomb_partial(rounded, integrals, screen):
    count, height = rounded.shape
    width = integrals.shape[1]
    members = lax.axis_size("aux")
    chunk = width // members
    return pl.pallas_call(
        coulomb_kernel,
        grid=(members,),
        in_specs=[
            SMEM,
            pl.BlockSpec((count, height), lambda j: (0, 0)),
            pl.BlockSpec((height, chunk), lambda j: (0, j)),
        ],
        out_specs=pl.BlockSpec((None, count, chunk), lambda j: (j, 0, 0)),
        out_shape=jax.ShapeDtypeStruct((members, count, chunk), BF16),
        compiler_params=pltpu.CompilerParams(vmem_limit_bytes=12 * MIB),
        name="coulomb",
    )(screen, rounded, integrals)


def scatter_sum(slabs):
    arrived = lax.all_to_all(slabs, "aux", 0, 0, tiled=True)
    return jnp.sum(arrived.astype(F32), axis=0)


def high_low(value):
    high = value.astype(BF16)
    return high, (value - high.astype(F32)).astype(BF16)


def times(value, high, low, dims):
    rows = value.shape[0]
    coarse = value.astype(BF16).astype(F32)
    pair = jnp.concatenate([coarse, value - coarse], axis=0).astype(BF16)
    both = lax.dot_general(pair, high, dims, preferred_element_type=F32)
    both += lax.dot_general(pair, low, dims, preferred_element_type=F32)
    return both[:rows] + both[rows:]


def my_block():
    return lax.axis_index("aux") // 2


def call(kernel, outs, *operands, limit=12):
    return pl.pallas_call(
        kernel,
        out_shape=outs,
        in_specs=[VMEM] * len(operands),
        out_specs=jax.tree.map(lambda _: VMEM, outs),
        compiler_params=pltpu.CompilerParams(vmem_limit_bytes=limit * MIB),
        name=kernel.__name__,
    )(*operands)


def prepare(own_inv, mate_inv, own_fac, mate_fac, inv_high, inv_low, k_high, k_low):
    side = lax.axis_index("aux") % 2
    height = own_inv.shape[0]
    here = pl.ds(pl.multiple_of(side * height, height), height)
    there = pl.ds(pl.multiple_of((1 - side) * height, height), height)
    for ref, rows in ((own_inv, here), (mate_inv, there)):
        high, low = high_low(ref[...])
        inv_high[rows, :] = high
        inv_low[rows, :] = low

    @pl.when(my_block() > 0)
    def _():
        total = jnp.zeros(k_high.shape, F32)
        for inv, fac in ((own_inv, own_fac), (mate_inv, mate_fac)):
            ih, il = high_low(inv[...])
            fh, fl = high_low(fac[...])
            total += lax.dot_general(ih, fh, TN, preferred_element_type=F32)
            total += lax.dot_general(ih, fl, TN, preferred_element_type=F32)
            total += lax.dot_general(il, fh, TN, preferred_element_type=F32)
        high, low = high_low(total)
        k_high[...] = high
        k_low[...] = low


def start_solve(f0, f1, f2, f3, high, low, out):
    out[...] = times(f0[...] + f1[...] + f2[...] + f3[...], high[...], low[...], NN)


def after_zero(known, e, high, low, out):
    term = times(known[...], high[...], low[...], NT)
    out[...] = jnp.where(my_block() == 1, e[...] - term, term)


def after_one(first, second, e, high, low, out):
    last = my_block() == 3
    known = jnp.where(last, second[...], first[...])
    behind = jnp.where(last, first[...], second[...])
    total = behind + times(known, high[...], low[...], NT)
    out[...] = jnp.where(last, total, e[...] - total)


def turn(known, behind, e, high, low, settled, back):
    value = e[...] - behind[...] - times(known[...], high[...], low[...], NT)
    settled[...] = value
    back[...] = times(value, high[...], low[...], NN)


def back_two(into, near, far, s, high, low, settled, back):
    value = jnp.where(my_block() == 3, near[...] + far[...], s[...] - into[...])
    settled[...] = value
    back[...] = times(value, high[...], low[...], NN)


def back_one(into, other, s, high, low, settled, back):
    two = my_block() == 2
    value = jnp.where(two, other[...], s[...] - into[...] - other[...])
    settled[...] = value
    back[...] = times(value, high[...], low[...], NN) + jnp.where(two, into[...], 0.0)


def finish(own, mate, high, low, out):
    side = lax.axis_index("aux") % 2
    height = out.shape[1]
    here = pl.ds(pl.multiple_of(side * height, height), height)
    even = side == 0
    value = jnp.concatenate(
        [jnp.where(even, own[...], mate[...]), jnp.where(even, mate[...], own[...])], axis=0
    )
    out[...] = times(value, high[here, :], low[here, :], NT).astype(out.dtype)


def mm(a, b):
    return jnp.dot(a, b, precision=HIGHEST, preferred_element_type=F32)


def mm_t(a, b):
    return lax.dot_general(a, b, NT, precision=HIGHEST, preferred_element_type=F32)


def chip_solve(partial_fit, factor, diag_inv):
    count, height = partial_fit.shape
    half = count // 2
    size = 2 * height
    planes = lax.axis_size("pair")
    row = lax.axis_index("aux")
    z = lax.axis_index("pair")
    block = row // 2
    side = row % 2

    def send(value, moves, fill=()):
        pairs = []
        for (k_from, z_from), (k_to, z_to) in tuple(moves) + tuple(fill):
            for c in range(2):
                pairs.append(
                    ((2 * k_from + c) * planes + z_from, (2 * k_to + c) * planes + z_to)
                )
        return lax.ppermute(value, AXES, pairs)

    def swap(value):
        return lax.ppermute(value, "aux", [(i, i ^ 1) for i in range(2 * SOLVE_BLOCKS)])

    panel = jax.ShapeDtypeStruct((half, size), F32)
    square = jax.ShapeDtypeStruct((size, size), BF16)
    inv_high, inv_low, k_high, k_low = call(
        prepare, [square] * 4, diag_inv, swap(diag_inv), factor, swap(factor), limit=32
    )
    kept = lax.dynamic_slice_in_dim(partial_fit, side * half, half, 0)
    given = lax.dynamic_slice_in_dim(partial_fit, (1 - side) * half, half, 0)
    mate = swap(given)
    fit = jnp.concatenate(
        [jnp.where(side == 0, kept, mate), jnp.where(side == 0, mate, kept)], axis=1
    )
    everyone = [(k, plane) for k in range(SOLVE_BLOCKS) for plane in range(planes)]
    shifted = [
        send(fit, [((k, plane), (k, (plane + step) % planes)) for k, plane in everyone])
        for step in range(1, planes)
    ]
    e = call(start_solve, panel, fit, *shifted, inv_high, inv_low)

    def at(k, plane):
        return (block == k) & (z == plane)

    got = send(
        e,
        [((0, 0), (1, 0)), ((0, 1), (2, 0)), ((0, 2), (3, 0))],
        [((1, 3), (0, 0)), ((2, 3), (0, 1)), ((3, 3), (0, 2))],
    )
    one = call(after_zero, panel, got, e, k_high, k_low)
    first = send(one, [((1, 0), (2, 1)), ((3, 0), (3, 1))], [((1, 3), (1, 0))])
    second = send(one, [((1, 0), (3, 1)), ((2, 0), (2, 1))], [((1, 3), (1, 0))])
    two = call(after_one, panel, first, second, e, k_high, k_low)
    known = send(two, [((2, 1), (3, 2))], [((2, 3), (2, 1))])
    behind = send(two, [((3, 1), (3, 2))], [((3, 3), (3, 1))])
    t_three, back = call(turn, [panel] * 2, known, behind, e, k_high, k_low)
    into_two = send(back, [((3, 2), (2, 1))], [((3, 3), (3, 2))])
    near = send(t_three, [((3, 2), (3, 1))], [((3, 3), (3, 2))])
    far = send(t_three, [((3, 2), (3, 0))], [((3, 3), (3, 2))])
    near = jnp.where(at(3, 1), near, 0.0)
    far = jnp.where(at(3, 0), far, 0.0)
    t_two, back = call(back_two, [panel] * 2, into_two, near, far, two, k_high, k_low)
    into_one = send(back, [((2, 1), (1, 0)), ((3, 0), (2, 0))], [((2, 3), (2, 1))])
    other = send(
        jnp.where(block == 3, back, t_two),
        [((3, 1), (1, 0)), ((2, 1), (2, 0))],
        [((2, 3), (2, 1))],
    )
    t_one, back = call(back_one, [panel] * 2, into_one, other, one, k_high, k_low)
    into_zero = [
        send(
            back,
            [((1, 0), (0, plane)), ((2, 0), (0, (plane + 1) % planes))],
            [((1, 3), (1, 0))],
        )
        for plane in range(planes)
    ]
    t_zero = e - sum(into_zero)
    t = jnp.where(at(1, 0), t_one, jnp.where(at(2, 1), t_two, jnp.where(at(3, 2), t_three, 0.0)))
    spread = t
    for step in range(1, planes):
        moves = [((1, 0), (1, step))]
        if 1 + step < planes:
            moves.append(((2, 1), (2, 1 + step)))
        if 2 + step < planes:
            moves.append(((3, 2), (3, 2 + step)))
        spread = spread + send(t, moves)
    spread = spread + near + far + jnp.where(at(2, 0), other, 0.0)
    t = jnp.where(block == 0, t_zero, spread)
    return call(
        finish, jax.ShapeDtypeStruct((count, height), BF16), t, swap(t), inv_high, inv_low
    )


def chain_solve(partial_fit, factor, diag_inv):
    count, height = partial_fit.shape
    breadth = factor.shape[1]
    block_size = diag_inv.shape[1]
    rows_aux = lax.axis_size("aux")
    total = height * rows_aux
    members = rows_aux // SOLVE_BLOCKS
    my_row = lax.axis_index("aux")
    my_column = lax.axis_index("pair")
    my_block = my_row // members
    column_block = (my_column * breadth + jnp.arange(breadth, dtype=jnp.int32)) // block_size
    factor_low = jnp.where((column_block < my_block)[None, :], factor, 0.0)

    def own_columns(whole):
        return lax.dynamic_slice_in_dim(whole, my_column * breadth, breadth, 1)

    zero_block = jnp.zeros((count, block_size), jnp.float32)
    solved = jnp.zeros((count, total), jnp.float32)
    for k in range(SOLVE_BLOCKS):

        def on_group(current):
            return mm(partial_fit - mm_t(own_columns(current), factor_low), diag_inv)

        def off_group(current):
            return zero_block

        summand = lax.cond(my_block == k, on_group, off_group, solved)
        arrived = lax.psum(summand, AXES)
        solved = lax.dynamic_update_slice_in_dim(solved, arrived, k * block_size, 1)
    own_coef = jnp.zeros((count, height), jnp.float32)
    contrib = jnp.zeros((count, total), jnp.float32)
    for target in reversed(range(SOLVE_BLOCKS)):
        settled = solved[:, target * block_size : (target + 1) * block_size]
        if target < SOLVE_BLOCKS - 1:
            portion = contrib[:, target * block_size : (target + 1) * block_size]
            settled = settled - lax.psum(portion, AXES)

        def on_group(state):
            coef = mm_t(settled, diag_inv)
            if target > 0:
                fresh = lax.dynamic_update_slice_in_dim(
                    jnp.zeros((count, total), jnp.float32),
                    mm(coef, factor_low),
                    my_column * breadth,
                    1,
                )
            else:
                fresh = state[1]
            return (coef, fresh)

        def keep_state(state):
            return state

        own_coef, contrib = lax.cond(my_block == target, on_group, keep_state, (own_coef, contrib))
    return own_coef.astype(jnp.bfloat16)


def shards(integrals, densities, screen, factor, diag_inv):
    block_size = diag_inv.shape[1]
    chip_blocks = (
        lax.axis_size("aux") == 2 * SOLVE_BLOCKS
        and factor.shape[1] == block_size
        and lax.axis_size("pair") == SOLVE_BLOCKS
    )
    solve = chip_solve if chip_blocks else chain_solve
    rounded = solve(fit_partial(densities, integrals, screen), factor, diag_inv)
    return scatter_sum(coulomb_partial(rounded, integrals, screen))


def solution(mesh):
    in_specs = (
        P("aux", "pair"),
        P(None, "pair"),
        P("aux", "pair"),
        P("aux", "pair"),
        P("aux", None),
    )
    out_specs = P(None, ("pair", "aux"))
    return jax.shard_map(shards, mesh=mesh, in_specs=in_specs, out_specs=out_specs, check_vma=False)
```

```python
import jax
import jax.numpy as jnp
from jax import lax
from jax.experimental import pallas as pl
from jax.experimental.pallas import tpu as pltpu
from jax.sharding import PartitionSpec as P

TILE = 128
SOLVE_BLOCKS = 4
AXES = ("aux", "pair")
HIGHEST = lax.Precision.HIGHEST
F32 = jnp.float32
BF16 = jnp.bfloat16
VMEM = pl.BlockSpec(memory_space=pltpu.VMEM)
SMEM = pl.BlockSpec(memory_space=pltpu.SMEM)
HBM = pl.BlockSpec(memory_space=pltpu.HBM)
MIB = 1024 * 1024
NN = (((1,), (0,)), ((), ()))
NT = (((1,), (1,)), ((), ()))
TN = (((0,), (0,)), ((), ()))


def struct(shape, dtype=F32):
    return jax.ShapeDtypeStruct(shape, dtype)


def call(kernel, outs, *operands, limit=12, specs=None, scratch=()):
    return pl.pallas_call(
        kernel,
        out_shape=outs,
        in_specs=specs or [VMEM] * len(operands),
        out_specs=jax.tree.map(lambda _: VMEM, outs),
        scratch_shapes=scratch,
        compiler_params=pltpu.CompilerParams(vmem_limit_bytes=limit * MIB),
        name=kernel.__name__,
    )(*operands)


def side_of():
    return lax.rem(lax.axis_index("aux"), 2)


def block_of():
    return lax.div(lax.axis_index("aux"), 2)


def fit(screen_in, densities_in, integrals, held, kept, given, screen, densities, total, arrived):
    height, width = integrals.shape
    pieces = arrived.shape[0] - 2
    chunk = width // pieces
    half = kept.shape[0]
    small = [
        pltpu.make_async_copy(screen_in, screen, arrived.at[pieces]),
        pltpu.make_async_copy(densities_in, densities, arrived.at[pieces + 1]),
    ]
    copies = [
        pltpu.make_async_copy(
            integrals.at[:, j * chunk : (j + 1) * chunk],
            held.at[:, j * chunk : (j + 1) * chunk],
            arrived.at[j],
        )
        for j in range(pieces)
    ]
    for copy in small + copies:
        copy.start()
    total[...] = jnp.zeros_like(total)
    for copy in small:
        copy.wait()
    for j in range(pieces):
        copies[j].wait()
        columns = slice(j * chunk, (j + 1) * chunk)
        for i in range(height // TILE):
            rows = slice(i * TILE, (i + 1) * TILE)
            masked = jnp.concatenate(
                [
                    jnp.where(
                        screen[i, t] != 0,
                        densities[:, t * TILE : (t + 1) * TILE],
                        jnp.zeros((), BF16),
                    )
                    for t in range(j * chunk // TILE, (j + 1) * chunk // TILE)
                ],
                axis=1,
            )
            total[rows, :] += lax.dot_general(
                held[rows, columns], masked, NT, preferred_element_type=F32
            )
    done = total[...].T
    even = side_of() == 0
    kept[...] = jnp.where(even, done[:half], done[half:])
    given[...] = jnp.where(even, done[half:], done[:half])


def fit_partial(densities, integrals, screen):
    count = densities.shape[0]
    height, width = integrals.shape
    pieces = 8 if width % (8 * TILE) == 0 else width // TILE
    half = struct((count // 2, height))
    return call(
        fit,
        [struct(integrals.shape, BF16), half, half],
        screen,
        densities,
        integrals,
        specs=[HBM] * 3,
        scratch=[
            pltpu.SMEM(screen.shape, jnp.int32),
            pltpu.VMEM(densities.shape, BF16),
            pltpu.VMEM((height, count), F32),
            pltpu.SemaphoreType.DMA((pieces + 2,)),
        ],
    )


def coulomb(screen, rounded, held, out):
    members, _, chunk = out.shape
    height = held.shape[0]
    for m in range(members):
        for t in range(m * chunk // TILE, (m + 1) * chunk // TILE):
            masked = jnp.concatenate(
                [
                    jnp.where(
                        screen[i, t] != 0,
                        rounded[:, i * TILE : (i + 1) * TILE],
                        jnp.zeros((), BF16),
                    )
                    for i in range(height // TILE)
                ],
                axis=1,
            )
            part = jnp.dot(
                masked, held[:, t * TILE : (t + 1) * TILE], preferred_element_type=F32
            )
            first = t * TILE - m * chunk
            out[m, :, first : first + TILE] = part.astype(out.dtype)


def coulomb_partial(rounded, held, screen):
    members = lax.axis_size("aux")
    out = struct((members, rounded.shape[0], held.shape[1] // members), BF16)
    return call(coulomb, out, screen, rounded, held, specs=[SMEM, VMEM, VMEM])


def scatter_sum(slabs):
    arrived = lax.all_to_all(slabs, "aux", 0, 0, tiled=True)
    return jnp.sum(arrived.astype(F32), axis=0)


def high_low(value):
    high = value.astype(BF16)
    return high, (value - high.astype(F32)).astype(BF16)


def times(value, high, low, dims=NN):
    rows = value.shape[0]
    coarse = value.astype(BF16).astype(F32)
    pair = jnp.concatenate([coarse, value - coarse], axis=0).astype(BF16)
    both = lax.dot_general(pair, high, dims, preferred_element_type=F32)
    both += lax.dot_general(pair, low, dims, preferred_element_type=F32)
    return both[:rows] + both[rows:]


def prepare(own_inv, mate_inv, own_fac, mate_fac, inv_high, inv_low, k_high, k_low, kt_high, kt_low):
    height = own_inv.shape[0]
    side = side_of()
    here = pl.ds(pl.multiple_of(side * height, height), height)
    there = pl.ds(pl.multiple_of((1 - side) * height, height), height)
    for ref, rows in ((own_inv, here), (mate_inv, there)):
        high, low = high_low(ref[...])
        inv_high[rows, :] = high
        inv_low[rows, :] = low

    @pl.when(block_of() > 0)
    def _():
        total = jnp.zeros(k_high.shape, F32)
        for inv, fac in ((own_inv, own_fac), (mate_inv, mate_fac)):
            ih, il = high_low(inv[...])
            fh, fl = high_low(fac[...])
            total += lax.dot_general(ih, fh, TN, preferred_element_type=F32)
            total += lax.dot_general(ih, fl, TN, preferred_element_type=F32)
            total += lax.dot_general(il, fh, TN, preferred_element_type=F32)
        high, low = high_low(total)
        k_high[...] = high
        k_low[...] = low
        high, low = high_low(total.T)
        kt_high[...] = high
        kt_low[...] = low


def merge(kept, mate, out):
    even = side_of() == 0
    height = kept.shape[1]
    out[:, :height] = jnp.where(even, kept[...], mate[...])
    out[:, height:] = jnp.where(even, mate[...], kept[...])


def begin(f0, f1, f2, f3, high, low, out):
    out[...] = times(f0[...] + f1[...] + f2[...] + f3[...], high[...], low[...])


def after_zero(one, two, three, e, high, low, out):
    block = block_of()
    known = jnp.where(block == 1, one[...], jnp.where(block == 2, two[...], three[...]))
    term = times(known, high[...], low[...])
    out[...] = jnp.where(block == 0, e[...], jnp.where(block == 1, e[...] - term, term))


def after_one(first, second, e, high, low, out):
    block = block_of()
    known = jnp.where(block == 3, second[...], first[...])
    behind = jnp.where(block == 3, first[...], second[...])
    total = behind + times(known, high[...], low[...])
    out[...] = jnp.where(block == 0, e[...], jnp.where(block == 3, total, e[...] - total))


def turn(known, behind, e, kt_high, kt_low, high, low, settled, back):
    value = e[...] - behind[...] - times(known[...], kt_high[...], kt_low[...])
    settled[...] = value
    back[...] = times(value, high[...], low[...])


def back_two(into, near, far, t, s, high, low, settled, back, mixed):
    plane = lax.axis_index("pair")
    last = block_of() == 3
    passed = jnp.where(plane == 0, far[...], jnp.where(plane == 1, near[...], t[...]))
    value = jnp.where(last, passed, s[...] - into[...])
    product = times(value, high[...], low[...])
    settled[...] = value
    back[...] = product
    mixed[...] = jnp.where(last, product, value)


def back_one(into, other, t, s, high, low, settled, back):
    plane = lax.axis_index("pair")
    block = block_of()
    passed = jnp.where(plane == 0, other[...], t[...])
    value = jnp.where(
        block == 1,
        s[...] - into[...] - other[...],
        jnp.where(block == 2, passed, t[...]),
    )
    settled[...] = value
    product = times(value, high[...], low[...])
    back[...] = jnp.where(block == 2, product + into[...], product)


def collect(e, z1, z2, z3, i0, i1, i2, i3, t, p1, p2, p3, out):
    plane = lax.axis_index("pair")
    block = block_of()

    def by_plane(a, b, c, d):
        return jnp.where(
            plane == 0, a[...], jnp.where(plane == 1, b[...], jnp.where(plane == 2, c[...], d[...]))
        )

    start = by_plane(e, z1, z2, z3)
    zero = start - by_plane(i0, i1, i2, i3) - by_plane(i3, i0, i1, i2)
    one = by_plane(t, p1, p2, p3)
    two = by_plane(t, t, p1, p2)
    three = by_plane(t, t, t, p1)
    out[...] = jnp.where(
        block == 0, zero, jnp.where(block == 1, one, jnp.where(block == 2, two, three))
    )


def finish(own, mate, inv, out):
    even = side_of() == 0
    value = jnp.concatenate(
        [jnp.where(even, own[...], mate[...]), jnp.where(even, mate[...], own[...])], axis=0
    )
    high, low = high_low(inv[...])
    out[...] = times(value, high, low, NT).astype(out.dtype)


def mm(a, b):
    return jnp.dot(a, b, precision=HIGHEST, preferred_element_type=F32)


def mm_t(a, b):
    return lax.dot_general(a, b, NT, precision=HIGHEST, preferred_element_type=F32)


def complete(moves, idle):
    chips = [(k, plane) for k in range(SOLVE_BLOCKS) for plane in range(SOLVE_BLOCKS)]
    used = {chip for move in moves for chip in move}
    spare = [chip for chip in idle if chip not in used] + [
        chip for chip in reversed(chips) if chip not in used and chip not in idle
    ]
    to = {}
    for (source, target), via in zip(moves, spare):
        to.update({source: target, target: via, via: source})
    return [(chip, to.get(chip, chip)) for chip in chips]


IDLE = [(1, 3), (2, 3), (3, 3), (0, 3), (1, 2), (2, 2), (0, 2), (1, 1), (0, 1)]


def chip_solve(kept, given, factor, diag_inv):
    half, height = kept.shape
    size = 2 * height
    planes = lax.axis_size("pair")

    def pairs_of(routes):
        pairs = []
        for (k_from, z_from), (k_to, z_to) in routes:
            for c in range(2):
                d = 1 - c if (k_from, z_from) == (k_to, z_to) else c
                pairs.append(
                    ((2 * k_from + c) * planes + z_from, (2 * k_to + d) * planes + z_to)
                )
        return pairs

    def send(value, *moves):
        return lax.ppermute(value, AXES, pairs_of(complete(moves, IDLE)))

    def swap(value):
        return lax.ppermute(value, "aux", [(i, i ^ 1) for i in range(2 * SOLVE_BLOCKS)])

    panel = struct((half, size))
    square = struct((size, size), BF16)
    inv_high, inv_low, k_high, k_low, kt_high, kt_low = call(
        prepare, [square] * 6, diag_inv, swap(diag_inv), factor, swap(factor), limit=32
    )
    part = call(merge, panel, kept, swap(given))
    home = [max(k - 1, 0) for k in range(SOLVE_BLOCKS)]
    gathered = []
    for step in range(1, planes):
        routes = []
        for k in range(SOLVE_BLOCKS):
            far = (home[k] + step) % planes
            for plane in range(planes):
                to = {home[k]: far, far: home[k]}.get(plane, plane)
                routes.append(((k, plane), (k, to)))
        gathered.append(lax.ppermute(part, AXES, pairs_of(routes)))
    e = call(begin, panel, part, *gathered, inv_high, inv_low)
    reach = [send(e, ((0, 0), (k, 0))) for k in range(1, SOLVE_BLOCKS)]
    one = call(after_zero, panel, *reach, e, kt_high, kt_low)
    first = send(one, ((1, 0), (2, 1)), ((3, 0), (3, 1)), ((0, 0), (0, 1)))
    second = send(one, ((1, 0), (3, 1)), ((2, 0), (2, 1)), ((0, 0), (0, 2)))
    two = call(after_one, panel, first, second, e, kt_high, kt_low)
    behind = send(two, ((3, 1), (3, 2)), ((0, 0), (0, 3)))
    known = send(two, ((2, 1), (3, 2)))
    t, back = call(turn, [panel] * 2, known, behind, e, kt_high, kt_low, k_high, k_low)
    into = send(back, ((3, 2), (2, 1)))
    near = send(t, ((3, 2), (3, 1)))
    far = send(t, ((3, 2), (3, 0)))
    t, back, mixed = call(back_two, [panel] * 3, into, near, far, t, two, k_high, k_low)
    into = send(back, ((2, 1), (1, 0)), ((3, 0), (2, 0)))
    other = send(mixed, ((3, 1), (1, 0)), ((2, 1), (2, 0)))
    t, back = call(back_one, [panel] * 2, into, other, t, one, k_high, k_low)
    into = [
        send(back, ((1, 0), (0, plane)), ((2, 0), (0, (plane + 1) % planes)))
        for plane in range(planes)
    ]
    spread = []
    for step in range(1, planes):
        moves = [((1, 0), (1, step))]
        if 1 + step < planes:
            moves.append(((2, 1), (2, 1 + step)))
        if 2 + step < planes:
            moves.append(((3, 2), (3, 2 + step)))
        spread.append(send(t, *moves))
    t = call(collect, panel, e, first, second, behind, *into, t, *spread)
    return call(finish, struct((2 * half, height), BF16), t, swap(t), diag_inv)


def chain_solve(kept, given, factor, diag_inv):
    even = lax.rem(lax.axis_index("aux"), 2) == 0
    partial_fit = jnp.concatenate(
        [jnp.where(even, kept, given), jnp.where(even, given, kept)], axis=0
    )
    count, height = partial_fit.shape
    breadth = factor.shape[1]
    block_size = diag_inv.shape[1]
    rows_aux = lax.axis_size("aux")
    total = height * rows_aux
    members = rows_aux // SOLVE_BLOCKS
    my_row = lax.axis_index("aux")
    my_column = lax.axis_index("pair")
    my_block = my_row // members
    column_block = (my_column * breadth + jnp.arange(breadth, dtype=jnp.int32)) // block_size
    factor_low = jnp.where((column_block < my_block)[None, :], factor, 0.0)

    def own_columns(whole):
        return lax.dynamic_slice_in_dim(whole, my_column * breadth, breadth, 1)

    zero_block = jnp.zeros((count, block_size), jnp.float32)
    solved = jnp.zeros((count, total), jnp.float32)
    for k in range(SOLVE_BLOCKS):

        def on_group(current):
            return mm(partial_fit - mm_t(own_columns(current), factor_low), diag_inv)

        def off_group(current):
            return zero_block

        summand = lax.cond(my_block == k, on_group, off_group, solved)
        arrived = lax.psum(summand, AXES)
        solved = lax.dynamic_update_slice_in_dim(solved, arrived, k * block_size, 1)
    own_coef = jnp.zeros((count, height), jnp.float32)
    contrib = jnp.zeros((count, total), jnp.float32)
    for target in reversed(range(SOLVE_BLOCKS)):
        settled = solved[:, target * block_size : (target + 1) * block_size]
        if target < SOLVE_BLOCKS - 1:
            portion = contrib[:, target * block_size : (target + 1) * block_size]
            settled = settled - lax.psum(portion, AXES)

        def on_group(state):
            coef = mm_t(settled, diag_inv)
            if target > 0:
                fresh = lax.dynamic_update_slice_in_dim(
                    jnp.zeros((count, total), jnp.float32),
                    mm(coef, factor_low),
                    my_column * breadth,
                    1,
                )
            else:
                fresh = state[1]
            return (coef, fresh)

        def keep_state(state):
            return state

        own_coef, contrib = lax.cond(my_block == target, on_group, keep_state, (own_coef, contrib))
    return own_coef.astype(jnp.bfloat16)


def shards(integrals, densities, screen, factor, diag_inv):
    block_size = diag_inv.shape[1]
    chip_blocks = (
        lax.axis_size("aux") == 2 * SOLVE_BLOCKS
        and factor.shape[1] == block_size
        and lax.axis_size("pair") == SOLVE_BLOCKS
    )
    solve = chip_solve if chip_blocks else chain_solve
    held, kept, given = fit_partial(densities, integrals, screen)
    rounded = solve(kept, given, factor, diag_inv)
    return scatter_sum(coulomb_partial(rounded, held, screen))


def solution(mesh):
    in_specs = (
        P("aux", "pair"),
        P(None, "pair"),
        P("aux", "pair"),
        P("aux", "pair"),
        P("aux", None),
    )
    out_specs = P(None, ("pair", "aux"))
    return jax.shard_map(shards, mesh=mesh, in_specs=in_specs, out_specs=out_specs, check_vma=False)
```

```python
import jax
import jax.numpy as jnp
from jax import lax
from jax.experimental import pallas as pl
from jax.experimental.pallas import tpu as pltpu
from jax.sharding import PartitionSpec as P

TILE = 128
SOLVE_BLOCKS = 4
AXES = ("aux", "pair")
HIGHEST = lax.Precision.HIGHEST
F32 = jnp.float32
BF16 = jnp.bfloat16
VMEM = pl.BlockSpec(memory_space=pltpu.VMEM)
SMEM = pl.BlockSpec(memory_space=pltpu.SMEM)
HBM = pl.BlockSpec(memory_space=pltpu.HBM)
MIB = 1024 * 1024
NN = (((1,), (0,)), ((), ()))
NT = (((1,), (1,)), ((), ()))
TN = (((0,), (0,)), ((), ()))


def struct(shape, dtype=F32):
    return jax.ShapeDtypeStruct(shape, dtype)


def call(kernel, outs, *operands, limit=12, specs=None, scratch=()):
    return pl.pallas_call(
        kernel,
        out_shape=outs,
        in_specs=specs or [VMEM] * len(operands),
        out_specs=jax.tree.map(lambda _: VMEM, outs),
        scratch_shapes=scratch,
        compiler_params=pltpu.CompilerParams(vmem_limit_bytes=limit * MIB),
    )(*operands)


def side_of():
    return lax.rem(lax.axis_index("aux"), 2)


def block_of():
    return lax.div(lax.axis_index("aux"), 2)


def fit(
    screen_in, densities_in, integrals, left, right, kept, given, screen, densities, total, arrived
):
    height, width = integrals.shape
    pieces = arrived.shape[0] - 2
    chunk = width // pieces
    half = kept.shape[0]
    small = [
        pltpu.make_async_copy(screen_in, screen, arrived.at[pieces]),
        pltpu.make_async_copy(densities_in, densities, arrived.at[pieces + 1]),
    ]
    copies = []
    held = []
    for j in range(pieces):
        ref = left if 2 * j < pieces else right
        start = j * chunk if ref is left else j * chunk - width // 2
        held.append(ref.at[:, start : start + chunk])
        copies.append(
            pltpu.make_async_copy(
                integrals.at[:, j * chunk : (j + 1) * chunk], held[j], arrived.at[j]
            )
        )
    for copy in small + copies:
        copy.start()
    total[...] = jnp.zeros_like(total)
    for copy in small:
        copy.wait()
    for j in range(pieces):
        copies[j].wait()
        for i in range(height // TILE):
            rows = slice(i * TILE, (i + 1) * TILE)
            masked = jnp.concatenate(
                [
                    jnp.where(
                        screen[i, t] != 0,
                        densities[:, t * TILE : (t + 1) * TILE],
                        jnp.zeros((), BF16),
                    )
                    for t in range(j * chunk // TILE, (j + 1) * chunk // TILE)
                ],
                axis=1,
            )
            total[rows, :] += lax.dot_general(
                held[j][rows, :], masked, NT, preferred_element_type=F32
            )
    done = total[...].T
    even = side_of() == 0
    kept[...] = jnp.where(even, done[:half], done[half:])
    given[...] = jnp.where(even, done[half:], done[:half])


def fit_partial(densities, integrals, screen):
    count = densities.shape[0]
    height, width = integrals.shape
    pieces = 8 if width % (8 * TILE) == 0 else width // TILE
    half = struct((count // 2, height))
    return call(
        fit,
        [struct((height, width // 2), BF16)] * 2 + [half, half],
        *(pltpu.with_memory_space_constraint(x, pltpu.HBM) for x in (screen, densities, integrals)),
        specs=[HBM] * 3,
        scratch=[
            pltpu.SMEM(screen.shape, jnp.int32),
            pltpu.VMEM(densities.shape, BF16),
            pltpu.VMEM((height, count), F32),
            pltpu.SemaphoreType.DMA((pieces + 2,)),
        ],
    )


def coulomb(screen, rounded, left, right, out):
    members, _, chunk = out.shape
    height, width = left.shape
    for m in range(members):
        for t in range(m * chunk // TILE, (m + 1) * chunk // TILE):
            masked = jnp.concatenate(
                [
                    jnp.where(
                        screen[i, t] != 0,
                        rounded[:, i * TILE : (i + 1) * TILE],
                        jnp.zeros((), BF16),
                    )
                    for i in range(height // TILE)
                ],
                axis=1,
            )
            held = left if t * TILE < width else right
            start = t * TILE if held is left else t * TILE - width
            part = jnp.dot(
                masked, held[:, start : start + TILE], preferred_element_type=F32
            )
            first = t * TILE - m * chunk
            out[m, :, first : first + TILE] = part.astype(out.dtype)


def coulomb_partial(rounded, left, right, screen):
    members = lax.axis_size("aux")
    out = struct((members, rounded.shape[0], 2 * left.shape[1] // members), BF16)
    return call(coulomb, out, screen, rounded, left, right, specs=[SMEM, VMEM, VMEM, VMEM])


def scatter_sum(slabs):
    arrived = lax.all_to_all(slabs, "aux", 0, 0, tiled=True)
    return jnp.sum(arrived.astype(F32), axis=0)


def high_low(value):
    high = value.astype(BF16)
    return high, (value - high.astype(F32)).astype(BF16)


def times(value, high, low, dims=NN):
    rows = value.shape[0]
    coarse = value.astype(BF16).astype(F32)
    pair = jnp.concatenate([coarse, value - coarse], axis=0).astype(BF16)
    both = lax.dot_general(pair, high, dims, preferred_element_type=F32)
    both += lax.dot_general(pair, low, dims, preferred_element_type=F32)
    return both[:rows] + both[rows:]


def prepare(own_inv, mate_inv, own_fac, mate_fac, inv_high, inv_low, k_high, k_low, kt_high, kt_low):
    height = own_inv.shape[0]
    side = side_of()
    here = pl.ds(pl.multiple_of(side * height, height), height)
    there = pl.ds(pl.multiple_of((1 - side) * height, height), height)
    for ref, rows in ((own_inv, here), (mate_inv, there)):
        high, low = high_low(ref[...])
        inv_high[rows, :] = high
        inv_low[rows, :] = low

    @pl.when(block_of() > 0)
    def _():
        total = jnp.zeros(k_high.shape, F32)
        for inv, fac in ((own_inv, own_fac), (mate_inv, mate_fac)):
            ih, il = high_low(inv[...])
            fh, fl = high_low(fac[...])
            total += lax.dot_general(ih, fh, TN, preferred_element_type=F32)
            total += lax.dot_general(ih, fl, TN, preferred_element_type=F32)
            total += lax.dot_general(il, fh, TN, preferred_element_type=F32)
        high, low = high_low(total)
        k_high[...] = high
        k_low[...] = low
        high, low = high_low(total.T)
        kt_high[...] = high
        kt_low[...] = low


def merge(kept, mate, out):
    even = side_of() == 0
    height = kept.shape[1]
    out[:, :height] = jnp.where(even, kept[...], mate[...])
    out[:, height:] = jnp.where(even, mate[...], kept[...])


def begin(f0, f1, f2, f3, high, low, out):
    out[...] = times(f0[...] + f1[...] + f2[...] + f3[...], high[...], low[...])


def after_zero(one, two, three, e, high, low, out):
    block = block_of()
    known = jnp.where(block == 1, one[...], jnp.where(block == 2, two[...], three[...]))
    term = times(known, high[...], low[...])
    out[...] = jnp.where(block == 0, e[...], jnp.where(block == 1, e[...] - term, term))


def after_one(first, second, e, high, low, out):
    block = block_of()
    known = jnp.where(block == 3, second[...], first[...])
    behind = jnp.where(block == 3, first[...], second[...])
    total = behind + times(known, high[...], low[...])
    out[...] = jnp.where(block == 0, e[...], jnp.where(block == 3, total, e[...] - total))


def turn(known, behind, e, kt_high, kt_low, high, low, settled, back):
    value = e[...] - behind[...] - times(known[...], kt_high[...], kt_low[...])
    settled[...] = value
    back[...] = times(value, high[...], low[...])


def back_two(into, near, far, t, s, high, low, settled, back, mixed):
    plane = lax.axis_index("pair")
    last = block_of() == 3
    passed = jnp.where(plane == 0, far[...], jnp.where(plane == 1, near[...], t[...]))
    value = jnp.where(last, passed, s[...] - into[...])
    product = times(value, high[...], low[...])
    settled[...] = value
    back[...] = product
    mixed[...] = jnp.where(last, product, value)


def back_one(into, other, t, s, high, low, settled, back):
    plane = lax.axis_index("pair")
    block = block_of()
    passed = jnp.where(plane == 0, other[...], t[...])
    value = jnp.where(
        block == 1,
        s[...] - into[...] - other[...],
        jnp.where(block == 2, passed, t[...]),
    )
    settled[...] = value
    product = times(value, high[...], low[...])
    back[...] = jnp.where(block == 2, product + into[...], product)


def collect(e, z1, z2, z3, i0, i1, i2, i3, t, p1, p2, p3, out):
    plane = lax.axis_index("pair")
    block = block_of()

    def by_plane(a, b, c, d):
        return jnp.where(
            plane == 0, a[...], jnp.where(plane == 1, b[...], jnp.where(plane == 2, c[...], d[...]))
        )

    start = by_plane(e, z1, z2, z3)
    zero = start - by_plane(i0, i1, i2, i3) - by_plane(i3, i0, i1, i2)
    one = by_plane(t, p1, p2, p3)
    two = by_plane(t, t, p1, p2)
    three = by_plane(t, t, t, p1)
    out[...] = jnp.where(
        block == 0, zero, jnp.where(block == 1, one, jnp.where(block == 2, two, three))
    )


def finish(own, mate, inv, out):
    even = side_of() == 0
    value = jnp.concatenate(
        [jnp.where(even, own[...], mate[...]), jnp.where(even, mate[...], own[...])], axis=0
    )
    high, low = high_low(inv[...])
    out[...] = times(value, high, low, NT).astype(out.dtype)


def mm(a, b):
    return jnp.dot(a, b, precision=HIGHEST, preferred_element_type=F32)


def mm_t(a, b):
    return lax.dot_general(a, b, NT, precision=HIGHEST, preferred_element_type=F32)


def complete(moves):
    to = {}
    for source, target, *via in moves:
        chain = [source, target, *via]
        to.update(zip(chain, chain[1:] + chain[:1]))
    chips = [(k, plane) for k in range(SOLVE_BLOCKS) for plane in range(SOLVE_BLOCKS)]
    return [(chip, to.get(chip, chip)) for chip in chips]


def chip_solve(kept, given, factor, diag_inv):
    half, height = kept.shape
    size = 2 * height
    planes = lax.axis_size("pair")

    def pairs_of(routes):
        pairs = []
        for (k_from, z_from), (k_to, z_to) in routes:
            for c in range(2):
                d = 1 - c if (k_from, z_from) == (k_to, z_to) else c
                pairs.append(
                    ((2 * k_from + c) * planes + z_from, (2 * k_to + d) * planes + z_to)
                )
        return pairs

    def send(value, *moves):
        return lax.ppermute(value, AXES, pairs_of(complete(moves)))

    def swap(value):
        return lax.ppermute(value, "aux", [(i, i ^ 1) for i in range(2 * SOLVE_BLOCKS)])

    panel = struct((half, size))
    square = struct((size, size), BF16)
    inv_high, inv_low, k_high, k_low, kt_high, kt_low = call(
        prepare, [square] * 6, diag_inv, swap(diag_inv), factor, swap(factor), limit=32
    )
    part = call(merge, panel, kept, swap(given))
    home = [max(k - 1, 0) for k in range(SOLVE_BLOCKS)]
    gathered = [
        send(
            part,
            *(((k, (home[k] + step) % planes), (k, home[k])) for k in range(SOLVE_BLOCKS)),
        )
        for step in range(1, planes)
    ]
    e = call(begin, panel, part, *gathered, inv_high, inv_low)
    reach = [send(e, ((0, 0), (k, 0))) for k in range(1, SOLVE_BLOCKS)]
    one = call(after_zero, panel, *reach, e, kt_high, kt_low)
    first = send(one, ((1, 0), (2, 1), (1, 3)), ((3, 0), (3, 1), (3, 3)), ((0, 0), (0, 1)))
    second = send(one, ((1, 0), (3, 1)), ((2, 0), (2, 1)), ((0, 0), (0, 2)))
    two = call(after_one, panel, first, second, e, kt_high, kt_low)
    behind = send(two, ((3, 1), (3, 2), (2, 3)), ((0, 0), (0, 3)))
    known = send(two, ((2, 1), (3, 2)))
    t, back = call(turn, [panel] * 2, known, behind, e, kt_high, kt_low, k_high, k_low)
    into = send(back, ((3, 2), (2, 1)))
    near = send(t, ((3, 2), (3, 1)))
    far = send(t, ((3, 2), (3, 0)))
    t, back, mixed = call(back_two, [panel] * 3, into, near, far, t, two, k_high, k_low)
    into = send(back, ((2, 1), (1, 0), (2, 3)), ((3, 0), (2, 0), (3, 3)))
    other = send(mixed, ((3, 1), (1, 0)), ((2, 1), (2, 0)))
    t, back = call(back_one, [panel] * 2, into, other, t, one, k_high, k_low)
    vias = [(2, 2), (2, 3), (3, 3), (3, 1)]
    into = [
        send(back, ((1, 0), (0, plane)), ((2, 0), (0, (plane + 1) % planes), vias[plane]))
        for plane in range(planes)
    ]
    spread = []
    for step in range(1, planes):
        moves = [((1, 0), (1, step))]
        if 1 + step < planes:
            moves.append(((2, 1), (2, 1 + step)))
        if 2 + step < planes:
            moves.append(((3, 2), (3, 2 + step)))
        spread.append(send(t, *moves))
    t = call(collect, panel, e, first, second, behind, *into, t, *spread)
    return call(finish, struct((2 * half, height), BF16), t, swap(t), diag_inv)


def chain_solve(kept, given, factor, diag_inv):
    even = lax.rem(lax.axis_index("aux"), 2) == 0
    partial_fit = jnp.concatenate(
        [jnp.where(even, kept, given), jnp.where(even, given, kept)], axis=0
    )
    count, height = partial_fit.shape
    breadth = factor.shape[1]
    block_size = diag_inv.shape[1]
    rows_aux = lax.axis_size("aux")
    total = height * rows_aux
    members = rows_aux // SOLVE_BLOCKS
    my_row = lax.axis_index("aux")
    my_column = lax.axis_index("pair")
    my_block = my_row // members
    column_block = (my_column * breadth + jnp.arange(breadth, dtype=jnp.int32)) // block_size
    factor_low = jnp.where((column_block < my_block)[None, :], factor, 0.0)

    def own_columns(whole):
        return lax.dynamic_slice_in_dim(whole, my_column * breadth, breadth, 1)

    zero_block = jnp.zeros((count, block_size), jnp.float32)
    solved = jnp.zeros((count, total), jnp.float32)
    for k in range(SOLVE_BLOCKS):

        def on_group(current):
            return mm(partial_fit - mm_t(own_columns(current), factor_low), diag_inv)

        def off_group(current):
            return zero_block

        summand = lax.cond(my_block == k, on_group, off_group, solved)
        arrived = lax.psum(summand, AXES)
        solved = lax.dynamic_update_slice_in_dim(solved, arrived, k * block_size, 1)
    own_coef = jnp.zeros((count, height), jnp.float32)
    contrib = jnp.zeros((count, total), jnp.float32)
    for target in reversed(range(SOLVE_BLOCKS)):
        settled = solved[:, target * block_size : (target + 1) * block_size]
        if target < SOLVE_BLOCKS - 1:
            portion = contrib[:, target * block_size : (target + 1) * block_size]
            settled = settled - lax.psum(portion, AXES)

        def on_group(state):
            coef = mm_t(settled, diag_inv)
            if target > 0:
                fresh = lax.dynamic_update_slice_in_dim(
                    jnp.zeros((count, total), jnp.float32),
                    mm(coef, factor_low),
                    my_column * breadth,
                    1,
                )
            else:
                fresh = state[1]
            return (coef, fresh)

        def keep_state(state):
            return state

        own_coef, contrib = lax.cond(my_block == target, on_group, keep_state, (own_coef, contrib))
    return own_coef.astype(jnp.bfloat16)


def shards(integrals, densities, screen, factor, diag_inv):
    block_size = diag_inv.shape[1]
    chip_blocks = (
        lax.axis_size("aux") == 2 * SOLVE_BLOCKS
        and factor.shape[1] == block_size
        and lax.axis_size("pair") == SOLVE_BLOCKS
    )
    solve = chip_solve if chip_blocks else chain_solve
    left, right, kept, given = fit_partial(densities, integrals, screen)
    rounded = solve(kept, given, factor, diag_inv)
    return scatter_sum(coulomb_partial(rounded, left, right, screen))


def solution(mesh):
    in_specs = (
        P("aux", "pair"),
        P(None, "pair"),
        P("aux", "pair"),
        P("aux", "pair"),
        P("aux", None),
    )
    out_specs = P(None, ("pair", "aux"))
    return jax.shard_map(shards, mesh=mesh, in_specs=in_specs, out_specs=out_specs, check_vma=False)
```

```python
import jax
import jax.numpy as jnp
from jax import lax
from jax.experimental import pallas as pl
from jax.experimental.pallas import tpu as pltpu
from jax.sharding import PartitionSpec as P

TILE = 128
SOLVE_BLOCKS = 4
AXES = ("aux", "pair")
HIGHEST = lax.Precision.HIGHEST
F32 = jnp.float32
BF16 = jnp.bfloat16
VMEM = pl.BlockSpec(memory_space=pltpu.VMEM)
SMEM = pl.BlockSpec(memory_space=pltpu.SMEM)
HBM = pl.BlockSpec(memory_space=pltpu.HBM)
MIB = 1024 * 1024
NN = (((1,), (0,)), ((), ()))
NT = (((1,), (1,)), ((), ()))
TN = (((0,), (0,)), ((), ()))


def struct(shape, dtype=F32):
    return jax.ShapeDtypeStruct(shape, dtype)


def call(kernel, outs, *operands, limit=12, specs=None, scratch=()):
    return pl.pallas_call(
        kernel,
        out_shape=outs,
        in_specs=specs or [VMEM] * len(operands),
        out_specs=jax.tree.map(lambda _: VMEM, outs),
        scratch_shapes=scratch,
        compiler_params=pltpu.CompilerParams(vmem_limit_bytes=limit * MIB),
    )(*operands)


def side_of():
    return lax.rem(lax.axis_index("aux"), 2)


def block_of():
    return lax.div(lax.axis_index("aux"), 2)


def fit(
    screen_in, densities_in, integrals, left, right, out, screen, densities, total, arrived
):
    height, width = integrals.shape
    pieces = arrived.shape[0] - 2
    chunk = width // pieces
    small = [
        pltpu.make_async_copy(screen_in, screen, arrived.at[pieces]),
        pltpu.make_async_copy(densities_in, densities, arrived.at[pieces + 1]),
    ]
    copies = []
    held = []
    for j in range(pieces):
        ref = left if 2 * j < pieces else right
        start = j * chunk if ref is left else j * chunk - width // 2
        held.append(ref.at[:, start : start + chunk])
        copies.append(
            pltpu.make_async_copy(
                integrals.at[:, j * chunk : (j + 1) * chunk], held[j], arrived.at[j]
            )
        )
    for copy in small + copies:
        copy.start()
    total[...] = jnp.zeros_like(total)
    for copy in small:
        copy.wait()
    for j in range(pieces):
        copies[j].wait()
        for i in range(height // TILE):
            rows = slice(i * TILE, (i + 1) * TILE)
            masked = jnp.concatenate(
                [
                    jnp.where(
                        screen[i, t] != 0,
                        densities[:, t * TILE : (t + 1) * TILE],
                        jnp.zeros((), BF16),
                    )
                    for t in range(j * chunk // TILE, (j + 1) * chunk // TILE)
                ],
                axis=1,
            )
            total[rows, :] += lax.dot_general(
                held[j][rows, :], masked, NT, preferred_element_type=F32
            )
    out[...] = total[...].T


def fit_partial(densities, integrals, screen):
    count = densities.shape[0]
    height, width = integrals.shape
    pieces = 8 if width % (8 * TILE) == 0 else width // TILE
    return call(
        fit,
        [struct((height, width // 2), BF16)] * 2 + [struct((count, height))],
        *(pltpu.with_memory_space_constraint(x, pltpu.HBM) for x in (screen, densities, integrals)),
        specs=[HBM] * 3,
        scratch=[
            pltpu.SMEM(screen.shape, jnp.int32),
            pltpu.VMEM(densities.shape, BF16),
            pltpu.VMEM((height, count), F32),
            pltpu.SemaphoreType.DMA((pieces + 2,)),
        ],
    )


def coulomb(screen, rounded, left, right, out):
    members, _, chunk = out.shape
    height, width = left.shape
    for m in range(members):
        for t in range(m * chunk // TILE, (m + 1) * chunk // TILE):
            masked = jnp.concatenate(
                [
                    jnp.where(
                        screen[i, t] != 0,
                        rounded[:, i * TILE : (i + 1) * TILE],
                        jnp.zeros((), BF16),
                    )
                    for i in range(height // TILE)
                ],
                axis=1,
            )
            held = left if t * TILE < width else right
            start = t * TILE if held is left else t * TILE - width
            part = jnp.dot(
                masked, held[:, start : start + TILE], preferred_element_type=F32
            )
            first = t * TILE - m * chunk
            out[m, :, first : first + TILE] = part.astype(out.dtype)


def coulomb_partial(rounded, left, right, screen):
    members = lax.axis_size("aux")
    out = struct((members, rounded.shape[0], 2 * left.shape[1] // members), BF16)
    return call(coulomb, out, screen, rounded, left, right, specs=[SMEM, VMEM, VMEM, VMEM])


def scatter_sum(slabs):
    arrived = lax.all_to_all(slabs, "aux", 0, 0, tiled=True)
    return jnp.sum(arrived.astype(F32), axis=0)


def high_low(value):
    high = value.astype(BF16)
    return high, (value - high.astype(F32)).astype(BF16)


def times(value, high, low, dims=NN):
    rows = value.shape[0]
    coarse = value.astype(BF16).astype(F32)
    pair = jnp.concatenate([coarse, value - coarse], axis=0).astype(BF16)
    both = lax.dot_general(pair, high, dims, preferred_element_type=F32)
    both += lax.dot_general(pair, low, dims, preferred_element_type=F32)
    return both[:rows] + both[rows:]


def prepare(own_inv, mate_inv, own_fac, mate_fac, k_high, k_low, kt_high, kt_low):
    @pl.when((block_of() > 0) & (side_of() == 0))
    def _():
        total = jnp.zeros(k_high.shape, F32)
        for inv, fac in ((own_inv, own_fac), (mate_inv, mate_fac)):
            ih, il = high_low(inv[...])
            fh, fl = high_low(fac[...])
            total += lax.dot_general(ih, fh, TN, preferred_element_type=F32)
            total += lax.dot_general(ih, fl, TN, preferred_element_type=F32)
            total += lax.dot_general(il, fh, TN, preferred_element_type=F32)
        high, low = high_low(total)
        k_high[...] = high
        k_low[...] = low
        high, low = high_low(total.T)
        kt_high[...] = high
        kt_low[...] = low


def begin(f0, f1, f2, f3, inv, after, out):
    high, low = high_low(inv[...])
    out[...] = times(f0[...] + f1[...] + f2[...] + f3[...], high, low)


def both(own, mate, out):
    out[...] = own[...] + mate[...]


def after_zero(one, two, three, e, high, low, out):
    block = block_of()
    known = jnp.where(block == 1, one[...], jnp.where(block == 2, two[...], three[...]))
    term = times(known, high[...], low[...])
    out[...] = jnp.where(block == 0, e[...], jnp.where(block == 1, e[...] - term, term))


def after_one(first, second, e, high, low, out):
    block = block_of()
    known = jnp.where(block == 3, second[...], first[...])
    behind = jnp.where(block == 3, first[...], second[...])
    total = behind + times(known, high[...], low[...])
    out[...] = jnp.where(block == 0, e[...], jnp.where(block == 3, total, e[...] - total))


def turn(known, behind, e, kt_high, kt_low, high, low, settled, back):
    value = e[...] - behind[...] - times(known[...], kt_high[...], kt_low[...])
    settled[...] = value
    back[...] = times(value, high[...], low[...])


def back_two(into, near, far, t, s, high, low, settled, back, mixed):
    plane = lax.axis_index("pair")
    last = block_of() == 3
    passed = jnp.where(plane == 0, far[...], jnp.where(plane == 1, near[...], t[...]))
    value = jnp.where(last, passed, s[...] - into[...])
    product = times(value, high[...], low[...])
    settled[...] = value
    back[...] = product
    mixed[...] = jnp.where(last, product, value)


def back_one(into, other, t, s, high, low, settled, back):
    plane = lax.axis_index("pair")
    block = block_of()
    passed = jnp.where(plane == 0, other[...], t[...])
    value = jnp.where(
        block == 1,
        s[...] - into[...] - other[...],
        jnp.where(block == 2, passed, t[...]),
    )
    settled[...] = value
    product = times(value, high[...], low[...])
    back[...] = jnp.where(block == 2, product + into[...], product)


def collect(e, z1, z2, z3, i0, i1, i2, i3, t, p1, p2, p3, out):
    plane = lax.axis_index("pair")
    block = block_of()

    def by_plane(a, b, c, d):
        return jnp.where(
            plane == 0, a[...], jnp.where(plane == 1, b[...], jnp.where(plane == 2, c[...], d[...]))
        )

    start = by_plane(e, z1, z2, z3)
    zero = start - by_plane(i0, i1, i2, i3) - by_plane(i3, i0, i1, i2)
    one = by_plane(t, p1, p2, p3)
    two = by_plane(t, t, p1, p2)
    three = by_plane(t, t, t, p1)
    out[...] = jnp.where(
        block == 0, zero, jnp.where(block == 1, one, jnp.where(block == 2, two, three))
    )


def finish(own, mate, inv, out):
    value = jnp.where(side_of() == 0, own[...], mate[...])
    high, low = high_low(inv[...])
    out[...] = times(value, high, low, NT).astype(out.dtype)


def mm(a, b):
    return jnp.dot(a, b, precision=HIGHEST, preferred_element_type=F32)


def mm_t(a, b):
    return lax.dot_general(a, b, NT, precision=HIGHEST, preferred_element_type=F32)


def chip_solve(partial_fit, factor, diag_inv):
    count, height = partial_fit.shape
    size = 2 * height
    planes = lax.axis_size("pair")
    chips = [(k, plane) for k in range(SOLVE_BLOCKS) for plane in range(planes)]

    def device(chip, c):
        return (2 * chip[0] + c) * planes + chip[1]

    def permute(value, to):
        for chip in chips:
            for c in range(2):
                to.setdefault(device(chip, c), device(chip, 1 - c))
        return lax.ppermute(value, AXES, sorted(to.items()))

    def send(value, *moves):
        to = {}
        for source, target in moves:
            loop = [device(source, 0), device(target, 0), device(target, 1), device(source, 1)]
            to.update(zip(loop, loop[1:] + loop[:1]))
        return permute(value, to)

    def swap(value):
        return lax.ppermute(value, "aux", [(i, i ^ 1) for i in range(2 * SOLVE_BLOCKS)])

    panel = struct((count, size))
    square = struct((size, size), BF16)
    k_high, k_low, kt_high, kt_low = call(
        prepare, [square] * 4, diag_inv, swap(diag_inv), factor, swap(factor), limit=32
    )
    home = [max(k - 1, 0) for k in range(SOLVE_BLOCKS)]
    gathered = []
    for step in range(1, planes):
        to = {}
        for k in range(SOLVE_BLOCKS):
            for c in range(2):
                near = device((k, home[k]), c)
                far = device((k, (home[k] + step) % planes), c)
                to.update({near: far, far: near})
        gathered.append(permute(partial_fit, to))
    e = call(begin, panel, partial_fit, *gathered, diag_inv, k_high)
    e = call(both, panel, e, swap(e))
    reach = [send(e, ((0, 0), (k, 0))) for k in range(1, SOLVE_BLOCKS)]
    one = call(after_zero, panel, *reach, e, kt_high, kt_low)
    first = send(one, ((1, 0), (2, 1)), ((3, 0), (3, 1)), ((0, 0), (0, 1)))
    second = send(one, ((1, 0), (3, 1)), ((2, 0), (2, 1)), ((0, 0), (0, 2)))
    two = call(after_one, panel, first, second, e, kt_high, kt_low)
    behind = send(two, ((3, 1), (3, 2)), ((0, 0), (0, 3)))
    known = send(two, ((2, 1), (3, 2)))
    t, back = call(turn, [panel] * 2, known, behind, e, kt_high, kt_low, k_high, k_low)
    into = send(back, ((3, 2), (2, 1)))
    near = send(t, ((3, 2), (3, 1)))
    far = send(t, ((3, 2), (3, 0)))
    t, back, mixed = call(back_two, [panel] * 3, into, near, far, t, two, k_high, k_low)
    into = send(back, ((2, 1), (1, 0)), ((3, 0), (2, 0)))
    other = send(mixed, ((3, 1), (1, 0)), ((2, 1), (2, 0)))
    t, back = call(back_one, [panel] * 2, into, other, t, one, k_high, k_low)
    into = [
        send(back, ((1, 0), (0, plane)), ((2, 0), (0, (plane + 1) % planes)))
        for plane in range(planes)
    ]
    spread = []
    for step in range(1, planes):
        moves = [((1, 0), (1, step))]
        if 1 + step < planes:
            moves.append(((2, 1), (2, 1 + step)))
        if 2 + step < planes:
            moves.append(((3, 2), (3, 2 + step)))
        spread.append(send(t, *moves))
    t = call(collect, panel, e, first, second, behind, *into, t, *spread)
    return call(finish, struct((count, height), BF16), t, swap(t), diag_inv)


def chain_solve(partial_fit, factor, diag_inv):
    count, height = partial_fit.shape
    breadth = factor.shape[1]
    block_size = diag_inv.shape[1]
    rows_aux = lax.axis_size("aux")
    total = height * rows_aux
    members = rows_aux // SOLVE_BLOCKS
    my_row = lax.axis_index("aux")
    my_column = lax.axis_index("pair")
    my_block = my_row // members
    column_block = (my_column * breadth + jnp.arange(breadth, dtype=jnp.int32)) // block_size
    factor_low = jnp.where((column_block < my_block)[None, :], factor, 0.0)

    def own_columns(whole):
        return lax.dynamic_slice_in_dim(whole, my_column * breadth, breadth, 1)

    zero_block = jnp.zeros((count, block_size), jnp.float32)
    solved = jnp.zeros((count, total), jnp.float32)
    for k in range(SOLVE_BLOCKS):

        def on_group(current):
            return mm(partial_fit - mm_t(own_columns(current), factor_low), diag_inv)

        def off_group(current):
            return zero_block

        summand = lax.cond(my_block == k, on_group, off_group, solved)
        arrived = lax.psum(summand, AXES)
        solved = lax.dynamic_update_slice_in_dim(solved, arrived, k * block_size, 1)
    own_coef = jnp.zeros((count, height), jnp.float32)
    contrib = jnp.zeros((count, total), jnp.float32)
    for target in reversed(range(SOLVE_BLOCKS)):
        settled = solved[:, target * block_size : (target + 1) * block_size]
        if target < SOLVE_BLOCKS - 1:
            portion = contrib[:, target * block_size : (target + 1) * block_size]
            settled = settled - lax.psum(portion, AXES)

        def on_group(state):
            coef = mm_t(settled, diag_inv)
            if target > 0:
                fresh = lax.dynamic_update_slice_in_dim(
                    jnp.zeros((count, total), jnp.float32),
                    mm(coef, factor_low),
                    my_column * breadth,
                    1,
                )
            else:
                fresh = state[1]
            return (coef, fresh)

        def keep_state(state):
            return state

        own_coef, contrib = lax.cond(my_block == target, on_group, keep_state, (own_coef, contrib))
    return own_coef.astype(jnp.bfloat16)


def shards(integrals, densities, screen, factor, diag_inv):
    block_size = diag_inv.shape[1]
    chip_blocks = (
        lax.axis_size("aux") == 2 * SOLVE_BLOCKS
        and factor.shape[1] == block_size
        and lax.axis_size("pair") == SOLVE_BLOCKS
    )
    solve = chip_solve if chip_blocks else chain_solve
    left, right, partial_fit = fit_partial(densities, integrals, screen)
    rounded = solve(partial_fit, factor, diag_inv)
    return scatter_sum(coulomb_partial(rounded, left, right, screen))


def solution(mesh):
    in_specs = (
        P("aux", "pair"),
        P(None, "pair"),
        P("aux", "pair"),
        P("aux", "pair"),
        P("aux", None),
    )
    out_specs = P(None, ("pair", "aux"))
    return jax.shard_map(shards, mesh=mesh, in_specs=in_specs, out_specs=out_specs, check_vma=False)
```

```python
import jax
import jax.numpy as jnp
from jax import lax
from jax.experimental import pallas as pl
from jax.experimental.pallas import tpu as pltpu
from jax.sharding import PartitionSpec as P

TILE = 128
SOLVE_BLOCKS = 4
AXES = ("aux", "pair")
HIGHEST = lax.Precision.HIGHEST
F32 = jnp.float32
BF16 = jnp.bfloat16
VMEM = pl.BlockSpec(memory_space=pltpu.VMEM)
SMEM = pl.BlockSpec(memory_space=pltpu.SMEM)
HBM = pl.BlockSpec(memory_space=pltpu.HBM)
MIB = 1024 * 1024
NN = (((1,), (0,)), ((), ()))
NT = (((1,), (1,)), ((), ()))
TN = (((0,), (0,)), ((), ()))


def struct(shape, dtype=F32):
    return jax.ShapeDtypeStruct(shape, dtype)


def call(kernel, outs, *operands, limit=12, specs=None, scratch=()):
    return pl.pallas_call(
        kernel,
        out_shape=outs,
        in_specs=specs or [VMEM] * len(operands),
        out_specs=jax.tree.map(lambda _: VMEM, outs),
        scratch_shapes=scratch,
        compiler_params=pltpu.CompilerParams(vmem_limit_bytes=limit * MIB),
    )(*operands)


def side_of():
    return lax.rem(lax.axis_index("aux"), 2)


def block_of():
    return lax.div(lax.axis_index("aux"), 2)


def masked_row(screen, densities, i, tiles):
    zero = jnp.zeros((), densities.dtype)
    return jnp.concatenate(
        [
            jnp.where(screen[i, t] != 0, densities[:, t * TILE : (t + 1) * TILE], zero)
            for t in tiles
        ],
        axis=1,
    )


def fit(
    screen_in, densities_in, integrals, left, right, out, screen, densities, total, arrived
):
    height, width = integrals.shape
    pieces = arrived.shape[0] - 2
    chunk = width // pieces
    small = [
        pltpu.make_async_copy(screen_in, screen, arrived.at[pieces]),
        pltpu.make_async_copy(densities_in, densities, arrived.at[pieces + 1]),
    ]
    copies = []
    held = []
    for j in range(pieces):
        ref = left if 2 * j < pieces else right
        start = j * chunk if ref is left else j * chunk - width // 2
        held.append(ref.at[:, start : start + chunk])
        copies.append(
            pltpu.make_async_copy(
                integrals.at[:, j * chunk : (j + 1) * chunk], held[j], arrived.at[j]
            )
        )
    for copy in small + copies:
        copy.start()
    total[...] = jnp.zeros_like(total)
    for copy in small:
        copy.wait()
    count = densities.shape[0]
    strips = height // TILE
    for j in range(pieces):
        tiles = range(j * chunk // TILE, (j + 1) * chunk // TILE)
        stacked = jnp.concatenate([masked_row(screen, densities, i, tiles) for i in range(strips)])
        copies[j].wait()
        total[...] += lax.dot_general(held[j][...], stacked, NT, preferred_element_type=F32)
    done = total[...].T
    for i in range(strips):
        out[:, i * TILE : (i + 1) * TILE] = done[
            i * count : (i + 1) * count, i * TILE : (i + 1) * TILE
        ]


def fit_partial(densities, integrals, screen):
    count = densities.shape[0]
    height, width = integrals.shape
    pieces = 8 if width % (8 * TILE) == 0 else width // TILE
    return call(
        fit,
        [struct((height, width // 2), BF16)] * 2 + [struct((count, height))],
        *(pltpu.with_memory_space_constraint(x, pltpu.HBM) for x in (screen, densities, integrals)),
        specs=[HBM] * 3,
        scratch=[
            pltpu.SMEM(screen.shape, jnp.int32),
            pltpu.VMEM(densities.shape, BF16),
            pltpu.VMEM((height, height // TILE * count), F32),
            pltpu.SemaphoreType.DMA((pieces + 2,)),
        ],
    )


def coulomb(screen, rounded, left, right, out):
    members, count, chunk = out.shape
    height, width = left.shape
    strips = height // TILE
    value = rounded[...]
    strip_of = lax.broadcasted_iota(jnp.int32, value.shape, 1) // TILE
    stacked = jnp.concatenate(
        [jnp.where(strip_of == i, value, jnp.zeros((), BF16)) for i in range(strips)]
    )
    for m in range(members):
        held = left if m * chunk < width else right
        start = m * chunk if held is left else m * chunk - width
        parts = jnp.dot(stacked, held[:, start : start + chunk], preferred_element_type=F32)
        for t in range(chunk // TILE):
            lanes = slice(t * TILE, (t + 1) * TILE)
            total = jnp.zeros((count, TILE), F32)
            for i in range(strips):
                part = parts[i * count : (i + 1) * count, lanes]
                total += jnp.where(screen[i, m * chunk // TILE + t] != 0, part, 0.0)
            out[m, :, lanes] = total.astype(out.dtype)


def coulomb_partial(rounded, left, right, screen):
    members = lax.axis_size("aux")
    out = struct((members, rounded.shape[0], 2 * left.shape[1] // members), BF16)
    return call(coulomb, out, screen, rounded, left, right, specs=[SMEM, VMEM, VMEM, VMEM])


def scatter_sum(slabs):
    arrived = lax.all_to_all(slabs, "aux", 0, 0, tiled=True)
    return jnp.sum(arrived.astype(F32), axis=0)


def high_low(value):
    high = value.astype(BF16)
    return high, (value - high.astype(F32)).astype(BF16)


def times(value, high, low, dims=NN):
    rows = value.shape[0]
    coarse = value.astype(BF16).astype(F32)
    pair = jnp.concatenate([coarse, value - coarse], axis=0).astype(BF16)
    both = lax.dot_general(pair, high, dims, preferred_element_type=F32)
    both += lax.dot_general(pair, low, dims, preferred_element_type=F32)
    return both[:rows] + both[rows:]


def prepare(inv0, inv1, fac0, fac1, k_high, k_low, kt_high, kt_low, lhs, rhs):
    height = inv0.shape[0]

    @pl.when((block_of() > 0) & (side_of() == 0))
    def _():
        for n, (inv, fac) in enumerate(((inv0, fac0), (inv1, fac1))):
            rows = [slice((3 * n + r) * height, (3 * n + r + 1) * height) for r in range(3)]
            high, low = high_low(inv[...])
            lhs[rows[0], :], lhs[rows[1], :], lhs[rows[2], :] = high, low, high
            high, low = high_low(fac[...])
            rhs[rows[0], :], rhs[rows[1], :], rhs[rows[2], :] = high, high, low
        depth = 3 * height
        halves = (
            (slice(0, height), slice(0, depth)),
            (slice(height, 2 * height), slice(0, 2 * depth)),
        )
        for part, used in halves:
            product = lax.dot_general(lhs[used, part], rhs[used, :], TN, preferred_element_type=F32)
            k_high[part, :], k_low[part, :] = high_low(product)
            kt_high[:, part], kt_low[:, part] = high_low(product.T)


def begin(f0, f1, f2, f3, inv, out):
    high, low = high_low(inv[...])
    out[...] = times(f0[...] + f1[...] + f2[...] + f3[...], high, low)


def both(own, mate, out):
    out[...] = own[...] + mate[...]


def after_zero(one, two, three, e, high, low, out):
    block = block_of()
    known = jnp.where(block == 1, one[...], jnp.where(block == 2, two[...], three[...]))
    term = times(known, high[...], low[...])
    out[...] = jnp.where(block == 0, e[...], jnp.where(block == 1, e[...] - term, term))


def after_one(first, second, e, high, low, out):
    block = block_of()
    known = jnp.where(block == 3, second[...], first[...])
    behind = jnp.where(block == 3, first[...], second[...])
    total = behind + times(known, high[...], low[...])
    out[...] = jnp.where(block == 0, e[...], jnp.where(block == 3, total, e[...] - total))


def turn(known, behind, e, kt_high, kt_low, high, low, settled, back):
    value = e[...] - behind[...] - times(known[...], kt_high[...], kt_low[...])
    settled[...] = value
    back[...] = times(value, high[...], low[...])


def back_two(into, near, far, t, s, high, low, settled, back, mixed):
    plane = lax.axis_index("pair")
    last = block_of() == 3
    passed = jnp.where(plane == 0, far[...], jnp.where(plane == 1, near[...], t[...]))
    value = jnp.where(last, passed, s[...] - into[...])
    product = times(value, high[...], low[...])
    settled[...] = value
    back[...] = product
    mixed[...] = jnp.where(last, product, value)


def back_one(into, other, t, s, high, low, settled, back):
    plane = lax.axis_index("pair")
    block = block_of()
    passed = jnp.where(plane == 0, other[...], t[...])
    value = jnp.where(
        block == 1,
        s[...] - into[...] - other[...],
        jnp.where(block == 2, passed, t[...]),
    )
    settled[...] = value
    product = times(value, high[...], low[...])
    back[...] = jnp.where(block == 2, product + into[...], product)


def collect(z0, z1, z2, z3, i0, i1, i2, i3, t, p1, p2, p3, out):
    plane = lax.axis_index("pair")
    block = block_of()

    def by_plane(a, b, c, d):
        return jnp.where(
            plane == 0, a[...], jnp.where(plane == 1, b[...], jnp.where(plane == 2, c[...], d[...]))
        )

    start = by_plane(z0, z1, z2, z3)
    zero = start - by_plane(i0, i1, i2, i3) - by_plane(i3, i0, i1, i2)
    one = by_plane(t, p1, p2, p3)
    two = by_plane(t, t, p1, p2)
    three = by_plane(t, t, t, p1)
    out[...] = jnp.where(
        block == 0, zero, jnp.where(block == 1, one, jnp.where(block == 2, two, three))
    )


def finish(own, mate, inv, out):
    value = jnp.where(side_of() == 0, own[...], mate[...])
    high, low = high_low(inv[...])
    out[...] = times(value, high, low, NT).astype(out.dtype)


def mm(a, b):
    return jnp.dot(a, b, precision=HIGHEST, preferred_element_type=F32)


def mm_t(a, b):
    return lax.dot_general(a, b, NT, precision=HIGHEST, preferred_element_type=F32)


def chip_solve(partial_fit, factor, diag_inv):
    count, height = partial_fit.shape
    size = 2 * height
    planes = lax.axis_size("pair")
    chips = [(k, plane) for k in range(SOLVE_BLOCKS) for plane in range(planes)]

    def device(chip, c):
        return (2 * chip[0] + c) * planes + chip[1]

    def permute(value, to):
        for chip in chips:
            for c in range(2):
                to.setdefault(device(chip, c), device(chip, 1 - c))
        return lax.ppermute(value, AXES, sorted(to.items()))

    def send(value, *moves):
        to = {}
        for source, target, *via in moves:
            loop = [device(source, 0), device(target, 0), device(target, 1)]
            for chip in via:
                loop += [device(chip, 0), device(chip, 1)]
            loop.append(device(source, 1))
            to.update(zip(loop, loop[1:] + loop[:1]))
        return permute(value, to)

    def swap(value):
        return lax.ppermute(value, "aux", [(i, i ^ 1) for i in range(2 * SOLVE_BLOCKS)])

    panel = struct((count, size))
    square = struct((size, size), BF16)
    k_high, k_low, kt_high, kt_low = call(
        prepare,
        [square] * 4,
        diag_inv,
        swap(diag_inv),
        factor,
        swap(factor),
        limit=32,
        scratch=[pltpu.VMEM((3 * size, size), BF16)] * 2,
    )
    home = [1] + list(range(SOLVE_BLOCKS - 1))
    gathered = []
    for step in reversed(range(1, planes)):
        to = {}
        for k in range(SOLVE_BLOCKS):
            for c in range(2):
                near = device((k, home[k]), c)
                far = device((k, (home[k] + step) % planes), c)
                to.update({near: far, far: near})
        gathered.append(permute(partial_fit, to))
    e = call(begin, panel, partial_fit, *gathered, diag_inv)
    e = call(both, panel, e, swap(e))
    reach = [send(e, ((0, 1), (k, 0))) for k in range(1, SOLVE_BLOCKS)]
    one = call(after_zero, panel, *reach, e, kt_high, kt_low)
    first = send(one, ((1, 0), (2, 1)), ((3, 0), (3, 1)), ((0, 1), (0, 0)))
    second = send(one, ((1, 0), (3, 1)), ((2, 0), (2, 1)), ((0, 1), (0, 2)))
    two = call(after_one, panel, first, second, e, kt_high, kt_low)
    behind = send(two, ((3, 1), (3, 2)), ((0, 1), (0, 3)))
    known = send(two, ((2, 1), (3, 2)))
    t, back = call(turn, [panel] * 2, known, behind, e, kt_high, kt_low, k_high, k_low)
    into = send(back, ((3, 2), (2, 1)))
    near = send(t, ((3, 2), (3, 1)))
    far = send(t, ((3, 2), (3, 0)))
    t, back, mixed = call(back_two, [panel] * 3, into, near, far, t, two, k_high, k_low)
    into = send(back, ((2, 1), (1, 0)), ((3, 0), (2, 0)))
    other = send(mixed, ((3, 1), (1, 0)), ((2, 1), (2, 0)))
    t, back = call(back_one, [panel] * 2, into, other, t, one, k_high, k_low)
    near = {
        ((1, 0), (0, 3)): (3, 0),
        ((1, 0), (0, 2)): (1, 1),
        ((2, 0), (0, 3)): (2, 1),
        ((2, 0), (0, 2)): (3, 1),
    }
    into = [None] * planes
    spread = [None] * planes
    for plane in reversed(range(planes)):
        moves = [((1, 0), (0, plane)), ((2, 0), (0, (plane + 1) % planes))]
        into[plane] = send(
            back, *((*move, near[move]) if move in near else move for move in moves)
        )
    for step in reversed(range(1, planes)):
        moves = [((1, 0), (1, step))]
        if 1 + step < planes:
            moves.append(((2, 1), (2, 1 + step)))
        if 2 + step < planes:
            moves.append(((3, 2), (3, 2 + step)))
        spread[step] = send(t, *moves)
    t = call(collect, panel, first, e, second, behind, *into, t, *spread[1:])
    return call(finish, struct((count, height), BF16), t, swap(t), diag_inv)


def chain_solve(partial_fit, factor, diag_inv):
    count, height = partial_fit.shape
    breadth = factor.shape[1]
    block_size = diag_inv.shape[1]
    rows_aux = lax.axis_size("aux")
    total = height * rows_aux
    members = rows_aux // SOLVE_BLOCKS
    my_row = lax.axis_index("aux")
    my_column = lax.axis_index("pair")
    my_block = my_row // members
    column_block = (my_column * breadth + jnp.arange(breadth, dtype=jnp.int32)) // block_size
    factor_low = jnp.where((column_block < my_block)[None, :], factor, 0.0)

    def own_columns(whole):
        return lax.dynamic_slice_in_dim(whole, my_column * breadth, breadth, 1)

    zero_block = jnp.zeros((count, block_size), jnp.float32)
    solved = jnp.zeros((count, total), jnp.float32)
    for k in range(SOLVE_BLOCKS):

        def on_group(current):
            return mm(partial_fit - mm_t(own_columns(current), factor_low), diag_inv)

        def off_group(current):
            return zero_block

        summand = lax.cond(my_block == k, on_group, off_group, solved)
        arrived = lax.psum(summand, AXES)
        solved = lax.dynamic_update_slice_in_dim(solved, arrived, k * block_size, 1)
    own_coef = jnp.zeros((count, height), jnp.float32)
    contrib = jnp.zeros((count, total), jnp.float32)
    for target in reversed(range(SOLVE_BLOCKS)):
        settled = solved[:, target * block_size : (target + 1) * block_size]
        if target < SOLVE_BLOCKS - 1:
            portion = contrib[:, target * block_size : (target + 1) * block_size]
            settled = settled - lax.psum(portion, AXES)

        def on_group(state):
            coef = mm_t(settled, diag_inv)
            if target > 0:
                fresh = lax.dynamic_update_slice_in_dim(
                    jnp.zeros((count, total), jnp.float32),
                    mm(coef, factor_low),
                    my_column * breadth,
                    1,
                )
            else:
                fresh = state[1]
            return (coef, fresh)

        def keep_state(state):
            return state

        own_coef, contrib = lax.cond(my_block == target, on_group, keep_state, (own_coef, contrib))
    return own_coef.astype(jnp.bfloat16)


def shards(integrals, densities, screen, factor, diag_inv):
    block_size = diag_inv.shape[1]
    chip_blocks = (
        lax.axis_size("aux") == 2 * SOLVE_BLOCKS
        and factor.shape[1] == block_size
        and lax.axis_size("pair") == SOLVE_BLOCKS
    )
    solve = chip_solve if chip_blocks else chain_solve
    left, right, partial_fit = fit_partial(densities, integrals, screen)
    rounded = solve(partial_fit, factor, diag_inv)
    return scatter_sum(coulomb_partial(rounded, left, right, screen))


def solution(mesh):
    in_specs = (
        P("aux", "pair"),
        P(None, "pair"),
        P("aux", "pair"),
        P("aux", "pair"),
        P("aux", None),
    )
    out_specs = P(None, ("pair", "aux"))
    return jax.shard_map(shards, mesh=mesh, in_specs=in_specs, out_specs=out_specs, check_vma=False)
```

```python
import jax
import jax.numpy as jnp
from jax import lax
from jax.experimental import pallas as pl
from jax.experimental.pallas import tpu as pltpu
from jax.sharding import PartitionSpec as P

TILE = 128
SOLVE_BLOCKS = 4
AXES = ("aux", "pair")
HIGHEST = lax.Precision.HIGHEST
F32 = jnp.float32
BF16 = jnp.bfloat16
VMEM = pl.BlockSpec(memory_space=pltpu.VMEM)
SMEM = pl.BlockSpec(memory_space=pltpu.SMEM)
HBM = pl.BlockSpec(memory_space=pltpu.HBM)
MIB = 1024 * 1024
NN = (((1,), (0,)), ((), ()))
NT = (((1,), (1,)), ((), ()))
TN = (((0,), (0,)), ((), ()))


def struct(shape, dtype=F32):
    return jax.ShapeDtypeStruct(shape, dtype)


def call(kernel, outs, *operands, limit=12, specs=None, scratch=()):
    return pl.pallas_call(
        kernel,
        out_shape=outs,
        in_specs=specs or [VMEM] * len(operands),
        out_specs=jax.tree.map(lambda _: VMEM, outs),
        scratch_shapes=scratch,
        compiler_params=pltpu.CompilerParams(vmem_limit_bytes=limit * MIB),
    )(*operands)


def side_of():
    return lax.rem(lax.axis_index("aux"), 2)


def block_of():
    return lax.div(lax.axis_index("aux"), 2)


def masked_row(screen, densities, i, tiles):
    zero = jnp.zeros((), densities.dtype)
    return jnp.concatenate(
        [
            jnp.where(screen[i, t] != 0, densities[:, t * TILE : (t + 1) * TILE], zero)
            for t in tiles
        ],
        axis=1,
    )


def fit(
    screen_in, densities_in, integrals, left, right, out, screen, densities, total, arrived
):
    height, width = integrals.shape
    pieces = arrived.shape[0] - 2
    chunk = width // pieces
    small = [
        pltpu.make_async_copy(screen_in, screen, arrived.at[pieces]),
        pltpu.make_async_copy(densities_in, densities, arrived.at[pieces + 1]),
    ]
    copies = []
    held = []
    for j in range(pieces):
        ref = left if 2 * j < pieces else right
        start = j * chunk if ref is left else j * chunk - width // 2
        held.append(ref.at[:, start : start + chunk])
        copies.append(
            pltpu.make_async_copy(
                integrals.at[:, j * chunk : (j + 1) * chunk], held[j], arrived.at[j]
            )
        )
    for copy in small + copies:
        copy.start()
    total[...] = jnp.zeros_like(total)
    for copy in small:
        copy.wait()
    count = densities.shape[0]
    strips = height // TILE
    for j in range(pieces):
        tiles = range(j * chunk // TILE, (j + 1) * chunk // TILE)
        stacked = jnp.concatenate([masked_row(screen, densities, i, tiles) for i in range(strips)])
        copies[j].wait()
        total[...] += lax.dot_general(held[j][...], stacked, NT, preferred_element_type=F32)
    done = total[...].T
    for i in range(strips):
        out[:, i * TILE : (i + 1) * TILE] = done[
            i * count : (i + 1) * count, i * TILE : (i + 1) * TILE
        ]


def fit_partial(densities, integrals, screen):
    count = densities.shape[0]
    height, width = integrals.shape
    pieces = 8 if width % (8 * TILE) == 0 else width // TILE
    return call(
        fit,
        [struct((height, width // 2), BF16)] * 2 + [struct((count, height))],
        *(pltpu.with_memory_space_constraint(x, pltpu.HBM) for x in (screen, densities, integrals)),
        specs=[HBM] * 3,
        scratch=[
            pltpu.SMEM(screen.shape, jnp.int32),
            pltpu.VMEM(densities.shape, BF16),
            pltpu.VMEM((height, height // TILE * count), F32),
            pltpu.SemaphoreType.DMA((pieces + 2,)),
        ],
    )


def coulomb(screen, rounded, left, right, out):
    members, count, chunk = out.shape
    height, width = left.shape
    strips = height // TILE
    value = rounded[...]
    strip_of = lax.broadcasted_iota(jnp.int32, value.shape, 1) // TILE
    stacked = jnp.concatenate(
        [jnp.where(strip_of == i, value, jnp.zeros((), BF16)) for i in range(strips)]
    )
    for m in range(members):
        held = left if m * chunk < width else right
        start = m * chunk if held is left else m * chunk - width
        parts = jnp.dot(stacked, held[:, start : start + chunk], preferred_element_type=F32)
        for t in range(chunk // TILE):
            lanes = slice(t * TILE, (t + 1) * TILE)
            total = jnp.zeros((count, TILE), F32)
            for i in range(strips):
                part = parts[i * count : (i + 1) * count, lanes]
                total += jnp.where(screen[i, m * chunk // TILE + t] != 0, part, 0.0)
            out[m, :, lanes] = total.astype(out.dtype)


def coulomb_partial(rounded, left, right, screen):
    members = lax.axis_size("aux")
    out = struct((members, rounded.shape[0], 2 * left.shape[1] // members), BF16)
    return call(coulomb, out, screen, rounded, left, right, specs=[SMEM, VMEM, VMEM, VMEM])


def scatter_sum(slabs):
    arrived = lax.all_to_all(slabs, "aux", 0, 0, tiled=True)
    return jnp.sum(arrived.astype(F32), axis=0)


def high_low(value):
    high = value.astype(BF16)
    return high, (value - high.astype(F32)).astype(BF16)


def times(value, high, low, dims=NN):
    rows = value.shape[0]
    coarse = value.astype(BF16).astype(F32)
    pair = jnp.concatenate([coarse, value - coarse], axis=0).astype(BF16)
    both = lax.dot_general(pair, high, dims, preferred_element_type=F32)
    both += lax.dot_general(pair, low, dims, preferred_element_type=F32)
    return both[:rows] + both[rows:]


def prepare(inv0, inv1, fac0, fac1, k_high, k_low, kt_high, kt_low, lhs, rhs):
    height = inv0.shape[0]

    @pl.when((block_of() > 0) & (side_of() == 0))
    def _():
        for n, (inv, fac) in enumerate(((inv0, fac0), (inv1, fac1))):
            rows = [slice((3 * n + r) * height, (3 * n + r + 1) * height) for r in range(3)]
            high, low = high_low(inv[...])
            lhs[rows[0], :], lhs[rows[1], :], lhs[rows[2], :] = high, low, high
            high, low = high_low(fac[...])
            rhs[rows[0], :], rhs[rows[1], :], rhs[rows[2], :] = high, high, low
        depth = 3 * height
        halves = (
            (slice(0, height), slice(0, depth)),
            (slice(height, 2 * height), slice(0, 2 * depth)),
        )
        for part, used in halves:
            product = lax.dot_general(lhs[used, part], rhs[used, :], TN, preferred_element_type=F32)
            k_high[part, :], k_low[part, :] = high_low(product)
            kt_high[:, part], kt_low[:, part] = high_low(product.T)


def begin(f0, f1, f2, f3, inv, out):
    high, low = high_low(inv[...])
    out[...] = times(f0[...] + f1[...] + f2[...] + f3[...], high, low)


def begin_late(f0, f1, f2, f3, inv, after, out):
    begin(f0, f1, f2, f3, inv, out)


def both(own, mate, out):
    out[...] = own[...] + mate[...]


def both_late(zero, own, mate, out):
    out[...] = jnp.where(block_of() == 0, zero[...], own[...] + mate[...])


def after_zero(one, two, three, e, high, low, out):
    block = block_of()
    known = jnp.where(block == 1, one[...], jnp.where(block == 2, two[...], three[...]))
    term = times(known, high[...], low[...])
    out[...] = jnp.where(block == 0, e[...], jnp.where(block == 1, e[...] - term, term))


def after_one(first, second, e, high, low, out):
    block = block_of()
    known = jnp.where(block == 3, second[...], first[...])
    behind = jnp.where(block == 3, first[...], second[...])
    total = behind + times(known, high[...], low[...])
    out[...] = jnp.where(block == 0, e[...], jnp.where(block == 3, total, e[...] - total))


def turn(known, behind, e, kt_high, kt_low, high, low, settled, back):
    value = e[...] - behind[...] - times(known[...], kt_high[...], kt_low[...])
    settled[...] = value
    back[...] = times(value, high[...], low[...])


def back_two(into, near, far, t, s, high, low, settled, back, mixed):
    plane = lax.axis_index("pair")
    last = block_of() == 3
    passed = jnp.where(plane == 0, far[...], jnp.where(plane == 1, near[...], t[...]))
    value = jnp.where(last, passed, s[...] - into[...])
    product = times(value, high[...], low[...])
    settled[...] = value
    back[...] = product
    mixed[...] = jnp.where(last, product, value)


def back_one(into, other, t, s, high, low, settled, back):
    plane = lax.axis_index("pair")
    block = block_of()
    passed = jnp.where(plane == 0, other[...], t[...])
    value = jnp.where(
        block == 1,
        s[...] - into[...] - other[...],
        jnp.where(block == 2, passed, t[...]),
    )
    settled[...] = value
    product = times(value, high[...], low[...])
    back[...] = jnp.where(block == 2, product + into[...], product)


def collect(z0, z1, z2, z3, i0, i1, i2, i3, t, p1, p2, p3, out):
    plane = lax.axis_index("pair")
    block = block_of()

    def by_plane(a, b, c, d):
        return jnp.where(
            plane == 0, a[...], jnp.where(plane == 1, b[...], jnp.where(plane == 2, c[...], d[...]))
        )

    start = by_plane(z0, z1, z2, z3)
    zero = start - by_plane(i0, i1, i2, i3) - by_plane(i3, i0, i1, i2)
    one = by_plane(t, p1, p2, p3)
    two = by_plane(t, t, p1, p2)
    three = by_plane(t, t, t, p1)
    out[...] = jnp.where(
        block == 0, zero, jnp.where(block == 1, one, jnp.where(block == 2, two, three))
    )


def finish(own, mate, inv, out):
    value = jnp.where(side_of() == 0, own[...], mate[...])
    high, low = high_low(inv[...])
    out[...] = times(value, high, low, NT).astype(out.dtype)


def mm(a, b):
    return jnp.dot(a, b, precision=HIGHEST, preferred_element_type=F32)


def mm_t(a, b):
    return lax.dot_general(a, b, NT, precision=HIGHEST, preferred_element_type=F32)


def chip_solve(partial_fit, factor, diag_inv):
    count, height = partial_fit.shape
    size = 2 * height
    planes = lax.axis_size("pair")
    chips = [(k, plane) for k in range(SOLVE_BLOCKS) for plane in range(planes)]

    def device(chip, c):
        return (2 * chip[0] + c) * planes + chip[1]

    def permute(value, to):
        for chip in chips:
            for c in range(2):
                to.setdefault(device(chip, c), device(chip, 1 - c))
        return lax.ppermute(value, AXES, sorted(to.items()))

    def send(value, *moves):
        to = {}
        for source, target, *via in moves:
            loop = [device(source, 0), device(target, 0), device(target, 1)]
            for chip in via:
                loop += [device(chip, 0), device(chip, 1)]
            loop.append(device(source, 1))
            to.update(zip(loop, loop[1:] + loop[:1]))
        return permute(value, to)

    def swap(value):
        return lax.ppermute(value, "aux", [(i, i ^ 1) for i in range(2 * SOLVE_BLOCKS)])

    def gather(blocks):
        gathered = []
        for step in reversed(range(1, planes)):
            to = {}
            for k in blocks:
                for c in range(2):
                    near = device((k, home[k]), c)
                    far = device((k, (home[k] + step) % planes), c)
                    to.update({near: far, far: near})
            gathered.append(permute(partial_fit, to))
        return gathered

    panel = struct((count, size))
    square = struct((size, size), BF16)
    diag_late, factor_late, partial_fit = lax.optimization_barrier((diag_inv, factor, partial_fit))
    inv_other = permute(diag_late, {})
    fac_other = permute(factor_late, {})
    home = [1] + list(range(SOLVE_BLOCKS - 1))
    gathered = gather([0])
    gathered_late = gather(range(1, SOLVE_BLOCKS))
    e = call(begin, panel, partial_fit, *gathered, diag_inv)
    e = call(both, panel, e, swap(e))
    reach = [send(e, ((0, 1), (k, 0))) for k in range(1, SOLVE_BLOCKS)]
    k_high, k_low, kt_high, kt_low = call(
        prepare,
        [square] * 4,
        diag_inv,
        inv_other,
        factor,
        fac_other,
        limit=32,
        scratch=[pltpu.VMEM((3 * size, size), BF16)] * 2,
    )
    e_late = call(begin_late, panel, partial_fit, *gathered_late, diag_inv, k_high)
    e = call(both_late, panel, e, e_late, swap(e_late))
    one = call(after_zero, panel, *reach, e, kt_high, kt_low)
    first = send(one, ((1, 0), (2, 1)), ((3, 0), (3, 1)), ((0, 1), (0, 0)))
    second = send(one, ((1, 0), (3, 1)), ((2, 0), (2, 1)), ((0, 1), (0, 2)))
    two = call(after_one, panel, first, second, e, kt_high, kt_low)
    behind = send(two, ((3, 1), (3, 2)), ((0, 1), (0, 3)))
    known = send(two, ((2, 1), (3, 2)))
    t, back = call(turn, [panel] * 2, known, behind, e, kt_high, kt_low, k_high, k_low)
    into = send(back, ((3, 2), (2, 1)))
    near = send(t, ((3, 2), (3, 1)))
    far = send(t, ((3, 2), (3, 0)))
    t, back, mixed = call(back_two, [panel] * 3, into, near, far, t, two, k_high, k_low)
    into = send(back, ((2, 1), (1, 0)), ((3, 0), (2, 0)))
    other = send(mixed, ((3, 1), (1, 0)), ((2, 1), (2, 0)))
    t, back = call(back_one, [panel] * 2, into, other, t, one, k_high, k_low)
    near = {
        ((1, 0), (0, 3)): (3, 0),
        ((1, 0), (0, 2)): (1, 1),
        ((2, 0), (0, 3)): (2, 1),
        ((2, 0), (0, 2)): (3, 1),
    }
    into = [None] * planes
    spread = [None] * planes
    for plane in reversed(range(planes)):
        moves = [((1, 0), (0, plane)), ((2, 0), (0, (plane + 1) % planes))]
        into[plane] = send(
            back, *((*move, near[move]) if move in near else move for move in moves)
        )
    for step in reversed(range(1, planes)):
        moves = [((1, 0), (1, step))]
        if 1 + step < planes:
            moves.append(((2, 1), (2, 1 + step)))
        if 2 + step < planes:
            moves.append(((3, 2), (3, 2 + step)))
        spread[step] = send(t, *moves)
    t = call(collect, panel, first, e, second, behind, *into, t, *spread[1:])
    return call(finish, struct((count, height), BF16), t, swap(t), diag_inv)


def chain_solve(partial_fit, factor, diag_inv):
    count, height = partial_fit.shape
    breadth = factor.shape[1]
    block_size = diag_inv.shape[1]
    rows_aux = lax.axis_size("aux")
    total = height * rows_aux
    members = rows_aux // SOLVE_BLOCKS
    my_row = lax.axis_index("aux")
    my_column = lax.axis_index("pair")
    my_block = my_row // members
    column_block = (my_column * breadth + jnp.arange(breadth, dtype=jnp.int32)) // block_size
    factor_low = jnp.where((column_block < my_block)[None, :], factor, 0.0)

    def own_columns(whole):
        return lax.dynamic_slice_in_dim(whole, my_column * breadth, breadth, 1)

    zero_block = jnp.zeros((count, block_size), jnp.float32)
    solved = jnp.zeros((count, total), jnp.float32)
    for k in range(SOLVE_BLOCKS):

        def on_group(current):
            return mm(partial_fit - mm_t(own_columns(current), factor_low), diag_inv)

        def off_group(current):
            return zero_block

        summand = lax.cond(my_block == k, on_group, off_group, solved)
        arrived = lax.psum(summand, AXES)
        solved = lax.dynamic_update_slice_in_dim(solved, arrived, k * block_size, 1)
    own_coef = jnp.zeros((count, height), jnp.float32)
    contrib = jnp.zeros((count, total), jnp.float32)
    for target in reversed(range(SOLVE_BLOCKS)):
        settled = solved[:, target * block_size : (target + 1) * block_size]
        if target < SOLVE_BLOCKS - 1:
            portion = contrib[:, target * block_size : (target + 1) * block_size]
            settled = settled - lax.psum(portion, AXES)

        def on_group(state):
            coef = mm_t(settled, diag_inv)
            if target > 0:
                fresh = lax.dynamic_update_slice_in_dim(
                    jnp.zeros((count, total), jnp.float32),
                    mm(coef, factor_low),
                    my_column * breadth,
                    1,
                )
            else:
                fresh = state[1]
            return (coef, fresh)

        def keep_state(state):
            return state

        own_coef, contrib = lax.cond(my_block == target, on_group, keep_state, (own_coef, contrib))
    return own_coef.astype(jnp.bfloat16)


def shards(integrals, densities, screen, factor, diag_inv):
    block_size = diag_inv.shape[1]
    chip_blocks = (
        lax.axis_size("aux") == 2 * SOLVE_BLOCKS
        and factor.shape[1] == block_size
        and lax.axis_size("pair") == SOLVE_BLOCKS
    )
    solve = chip_solve if chip_blocks else chain_solve
    left, right, partial_fit = fit_partial(densities, integrals, screen)
    rounded = solve(partial_fit, factor, diag_inv)
    return scatter_sum(coulomb_partial(rounded, left, right, screen))


def solution(mesh):
    in_specs = (
        P("aux", "pair"),
        P(None, "pair"),
        P("aux", "pair"),
        P("aux", "pair"),
        P("aux", None),
    )
    out_specs = P(None, ("pair", "aux"))
    return jax.shard_map(shards, mesh=mesh, in_specs=in_specs, out_specs=out_specs, check_vma=False)
```

```python
import jax
import jax.numpy as jnp
from jax import lax
from jax.experimental import pallas as pl
from jax.experimental.pallas import tpu as pltpu
from jax.sharding import PartitionSpec as P

TILE = 128
SOLVE_BLOCKS = 4
LEAD = 1
AXES = ("aux", "pair")
HIGHEST = lax.Precision.HIGHEST
F32 = jnp.float32
BF16 = jnp.bfloat16
VMEM = pl.BlockSpec(memory_space=pltpu.VMEM)
SMEM = pl.BlockSpec(memory_space=pltpu.SMEM)
HBM = pl.BlockSpec(memory_space=pltpu.HBM)
MIB = 1024 * 1024
NN = (((1,), (0,)), ((), ()))
NT = (((1,), (1,)), ((), ()))
TN = (((0,), (0,)), ((), ()))


def struct(shape, dtype=F32):
    return jax.ShapeDtypeStruct(shape, dtype)


def call(kernel, outs, *operands, limit=12, specs=None, scratch=()):
    return pl.pallas_call(
        kernel,
        out_shape=outs,
        in_specs=specs or [VMEM] * len(operands),
        out_specs=jax.tree.map(lambda _: VMEM, outs),
        scratch_shapes=scratch,
        compiler_params=pltpu.CompilerParams(vmem_limit_bytes=limit * MIB),
    )(*operands)


def side_of():
    return lax.rem(lax.axis_index("aux"), 2)


def block_of():
    return lax.div(lax.axis_index("aux"), 2)


def masked_row(screen, densities, i, tiles):
    zero = jnp.zeros((), densities.dtype)
    return jnp.concatenate(
        [
            jnp.where(screen[i, t] != 0, densities[:, t * TILE : (t + 1) * TILE], zero)
            for t in tiles
        ],
        axis=1,
    )


def fit(
    screen_in, densities_in, integrals, left, right, out, screen, densities, total, arrived
):
    height, width = integrals.shape
    pieces = arrived.shape[0] - 2
    chunk = width // pieces
    small = [
        pltpu.make_async_copy(screen_in, screen, arrived.at[pieces]),
        pltpu.make_async_copy(densities_in, densities, arrived.at[pieces + 1]),
    ]
    copies = []
    held = []
    for j in range(pieces):
        ref = left if 2 * j < pieces else right
        start = j * chunk if ref is left else j * chunk - width // 2
        held.append(ref.at[:, start : start + chunk])
        copies.append(
            pltpu.make_async_copy(
                integrals.at[:, j * chunk : (j + 1) * chunk], held[j], arrived.at[j]
            )
        )
    for copy in small + copies:
        copy.start()
    total[...] = jnp.zeros_like(total)
    for copy in small:
        copy.wait()
    count = densities.shape[0]
    strips = height // TILE
    for j in range(pieces):
        tiles = range(j * chunk // TILE, (j + 1) * chunk // TILE)
        stacked = jnp.concatenate([masked_row(screen, densities, i, tiles) for i in range(strips)])
        copies[j].wait()
        total[...] += lax.dot_general(held[j][...], stacked, NT, preferred_element_type=F32)
    done = total[...].T
    for i in range(strips):
        out[:, i * TILE : (i + 1) * TILE] = done[
            i * count : (i + 1) * count, i * TILE : (i + 1) * TILE
        ]


def fit_partial(densities, integrals, screen):
    count = densities.shape[0]
    height, width = integrals.shape
    pieces = 8 if width % (8 * TILE) == 0 else width // TILE
    return call(
        fit,
        [struct((height, width // 2), BF16)] * 2 + [struct((count, height))],
        *(pltpu.with_memory_space_constraint(x, pltpu.HBM) for x in (screen, densities, integrals)),
        specs=[HBM] * 3,
        scratch=[
            pltpu.SMEM(screen.shape, jnp.int32),
            pltpu.VMEM(densities.shape, BF16),
            pltpu.VMEM((height, height // TILE * count), F32),
            pltpu.SemaphoreType.DMA((pieces + 2,)),
        ],
    )


def coulomb(screen, rounded, left, right, out):
    members, count, chunk = out.shape
    height, width = left.shape
    strips = height // TILE
    value = rounded[...]
    strip_of = lax.broadcasted_iota(jnp.int32, value.shape, 1) // TILE
    stacked = jnp.concatenate(
        [jnp.where(strip_of == i, value, jnp.zeros((), BF16)) for i in range(strips)]
    )
    for m in range(members):
        held = left if m * chunk < width else right
        start = m * chunk if held is left else m * chunk - width
        parts = jnp.dot(stacked, held[:, start : start + chunk], preferred_element_type=F32)
        for t in range(chunk // TILE):
            lanes = slice(t * TILE, (t + 1) * TILE)
            total = jnp.zeros((count, TILE), F32)
            for i in range(strips):
                part = parts[i * count : (i + 1) * count, lanes]
                total += jnp.where(screen[i, m * chunk // TILE + t] != 0, part, 0.0)
            out[m, :, lanes] = total.astype(out.dtype)


def coulomb_partial(rounded, left, right, screen):
    members = lax.axis_size("aux")
    out = struct((members, rounded.shape[0], 2 * left.shape[1] // members), BF16)
    return call(coulomb, out, screen, rounded, left, right, specs=[SMEM, VMEM, VMEM, VMEM])


def scatter_sum(slabs):
    arrived = lax.all_to_all(slabs, "aux", 0, 0, tiled=True)
    return jnp.sum(arrived.astype(F32), axis=0)


def high_low(value):
    high = value.astype(BF16)
    return high, (value - high.astype(F32)).astype(BF16)


def times(value, high, low, dims=NN):
    rows = value.shape[0]
    coarse = value.astype(BF16).astype(F32)
    pair = jnp.concatenate([coarse, value - coarse], axis=0).astype(BF16)
    both = lax.dot_general(pair, high, dims, preferred_element_type=F32)
    both += lax.dot_general(pair, low, dims, preferred_element_type=F32)
    return both[:rows] + both[rows:]


def prepare(inv_own, inv_mate, fac_own, fac_mate, k_high, k_low, kt_high, kt_low, lhs, rhs):
    height = inv_own.shape[0]
    halves = [(inv_own, fac_own), (inv_mate, fac_mate)]
    if LEAD == 1:
        halves.reverse()

    @pl.when((block_of() > 0) & (side_of() == LEAD))
    def _():
        for n, (inv, fac) in enumerate(halves):
            rows = [slice((3 * n + r) * height, (3 * n + r + 1) * height) for r in range(3)]
            high, low = high_low(inv[...])
            lhs[rows[0], :], lhs[rows[1], :], lhs[rows[2], :] = high, low, high
            high, low = high_low(fac[...])
            rhs[rows[0], :], rhs[rows[1], :], rhs[rows[2], :] = high, high, low
        depth = 3 * height
        parts = (
            (slice(0, height), slice(0, depth)),
            (slice(height, 2 * height), slice(0, 2 * depth)),
        )
        for part, used in parts:
            product = lax.dot_general(lhs[used, part], rhs[used, :], TN, preferred_element_type=F32)
            k_high[part, :], k_low[part, :] = high_low(product)
            kt_high[:, part], kt_low[:, part] = high_low(product.T)


def begin(f0, f1, f2, f3, inv, after, out):
    begin_late(f0, f1, f2, f3, inv, out)


def begin_late(f0, f1, f2, f3, inv, out):
    high, low = high_low(inv[...])
    out[...] = times(f0[...] + f1[...] + f2[...] + f3[...], high, low)


def both(own, mate, out):
    out[...] = own[...] + mate[...]


def both_late(zero, own, mate, out):
    out[...] = jnp.where(block_of() == 0, zero[...], own[...] + mate[...])


def after_zero(one, two, three, e, high, low, out):
    block = block_of()
    known = jnp.where(block == 1, one[...], jnp.where(block == 2, two[...], three[...]))
    term = times(known, high[...], low[...])
    out[...] = jnp.where(block == 0, e[...], jnp.where(block == 1, e[...] - term, term))


def after_one(first, second, e, high, low, out):
    block = block_of()
    known = jnp.where(block == 3, second[...], first[...])
    behind = jnp.where(block == 3, first[...], second[...])
    total = behind + times(known, high[...], low[...])
    out[...] = jnp.where(block == 0, e[...], jnp.where(block == 3, total, e[...] - total))


def turn(known, behind, e, kt_high, kt_low, high, low, settled, back):
    value = e[...] - behind[...] - times(known[...], kt_high[...], kt_low[...])
    settled[...] = value
    back[...] = times(value, high[...], low[...])


def back_two(into, near, far, t, s, high, low, settled, back, mixed):
    plane = lax.axis_index("pair")
    last = block_of() == 3
    passed = jnp.where(plane == 0, far[...], jnp.where(plane == 1, near[...], t[...]))
    value = jnp.where(last, passed, s[...] - into[...])
    product = times(value, high[...], low[...])
    settled[...] = value
    back[...] = product
    mixed[...] = jnp.where(last, product, value)


def back_one(into, other, t, s, high, low, settled, back):
    plane = lax.axis_index("pair")
    block = block_of()
    passed = jnp.where(plane == 0, other[...], t[...])
    value = jnp.where(
        block == 1,
        s[...] - into[...] - other[...],
        jnp.where(block == 2, passed, t[...]),
    )
    settled[...] = value
    product = times(value, high[...], low[...])
    back[...] = jnp.where(block == 2, product + into[...], product)


def collect(z0, z1, z2, z3, i0, i1, i2, i3, t, p1, p2, p3, out):
    plane = lax.axis_index("pair")
    block = block_of()

    def by_plane(a, b, c, d):
        return jnp.where(
            plane == 0, a[...], jnp.where(plane == 1, b[...], jnp.where(plane == 2, c[...], d[...]))
        )

    start = by_plane(z0, z1, z2, z3)
    zero = start - by_plane(i0, i1, i2, i3) - by_plane(i3, i0, i1, i2)
    one = by_plane(t, p1, p2, p3)
    two = by_plane(t, t, p1, p2)
    three = by_plane(t, t, t, p1)
    out[...] = jnp.where(
        block == 0, zero, jnp.where(block == 1, one, jnp.where(block == 2, two, three))
    )


def finish(own, mate, inv, out):
    value = jnp.where(side_of() == LEAD, own[...], mate[...])
    high, low = high_low(inv[...])
    out[...] = times(value, high, low, NT).astype(out.dtype)


def mm(a, b):
    return jnp.dot(a, b, precision=HIGHEST, preferred_element_type=F32)


def mm_t(a, b):
    return lax.dot_general(a, b, NT, precision=HIGHEST, preferred_element_type=F32)


def chip_solve(partial_fit, factor, diag_inv):
    count, height = partial_fit.shape
    size = 2 * height
    planes = lax.axis_size("pair")
    chips = [(k, plane) for k in range(SOLVE_BLOCKS) for plane in range(planes)]

    def device(chip, c):
        return (2 * chip[0] + c) * planes + chip[1]

    def permute(value, to):
        for chip in chips:
            for c in range(2):
                to.setdefault(device(chip, c), device(chip, 1 - c))
        return lax.ppermute(value, AXES, sorted(to.items()))

    def send(value, *moves):
        to = {}
        for source, target, *via in moves:
            loop = [device(source, LEAD), device(target, LEAD), device(target, 1 - LEAD)]
            for chip in via:
                loop += [device(chip, LEAD), device(chip, 1 - LEAD)]
            loop.append(device(source, 1 - LEAD))
            to.update(zip(loop, loop[1:] + loop[:1]))
        return permute(value, to)

    def swap(value):
        return lax.ppermute(value, "aux", [(i, i ^ 1) for i in range(2 * SOLVE_BLOCKS)])

    def gather(blocks, near):
        gathered = []
        for index, step in enumerate(reversed(range(1, planes))):
            to = {}
            for k in blocks:
                for c in range(2):
                    loop = [device((k, (home[k] + step) % planes), c), device((k, home[k]), c)]
                    if k in near:
                        loop.append(device(near[k][index], c))
                    to.update(zip(loop, loop[1:] + loop[:1]))
            gathered.append(permute(partial_fit, to))
        return gathered

    panel = struct((count, size))
    square = struct((size, size), BF16)
    inv_other = swap(diag_inv)
    fac_other = swap(factor)
    home = [1] + list(range(SOLVE_BLOCKS - 1))
    gathered = gather([0], {0: [(1, 1), (2, 1), (3, 1)]})
    gathered_late = gather(range(1, SOLVE_BLOCKS), {1: [(0, 0), (0, 2), (0, 3)]})
    k_high, k_low, kt_high, kt_low = call(
        prepare,
        [square] * 4,
        diag_inv,
        inv_other,
        factor,
        fac_other,
        limit=32,
        scratch=[pltpu.VMEM((3 * size, size), BF16)] * 2,
    )
    e = call(begin, panel, partial_fit, *gathered, diag_inv, k_high)
    e = call(both, panel, e, swap(e))
    reach = [send(e, ((0, 1), (k, 0))) for k in range(1, SOLVE_BLOCKS)]
    e_late = call(begin_late, panel, partial_fit, *gathered_late, diag_inv)
    e = call(both_late, panel, e, e_late, swap(e_late))
    one = call(after_zero, panel, *reach, e, kt_high, kt_low)
    first = send(one, ((1, 0), (2, 1)), ((3, 0), (3, 1)), ((0, 1), (0, 0)))
    second = send(one, ((1, 0), (3, 1)), ((2, 0), (2, 1)), ((0, 1), (0, 2)))
    two = call(after_one, panel, first, second, e, kt_high, kt_low)
    behind = send(two, ((3, 1), (3, 2)), ((0, 1), (0, 3)))
    known = send(two, ((2, 1), (3, 2)))
    t, back = call(turn, [panel] * 2, known, behind, e, kt_high, kt_low, k_high, k_low)
    into = send(back, ((3, 2), (2, 1)))
    near = send(t, ((3, 2), (3, 1)))
    far = send(t, ((3, 2), (3, 0)))
    t, back, mixed = call(back_two, [panel] * 3, into, near, far, t, two, k_high, k_low)
    into = send(back, ((2, 1), (1, 0)), ((3, 0), (2, 0)))
    other = send(mixed, ((3, 1), (1, 0)), ((2, 1), (2, 0)))
    t, back = call(back_one, [panel] * 2, into, other, t, one, k_high, k_low)
    near = {
        ((1, 0), (0, 3)): (3, 0),
        ((1, 0), (0, 2)): (1, 1),
        ((2, 0), (0, 3)): (2, 1),
        ((2, 0), (0, 2)): (3, 1),
    }
    into = [None] * planes
    spread = [None] * planes
    for plane in reversed(range(planes)):
        moves = [((1, 0), (0, plane)), ((2, 0), (0, (plane + 1) % planes))]
        into[plane] = send(
            back, *((*move, near[move]) if move in near else move for move in moves)
        )
    for step in reversed(range(1, planes)):
        moves = [((1, 0), (1, step))]
        if 1 + step < planes:
            moves.append(((2, 1), (2, 1 + step)))
        if 2 + step < planes:
            moves.append(((3, 2), (3, 2 + step)))
        spread[step] = send(t, *moves)
    t = call(collect, panel, first, e, second, behind, *into, t, *spread[1:])
    return call(finish, struct((count, height), BF16), t, swap(t), diag_inv)


def chain_solve(partial_fit, factor, diag_inv):
    count, height = partial_fit.shape
    breadth = factor.shape[1]
    block_size = diag_inv.shape[1]
    rows_aux = lax.axis_size("aux")
    total = height * rows_aux
    members = rows_aux // SOLVE_BLOCKS
    my_row = lax.axis_index("aux")
    my_column = lax.axis_index("pair")
    my_block = my_row // members
    column_block = (my_column * breadth + jnp.arange(breadth, dtype=jnp.int32)) // block_size
    factor_low = jnp.where((column_block < my_block)[None, :], factor, 0.0)

    def own_columns(whole):
        return lax.dynamic_slice_in_dim(whole, my_column * breadth, breadth, 1)

    zero_block = jnp.zeros((count, block_size), jnp.float32)
    solved = jnp.zeros((count, total), jnp.float32)
    for k in range(SOLVE_BLOCKS):

        def on_group(current):
            return mm(partial_fit - mm_t(own_columns(current), factor_low), diag_inv)

        def off_group(current):
            return zero_block

        summand = lax.cond(my_block == k, on_group, off_group, solved)
        arrived = lax.psum(summand, AXES)
        solved = lax.dynamic_update_slice_in_dim(solved, arrived, k * block_size, 1)
    own_coef = jnp.zeros((count, height), jnp.float32)
    contrib = jnp.zeros((count, total), jnp.float32)
    for target in reversed(range(SOLVE_BLOCKS)):
        settled = solved[:, target * block_size : (target + 1) * block_size]
        if target < SOLVE_BLOCKS - 1:
            portion = contrib[:, target * block_size : (target + 1) * block_size]
            settled = settled - lax.psum(portion, AXES)

        def on_group(state):
            coef = mm_t(settled, diag_inv)
            if target > 0:
                fresh = lax.dynamic_update_slice_in_dim(
                    jnp.zeros((count, total), jnp.float32),
                    mm(coef, factor_low),
                    my_column * breadth,
                    1,
                )
            else:
                fresh = state[1]
            return (coef, fresh)

        def keep_state(state):
            return state

        own_coef, contrib = lax.cond(my_block == target, on_group, keep_state, (own_coef, contrib))
    return own_coef.astype(jnp.bfloat16)


def shards(integrals, densities, screen, factor, diag_inv):
    block_size = diag_inv.shape[1]
    chip_blocks = (
        lax.axis_size("aux") == 2 * SOLVE_BLOCKS
        and factor.shape[1] == block_size
        and lax.axis_size("pair") == SOLVE_BLOCKS
    )
    solve = chip_solve if chip_blocks else chain_solve
    left, right, partial_fit = fit_partial(densities, integrals, screen)
    rounded = solve(partial_fit, factor, diag_inv)
    return scatter_sum(coulomb_partial(rounded, left, right, screen))


def solution(mesh):
    in_specs = (
        P("aux", "pair"),
        P(None, "pair"),
        P("aux", "pair"),
        P("aux", "pair"),
        P("aux", None),
    )
    out_specs = P(None, ("pair", "aux"))
    return jax.shard_map(shards, mesh=mesh, in_specs=in_specs, out_specs=out_specs, check_vma=False)
```

```python
import jax
import jax.numpy as jnp
from jax import lax
from jax.experimental import pallas as pl
from jax.experimental.pallas import tpu as pltpu
from jax.sharding import PartitionSpec as P

TILE = 128
SOLVE_BLOCKS = 4
AXES = ("aux", "pair")
HIGHEST = lax.Precision.HIGHEST
F32 = jnp.float32
BF16 = jnp.bfloat16
VMEM = pl.BlockSpec(memory_space=pltpu.VMEM)
SMEM = pl.BlockSpec(memory_space=pltpu.SMEM)
HBM = pl.BlockSpec(memory_space=pltpu.HBM)
MIB = 1024 * 1024
NN = (((1,), (0,)), ((), ()))
NT = (((1,), (1,)), ((), ()))
TN = (((0,), (0,)), ((), ()))


def struct(shape, dtype=F32):
    return jax.ShapeDtypeStruct(shape, dtype)


def call(kernel, outs, *operands, limit=12, specs=None, scratch=()):
    return pl.pallas_call(
        kernel,
        out_shape=outs,
        in_specs=specs or [VMEM] * len(operands),
        out_specs=jax.tree.map(lambda _: VMEM, outs),
        scratch_shapes=scratch,
        compiler_params=pltpu.CompilerParams(vmem_limit_bytes=limit * MIB),
    )(*operands)


def side_of():
    return lax.rem(lax.axis_index("aux"), 2)


def block_of():
    return lax.div(lax.axis_index("aux"), 2)


def masked_row(screen, densities, i, tiles):
    zero = jnp.zeros((), densities.dtype)
    return jnp.concatenate(
        [
            jnp.where(screen[i, t] != 0, densities[:, t * TILE : (t + 1) * TILE], zero)
            for t in tiles
        ],
        axis=1,
    )


def fit(
    screen_in, densities_in, integrals, left, right, out, screen, densities, total, arrived
):
    height, width = integrals.shape
    pieces = arrived.shape[0] - 2
    chunk = width // pieces
    small = [
        pltpu.make_async_copy(screen_in, screen, arrived.at[pieces]),
        pltpu.make_async_copy(densities_in, densities, arrived.at[pieces + 1]),
    ]
    copies = []
    held = []
    for j in range(pieces):
        ref = left if 2 * j < pieces else right
        start = j * chunk if ref is left else j * chunk - width // 2
        held.append(ref.at[:, start : start + chunk])
        copies.append(
            pltpu.make_async_copy(
                integrals.at[:, j * chunk : (j + 1) * chunk], held[j], arrived.at[j]
            )
        )
    for copy in small + copies:
        copy.start()
    total[...] = jnp.zeros_like(total)
    for copy in small:
        copy.wait()
    count = densities.shape[0]
    strips = height // TILE
    for j in range(pieces):
        tiles = range(j * chunk // TILE, (j + 1) * chunk // TILE)
        stacked = jnp.concatenate([masked_row(screen, densities, i, tiles) for i in range(strips)])
        copies[j].wait()
        total[...] += lax.dot_general(held[j][...], stacked, NT, preferred_element_type=F32)
    done = total[...].T
    for i in range(strips):
        out[:, i * TILE : (i + 1) * TILE] = done[
            i * count : (i + 1) * count, i * TILE : (i + 1) * TILE
        ]


def fit_partial(densities, integrals, screen):
    count = densities.shape[0]
    height, width = integrals.shape
    pieces = 8 if width % (8 * TILE) == 0 else width // TILE
    return call(
        fit,
        [struct((height, width // 2), BF16)] * 2 + [struct((count, height))],
        *(pltpu.with_memory_space_constraint(x, pltpu.HBM) for x in (screen, densities, integrals)),
        specs=[HBM] * 3,
        scratch=[
            pltpu.SMEM(screen.shape, jnp.int32),
            pltpu.VMEM(densities.shape, BF16),
            pltpu.VMEM((height, height // TILE * count), F32),
            pltpu.SemaphoreType.DMA((pieces + 2,)),
        ],
    )


def coulomb(screen, rounded, left, right, out):
    members, count, chunk = out.shape
    height, width = left.shape
    strips = height // TILE
    value = rounded[...]
    strip_of = lax.broadcasted_iota(jnp.int32, value.shape, 1) // TILE
    stacked = jnp.concatenate(
        [jnp.where(strip_of == i, value, jnp.zeros((), BF16)) for i in range(strips)]
    )
    for m in range(members):
        held = left if m * chunk < width else right
        start = m * chunk if held is left else m * chunk - width
        parts = jnp.dot(stacked, held[:, start : start + chunk], preferred_element_type=F32)
        for t in range(chunk // TILE):
            lanes = slice(t * TILE, (t + 1) * TILE)
            total = jnp.zeros((count, TILE), F32)
            for i in range(strips):
                part = parts[i * count : (i + 1) * count, lanes]
                total += jnp.where(screen[i, m * chunk // TILE + t] != 0, part, 0.0)
            out[m, :, lanes] = total.astype(out.dtype)


def coulomb_partial(rounded, left, right, screen):
    members = lax.axis_size("aux")
    out = struct((members, rounded.shape[0], 2 * left.shape[1] // members), BF16)
    return call(coulomb, out, screen, rounded, left, right, specs=[SMEM, VMEM, VMEM, VMEM])


def scatter_sum(slabs):
    arrived = lax.all_to_all(slabs, "aux", 0, 0, tiled=True)
    return jnp.sum(arrived.astype(F32), axis=0)


def high_low(value):
    high = value.astype(BF16)
    return high, (value - high.astype(F32)).astype(BF16)


def times(value, high, low, dims=NN):
    rows = value.shape[0]
    coarse = value.astype(BF16).astype(F32)
    pair = jnp.concatenate([coarse, value - coarse], axis=0).astype(BF16)
    both = lax.dot_general(pair, high, dims, preferred_element_type=F32)
    both += lax.dot_general(pair, low, dims, preferred_element_type=F32)
    return both[:rows] + both[rows:]


def prepare(inv0, inv1, fac0, fac1, k_high, k_low, kt_high, kt_low, lhs, rhs):
    height = inv0.shape[0]

    @pl.when((block_of() > 0) & (side_of() == 0))
    def _():
        for n, (inv, fac) in enumerate(((inv0, fac0), (inv1, fac1))):
            rows = [slice((3 * n + r) * height, (3 * n + r + 1) * height) for r in range(3)]
            high, low = high_low(inv[...])
            lhs[rows[0], :], lhs[rows[1], :], lhs[rows[2], :] = high, low, high
            high, low = high_low(fac[...])
            rhs[rows[0], :], rhs[rows[1], :], rhs[rows[2], :] = high, high, low
        depth = 3 * height
        halves = (
            (slice(0, height), slice(0, depth)),
            (slice(height, 2 * height), slice(0, 2 * depth)),
        )
        for part, used in halves:
            product = lax.dot_general(lhs[used, part], rhs[used, :], TN, preferred_element_type=F32)
            k_high[part, :], k_low[part, :] = high_low(product)
            kt_high[:, part], kt_low[:, part] = high_low(product.T)


def begin(f0, f1, f2, f3, inv, after, out):
    high, low = high_low(inv[...])
    out[...] = times(f0[...] + f1[...] + f2[...] + f3[...], high, low)


def both(own, mate, out):
    out[...] = own[...] + mate[...]


def after_zero(one, two, three, e, high, low, out):
    block = block_of()
    known = jnp.where(block == 1, one[...], jnp.where(block == 2, two[...], three[...]))
    term = times(known, high[...], low[...])
    out[...] = jnp.where(block == 0, e[...], jnp.where(block == 1, two[...] - term, term))


def after_one(first, second, e, high, low, out):
    block = block_of()
    known = jnp.where(block == 3, second[...], first[...])
    behind = jnp.where(block == 3, first[...], second[...])
    total = behind + times(known, high[...], low[...])
    out[...] = jnp.where(block == 0, e[...], jnp.where(block == 3, total, e[...] - total))


def turn(known, behind, e, kt_high, kt_low, high, low, settled, back):
    value = e[...] - behind[...] - times(known[...], kt_high[...], kt_low[...])
    settled[...] = value
    back[...] = times(value, high[...], low[...])


def back_two(into, near, far, t, s, high, low, settled, back, mixed):
    plane = lax.axis_index("pair")
    last = block_of() == 3
    passed = jnp.where(plane == 0, far[...], jnp.where(plane == 1, near[...], t[...]))
    value = jnp.where(last, passed, s[...] - into[...])
    product = times(value, high[...], low[...])
    settled[...] = value
    back[...] = product
    mixed[...] = jnp.where(last, product, value)


def back_one(into, other, t, s, high, low, settled, back):
    plane = lax.axis_index("pair")
    block = block_of()
    passed = jnp.where(plane == 0, other[...], t[...])
    value = jnp.where(
        block == 1,
        s[...] - into[...] - other[...],
        jnp.where(block == 2, passed, t[...]),
    )
    settled[...] = value
    product = times(value, high[...], low[...])
    back[...] = jnp.where(block == 2, product + into[...], product)


def collect(z0, z1, z2, z3, i0, i1, i2, i3, t, p1, p2, p3, out):
    plane = lax.axis_index("pair")
    block = block_of()

    def by_plane(a, b, c, d):
        return jnp.where(
            plane == 0, a[...], jnp.where(plane == 1, b[...], jnp.where(plane == 2, c[...], d[...]))
        )

    start = by_plane(z0, z1, z2, z3)
    zero = start - by_plane(i0, i1, i2, i3) - by_plane(i3, i0, i1, i2)
    one = by_plane(t, p1, p2, p3)
    two = by_plane(t, t, p1, p2)
    three = by_plane(t, t, t, p1)
    out[...] = jnp.where(
        block == 0, zero, jnp.where(block == 1, one, jnp.where(block == 2, two, three))
    )


def finish(own, mate, inv, out):
    value = jnp.where(side_of() == 0, own[...], mate[...])
    high, low = high_low(inv[...])
    out[...] = times(value, high, low, NT).astype(out.dtype)


def mm(a, b):
    return jnp.dot(a, b, precision=HIGHEST, preferred_element_type=F32)


def mm_t(a, b):
    return lax.dot_general(a, b, NT, precision=HIGHEST, preferred_element_type=F32)


def chip_solve(partial_fit, factor, diag_inv):
    count, height = partial_fit.shape
    size = 2 * height
    planes = lax.axis_size("pair")
    chips = [(k, plane) for k in range(SOLVE_BLOCKS) for plane in range(planes)]

    def device(chip, c):
        return (2 * chip[0] + c) * planes + chip[1]

    def permute(value, to):
        for chip in chips:
            for c in range(2):
                to.setdefault(device(chip, c), device(chip, 1 - c))
        return lax.ppermute(value, AXES, sorted(to.items()))

    def send(value, *moves):
        to = {}
        for source, target, *via in moves:
            loop = [device(source, 0), device(target, 0), device(target, 1)]
            for chip in via:
                loop += [device(chip, 0), device(chip, 1)]
            loop.append(device(source, 1))
            to.update(zip(loop, loop[1:] + loop[:1]))
        return permute(value, to)

    def swap(value):
        return lax.ppermute(value, "aux", [(i, i ^ 1) for i in range(2 * SOLVE_BLOCKS)])

    panel = struct((count, size))
    square = struct((size, size), BF16)
    k_high, k_low, kt_high, kt_low = call(
        prepare,
        [square] * 4,
        diag_inv,
        swap(diag_inv),
        factor,
        swap(factor),
        limit=32,
        scratch=[pltpu.VMEM((3 * size, size), BF16)] * 2,
    )
    home = [1, 1, 1, 2]
    gathered = []
    for route in ("far", "middle", "other"):
        to = {}
        for k in range(SOLVE_BLOCKS):
            turn_to = 1 if home[k] < 2 else -1
            middle, far, other = home[k] + turn_to, home[k] + 2 * turn_to, home[k] - turn_to
            ring = {"far": (far, home[k], middle), "middle": (middle, home[k]), "other": (other, home[k])}
            for c in range(2):
                loop = [device((k, plane), c) for plane in ring[route]]
                to.update(zip(loop, loop[1:] + loop[:1]))
        gathered.append(permute(partial_fit, to))
    e = call(begin, panel, partial_fit, *gathered, diag_inv, k_high)
    e = call(both, panel, e, swap(e))
    reach = [
        send(e, ((0, 1), (1, 0))),
        send(e, ((0, 1), (2, 0)), ((1, 1), (1, 0))),
        send(e, ((0, 1), (3, 0))),
    ]
    one = call(after_zero, panel, *reach, e, kt_high, kt_low)
    first = send(one, ((1, 0), (2, 1)), ((3, 0), (3, 1)), ((0, 1), (0, 0)))
    second = send(one, ((1, 0), (3, 1)), ((2, 0), (2, 1)), ((0, 1), (0, 2)))
    two = call(after_one, panel, first, second, e, kt_high, kt_low)
    behind = send(two, ((3, 1), (3, 2)), ((0, 1), (0, 3)))
    known = send(two, ((2, 1), (3, 2), (2, 2)))
    t, back = call(turn, [panel] * 2, known, behind, e, kt_high, kt_low, k_high, k_low)
    into = send(back, ((3, 2), (2, 1)))
    near = send(t, ((3, 2), (3, 1)))
    far = send(t, ((3, 2), (3, 0)))
    t, back, mixed = call(back_two, [panel] * 3, into, near, far, t, two, k_high, k_low)
    into = send(back, ((2, 1), (1, 0)), ((3, 0), (2, 0)))
    other = send(mixed, ((3, 1), (1, 0)), ((2, 1), (2, 0)))
    t, back = call(back_one, [panel] * 2, into, other, t, one, k_high, k_low)
    near = {
        ((1, 0), (0, 3)): (3, 0),
        ((1, 0), (0, 2)): (1, 1),
        ((2, 0), (0, 3)): (2, 1),
        ((2, 0), (0, 2)): (3, 1),
    }
    into = [None] * planes
    spread = [None] * planes
    for plane in reversed(range(planes)):
        moves = [((1, 0), (0, plane)), ((2, 0), (0, (plane + 1) % planes))]
        into[plane] = send(
            back, *((*move, near[move]) if move in near else move for move in moves)
        )
    for step in reversed(range(1, planes)):
        moves = [((1, 0), (1, step))]
        if 1 + step < planes:
            moves.append(((2, 1), (2, 1 + step)))
        if 2 + step < planes:
            moves.append(((3, 2), (3, 2 + step)))
        spread[step] = send(t, *moves)
    t = call(collect, panel, first, e, second, behind, *into, t, *spread[1:])
    return call(finish, struct((count, height), BF16), t, swap(t), diag_inv)


def chain_solve(partial_fit, factor, diag_inv):
    count, height = partial_fit.shape
    breadth = factor.shape[1]
    block_size = diag_inv.shape[1]
    rows_aux = lax.axis_size("aux")
    total = height * rows_aux
    members = rows_aux // SOLVE_BLOCKS
    my_row = lax.axis_index("aux")
    my_column = lax.axis_index("pair")
    my_block = my_row // members
    column_block = (my_column * breadth + jnp.arange(breadth, dtype=jnp.int32)) // block_size
    factor_low = jnp.where((column_block < my_block)[None, :], factor, 0.0)

    def own_columns(whole):
        return lax.dynamic_slice_in_dim(whole, my_column * breadth, breadth, 1)

    zero_block = jnp.zeros((count, block_size), jnp.float32)
    solved = jnp.zeros((count, total), jnp.float32)
    for k in range(SOLVE_BLOCKS):

        def on_group(current):
            return mm(partial_fit - mm_t(own_columns(current), factor_low), diag_inv)

        def off_group(current):
            return zero_block

        summand = lax.cond(my_block == k, on_group, off_group, solved)
        arrived = lax.psum(summand, AXES)
        solved = lax.dynamic_update_slice_in_dim(solved, arrived, k * block_size, 1)
    own_coef = jnp.zeros((count, height), jnp.float32)
    contrib = jnp.zeros((count, total), jnp.float32)
    for target in reversed(range(SOLVE_BLOCKS)):
        settled = solved[:, target * block_size : (target + 1) * block_size]
        if target < SOLVE_BLOCKS - 1:
            portion = contrib[:, target * block_size : (target + 1) * block_size]
            settled = settled - lax.psum(portion, AXES)

        def on_group(state):
            coef = mm_t(settled, diag_inv)
            if target > 0:
                fresh = lax.dynamic_update_slice_in_dim(
                    jnp.zeros((count, total), jnp.float32),
                    mm(coef, factor_low),
                    my_column * breadth,
                    1,
                )
            else:
                fresh = state[1]
            return (coef, fresh)

        def keep_state(state):
            return state

        own_coef, contrib = lax.cond(my_block == target, on_group, keep_state, (own_coef, contrib))
    return own_coef.astype(jnp.bfloat16)


def shards(integrals, densities, screen, factor, diag_inv):
    block_size = diag_inv.shape[1]
    chip_blocks = (
        lax.axis_size("aux") == 2 * SOLVE_BLOCKS
        and factor.shape[1] == block_size
        and lax.axis_size("pair") == SOLVE_BLOCKS
    )
    solve = chip_solve if chip_blocks else chain_solve
    left, right, partial_fit = fit_partial(densities, integrals, screen)
    rounded = solve(partial_fit, factor, diag_inv)
    return scatter_sum(coulomb_partial(rounded, left, right, screen))


def solution(mesh):
    in_specs = (
        P("aux", "pair"),
        P(None, "pair"),
        P("aux", "pair"),
        P("aux", "pair"),
        P("aux", None),
    )
    out_specs = P(None, ("pair", "aux"))
    return jax.shard_map(shards, mesh=mesh, in_specs=in_specs, out_specs=out_specs, check_vma=False)
```

```python
import functools

import jax
import jax.numpy as jnp
from jax import lax
from jax.experimental import pallas as pl
from jax.experimental.pallas import tpu as pltpu
from jax.sharding import PartitionSpec as P

TILE = 128
SOLVE_BLOCKS = 4
AXES = ("aux", "pair")
HIGHEST = lax.Precision.HIGHEST
F32 = jnp.float32
BF16 = jnp.bfloat16
VMEM = pl.BlockSpec(memory_space=pltpu.VMEM)
SMEM = pl.BlockSpec(memory_space=pltpu.SMEM)
HBM = pl.BlockSpec(memory_space=pltpu.HBM)
MIB = 1024 * 1024
NN = (((1,), (0,)), ((), ()))
NT = (((1,), (1,)), ((), ()))
TN = (((0,), (0,)), ((), ()))


def struct(shape, dtype=F32):
    return jax.ShapeDtypeStruct(shape, dtype)


def call(kernel, outs, *operands, limit=12, specs=None, scratch=()):
    return pl.pallas_call(
        kernel,
        out_shape=outs,
        in_specs=specs or [VMEM] * len(operands),
        out_specs=jax.tree.map(lambda _: VMEM, outs),
        scratch_shapes=scratch,
        compiler_params=pltpu.CompilerParams(vmem_limit_bytes=limit * MIB),
    )(*operands)


def side_of():
    return lax.rem(lax.axis_index("aux"), 2)


def block_of():
    return lax.div(lax.axis_index("aux"), 2)


def masked_row(screen, densities, i, tiles):
    zero = jnp.zeros((), densities.dtype)
    return jnp.concatenate(
        [
            jnp.where(screen[i, t] != 0, densities[:, t * TILE : (t + 1) * TILE], zero)
            for t in tiles
        ],
        axis=1,
    )


def fit(
    screen_in, densities_in, integrals, left, right, out, screen, densities, total, arrived
):
    height, width = integrals.shape
    pieces = arrived.shape[0] - 2
    chunk = width // pieces
    small = [
        pltpu.make_async_copy(screen_in, screen, arrived.at[pieces]),
        pltpu.make_async_copy(densities_in, densities, arrived.at[pieces + 1]),
    ]
    copies = []
    held = []
    for j in range(pieces):
        ref = left if 2 * j < pieces else right
        start = j * chunk if ref is left else j * chunk - width // 2
        held.append(ref.at[:, start : start + chunk])
        copies.append(
            pltpu.make_async_copy(
                integrals.at[:, j * chunk : (j + 1) * chunk], held[j], arrived.at[j]
            )
        )
    for copy in small + copies:
        copy.start()
    total[...] = jnp.zeros_like(total)
    for copy in small:
        copy.wait()
    count = densities.shape[0]
    strips = height // TILE
    for j in range(pieces):
        tiles = range(j * chunk // TILE, (j + 1) * chunk // TILE)
        stacked = jnp.concatenate([masked_row(screen, densities, i, tiles) for i in range(strips)])
        copies[j].wait()
        total[...] += lax.dot_general(held[j][...], stacked, NT, preferred_element_type=F32)
    done = total[...].T
    for i in range(strips):
        out[:, i * TILE : (i + 1) * TILE] = done[
            i * count : (i + 1) * count, i * TILE : (i + 1) * TILE
        ]


def fit_partial(densities, integrals, screen):
    count = densities.shape[0]
    height, width = integrals.shape
    pieces = 8 if width % (8 * TILE) == 0 else width // TILE
    return call(
        fit,
        [struct((height, width // 2), BF16)] * 2 + [struct((count, height))],
        *(pltpu.with_memory_space_constraint(x, pltpu.HBM) for x in (screen, densities, integrals)),
        specs=[HBM] * 3,
        scratch=[
            pltpu.SMEM(screen.shape, jnp.int32),
            pltpu.VMEM(densities.shape, BF16),
            pltpu.VMEM((height, height // TILE * count), F32),
            pltpu.SemaphoreType.DMA((pieces + 2,)),
        ],
    )


def coulomb(screen, rounded, left, right, out):
    members, count, chunk = out.shape
    height, width = left.shape
    strips = height // TILE
    value = rounded[...]
    strip_of = lax.broadcasted_iota(jnp.int32, value.shape, 1) // TILE
    stacked = jnp.concatenate(
        [jnp.where(strip_of == i, value, jnp.zeros((), BF16)) for i in range(strips)]
    )
    for m in range(members):
        held = left if m * chunk < width else right
        start = m * chunk if held is left else m * chunk - width
        parts = jnp.dot(stacked, held[:, start : start + chunk], preferred_element_type=F32)
        for t in range(chunk // TILE):
            lanes = slice(t * TILE, (t + 1) * TILE)
            total = jnp.zeros((count, TILE), F32)
            for i in range(strips):
                part = parts[i * count : (i + 1) * count, lanes]
                total += jnp.where(screen[i, m * chunk // TILE + t] != 0, part, 0.0)
            out[m, :, lanes] = total.astype(out.dtype)


def coulomb_partial(rounded, left, right, screen):
    members = lax.axis_size("aux")
    out = struct((members, rounded.shape[0], 2 * left.shape[1] // members), BF16)
    return call(coulomb, out, screen, rounded, left, right, specs=[SMEM, VMEM, VMEM, VMEM])


def scatter_sum(slabs):
    arrived = lax.all_to_all(slabs, "aux", 0, 0, tiled=True)
    return jnp.sum(arrived.astype(F32), axis=0)


def high_low(value):
    high = value.astype(BF16)
    return high, (value - high.astype(F32)).astype(BF16)


def times(value, high, low, dims=NN):
    rows = value.shape[0]
    coarse = value.astype(BF16).astype(F32)
    pair = jnp.concatenate([coarse, value - coarse], axis=0).astype(BF16)
    both = lax.dot_general(pair, high, dims, preferred_element_type=F32)
    both += lax.dot_general(pair, low, dims, preferred_element_type=F32)
    return both[:rows] + both[rows:]


def prepare(inv0, inv1, fac0, fac1, k_high, k_low, kt_high, kt_low, lhs, rhs):
    height = inv0.shape[0]

    @pl.when((block_of() > 0) & (side_of() == 0))
    def _():
        for n, (inv, fac) in enumerate(((inv0, fac0), (inv1, fac1))):
            rows = [slice((3 * n + r) * height, (3 * n + r + 1) * height) for r in range(3)]
            high, low = high_low(inv[...])
            lhs[rows[0], :], lhs[rows[1], :], lhs[rows[2], :] = high, low, high
            high, low = high_low(fac[...])
            rhs[rows[0], :], rhs[rows[1], :], rhs[rows[2], :] = high, high, low
        depth = 3 * height
        halves = (
            (slice(0, height), slice(0, depth)),
            (slice(height, 2 * height), slice(0, 2 * depth)),
        )
        for part, used in halves:
            product = lax.dot_general(lhs[used, part], rhs[used, :], TN, preferred_element_type=F32)
            k_high[part, :], k_low[part, :] = high_low(product)
            kt_high[:, part], kt_low[:, part] = high_low(product.T)


def begin(f0, f1, f2, f3, inv, out):
    high, low = high_low(inv[...])
    out[...] = times(f0[...] + f1[...] + f2[...] + f3[...], high, low)


def both(own, mate, out):
    out[...] = own[...] + mate[...]


def lead_only(kernel):
    @functools.wraps(kernel)
    def guarded(*refs):
        pl.when(side_of() == 0)(lambda: kernel(*refs))

    return guarded


@lead_only
def after_zero(one, two, three, e, high, low, out):
    block = block_of()
    known = jnp.where(block == 1, one[...], jnp.where(block == 2, two[...], three[...]))
    term = times(known, high[...], low[...])
    out[...] = jnp.where(block == 0, e[...], jnp.where(block == 1, two[...] - term, term))


@lead_only
def after_one(first, second, e, high, low, out):
    block = block_of()
    known = jnp.where(block == 3, second[...], first[...])
    behind = jnp.where(block == 3, first[...], second[...])
    total = behind + times(known, high[...], low[...])
    out[...] = jnp.where(block == 0, e[...], jnp.where(block == 3, total, e[...] - total))


@lead_only
def turn(known, behind, e, kt_high, kt_low, high, low, settled, back):
    value = e[...] - behind[...] - times(known[...], kt_high[...], kt_low[...])
    settled[...] = value
    back[...] = times(value, high[...], low[...])


@lead_only
def back_two(into, near, far, t, s, high, low, settled, back, mixed):
    plane = lax.axis_index("pair")
    last = block_of() == 3
    passed = jnp.where(plane == 0, far[...], jnp.where(plane == 1, near[...], t[...]))
    value = jnp.where(last, passed, s[...] - into[...])
    product = times(value, high[...], low[...])
    settled[...] = value
    back[...] = product
    mixed[...] = jnp.where(last, product, value)


@lead_only
def back_one(into, other, t, s, high, low, settled, back):
    plane = lax.axis_index("pair")
    block = block_of()
    passed = jnp.where(plane == 0, other[...], t[...])
    value = jnp.where(
        block == 1,
        s[...] - into[...] - other[...],
        jnp.where(block == 2, passed, t[...]),
    )
    settled[...] = value
    product = times(value, high[...], low[...])
    back[...] = jnp.where(block == 2, product + into[...], product)


def collect(z0, z1, z2, z3, i0, i1, i2, i3, t, p1, p2, p3, out):
    plane = lax.axis_index("pair")
    block = block_of()

    def by_plane(a, b, c, d):
        return jnp.where(
            plane == 0, a[...], jnp.where(plane == 1, b[...], jnp.where(plane == 2, c[...], d[...]))
        )

    start = by_plane(z0, z1, z2, z3)
    zero = start - by_plane(i0, i1, i2, i3) - by_plane(i3, i0, i1, i2)
    one = by_plane(t, p1, p2, p3)
    two = by_plane(t, t, p1, p2)
    three = by_plane(t, t, t, p1)
    out[...] = jnp.where(
        block == 0, zero, jnp.where(block == 1, one, jnp.where(block == 2, two, three))
    )


def finish(own, mate, inv, out):
    value = jnp.where(side_of() == 0, own[...], mate[...])
    high, low = high_low(inv[...])
    out[...] = times(value, high, low, NT).astype(out.dtype)


def mm(a, b):
    return jnp.dot(a, b, precision=HIGHEST, preferred_element_type=F32)


def mm_t(a, b):
    return lax.dot_general(a, b, NT, precision=HIGHEST, preferred_element_type=F32)


def chip_solve(partial_fit, factor, diag_inv):
    count, height = partial_fit.shape
    size = 2 * height
    planes = lax.axis_size("pair")
    chips = [(k, plane) for k in range(SOLVE_BLOCKS) for plane in range(planes)]

    def device(chip, c):
        return (2 * chip[0] + c) * planes + chip[1]

    def permute(value, to):
        for chip in chips:
            for c in range(2):
                to.setdefault(device(chip, c), device(chip, 1 - c))
        return lax.ppermute(value, AXES, sorted(to.items()))

    def send(value, *moves):
        to = {}
        for source, target, *via in moves:
            loop = [device(source, 0), device(target, 0), device(target, 1)]
            for chip in via:
                loop += [device(chip, 0), device(chip, 1)]
            loop.append(device(source, 1))
            to.update(zip(loop, loop[1:] + loop[:1]))
        return permute(value, to)

    def swap(value):
        return lax.ppermute(value, "aux", [(i, i ^ 1) for i in range(2 * SOLVE_BLOCKS)])

    panel = struct((count, size))
    square = struct((size, size), BF16)
    k_high, k_low, kt_high, kt_low = call(
        prepare,
        [square] * 4,
        diag_inv,
        swap(diag_inv),
        factor,
        swap(factor),
        limit=32,
        scratch=[pltpu.VMEM((3 * size, size), BF16)] * 2,
    )
    home = [1, 1, 1, 2]
    gathered = []
    for route in ("far", "middle", "other"):
        to = {}
        for k in range(SOLVE_BLOCKS):
            turn_to = 1 if home[k] < 2 else -1
            middle, far, other = home[k] + turn_to, home[k] + 2 * turn_to, home[k] - turn_to
            ring = {"far": (far, home[k], middle), "middle": (middle, home[k]), "other": (other, home[k])}
            for c in range(2):
                loop = [device((k, plane), c) for plane in ring[route]]
                to.update(zip(loop, loop[1:] + loop[:1]))
        gathered.append(permute(partial_fit, to))
    e = call(begin, panel, partial_fit, *gathered, diag_inv)
    e = call(both, panel, e, swap(e))
    reach = [
        send(e, ((0, 1), (1, 0))),
        send(e, ((0, 1), (2, 0)), ((1, 1), (1, 0))),
        send(e, ((0, 1), (3, 0))),
    ]
    one = call(after_zero, panel, *reach, e, kt_high, kt_low)
    first = send(one, ((1, 0), (2, 1)), ((3, 0), (3, 1)), ((0, 1), (0, 0)))
    second = send(one, ((1, 0), (3, 1)), ((2, 0), (2, 1)), ((0, 1), (0, 2)))
    two = call(after_one, panel, first, second, e, kt_high, kt_low)
    behind = send(two, ((3, 1), (3, 2)), ((0, 1), (0, 3)))
    known = send(two, ((2, 1), (3, 2), (2, 2)))
    t, back = call(turn, [panel] * 2, known, behind, e, kt_high, kt_low, k_high, k_low)
    into = send(back, ((3, 2), (2, 1)))
    near = send(t, ((3, 2), (3, 1)))
    far = send(t, ((3, 2), (3, 0)))
    t, back, mixed = call(back_two, [panel] * 3, into, near, far, t, two, k_high, k_low)
    into = send(back, ((2, 1), (1, 0)), ((3, 0), (2, 0)))
    other = send(mixed, ((3, 1), (1, 0)), ((2, 1), (2, 0)))
    t, back = call(back_one, [panel] * 2, into, other, t, one, k_high, k_low)
    near = {
        ((1, 0), (0, 3)): (3, 0),
        ((1, 0), (0, 2)): (1, 1),
        ((2, 0), (0, 3)): (2, 1),
        ((2, 0), (0, 2)): (3, 1),
    }
    into = [None] * planes
    spread = [None] * planes
    for plane in reversed(range(planes)):
        moves = [((1, 0), (0, plane)), ((2, 0), (0, (plane + 1) % planes))]
        into[plane] = send(
            back, *((*move, near[move]) if move in near else move for move in moves)
        )
    for step in reversed(range(1, planes)):
        moves = [((1, 0), (1, step))]
        if 1 + step < planes:
            moves.append(((2, 1), (2, 1 + step)))
        if 2 + step < planes:
            moves.append(((3, 2), (3, 2 + step)))
        spread[step] = send(t, *moves)
    t = call(collect, panel, first, e, second, behind, *into, t, *spread[1:])
    return call(finish, struct((count, height), BF16), t, swap(t), diag_inv)


def chain_solve(partial_fit, factor, diag_inv):
    count, height = partial_fit.shape
    breadth = factor.shape[1]
    block_size = diag_inv.shape[1]
    rows_aux = lax.axis_size("aux")
    total = height * rows_aux
    members = rows_aux // SOLVE_BLOCKS
    my_row = lax.axis_index("aux")
    my_column = lax.axis_index("pair")
    my_block = my_row // members
    column_block = (my_column * breadth + jnp.arange(breadth, dtype=jnp.int32)) // block_size
    factor_low = jnp.where((column_block < my_block)[None, :], factor, 0.0)

    def own_columns(whole):
        return lax.dynamic_slice_in_dim(whole, my_column * breadth, breadth, 1)

    zero_block = jnp.zeros((count, block_size), jnp.float32)
    solved = jnp.zeros((count, total), jnp.float32)
    for k in range(SOLVE_BLOCKS):

        def on_group(current):
            return mm(partial_fit - mm_t(own_columns(current), factor_low), diag_inv)

        def off_group(current):
            return zero_block

        summand = lax.cond(my_block == k, on_group, off_group, solved)
        arrived = lax.psum(summand, AXES)
        solved = lax.dynamic_update_slice_in_dim(solved, arrived, k * block_size, 1)
    own_coef = jnp.zeros((count, height), jnp.float32)
    contrib = jnp.zeros((count, total), jnp.float32)
    for target in reversed(range(SOLVE_BLOCKS)):
        settled = solved[:, target * block_size : (target + 1) * block_size]
        if target < SOLVE_BLOCKS - 1:
            portion = contrib[:, target * block_size : (target + 1) * block_size]
            settled = settled - lax.psum(portion, AXES)

        def on_group(state):
            coef = mm_t(settled, diag_inv)
            if target > 0:
                fresh = lax.dynamic_update_slice_in_dim(
                    jnp.zeros((count, total), jnp.float32),
                    mm(coef, factor_low),
                    my_column * breadth,
                    1,
                )
            else:
                fresh = state[1]
            return (coef, fresh)

        def keep_state(state):
            return state

        own_coef, contrib = lax.cond(my_block == target, on_group, keep_state, (own_coef, contrib))
    return own_coef.astype(jnp.bfloat16)


def shards(integrals, densities, screen, factor, diag_inv):
    block_size = diag_inv.shape[1]
    chip_blocks = (
        lax.axis_size("aux") == 2 * SOLVE_BLOCKS
        and factor.shape[1] == block_size
        and lax.axis_size("pair") == SOLVE_BLOCKS
    )
    solve = chip_solve if chip_blocks else chain_solve
    left, right, partial_fit = fit_partial(densities, integrals, screen)
    rounded = solve(partial_fit, factor, diag_inv)
    return scatter_sum(coulomb_partial(rounded, left, right, screen))


def solution(mesh):
    in_specs = (
        P("aux", "pair"),
        P(None, "pair"),
        P("aux", "pair"),
        P("aux", "pair"),
        P("aux", None),
    )
    out_specs = P(None, ("pair", "aux"))
    return jax.shard_map(shards, mesh=mesh, in_specs=in_specs, out_specs=out_specs, check_vma=False)
```

```python
import functools

import jax
import jax.numpy as jnp
from jax import lax
from jax.experimental import pallas as pl
from jax.experimental.pallas import tpu as pltpu
from jax.sharding import PartitionSpec as P

TILE = 128
SOLVE_BLOCKS = 4
AXES = ("aux", "pair")
HIGHEST = lax.Precision.HIGHEST
F32 = jnp.float32
BF16 = jnp.bfloat16
VMEM = pl.BlockSpec(memory_space=pltpu.VMEM)
SMEM = pl.BlockSpec(memory_space=pltpu.SMEM)
HBM = pl.BlockSpec(memory_space=pltpu.HBM)
MIB = 1024 * 1024
NN = (((1,), (0,)), ((), ()))
NT = (((1,), (1,)), ((), ()))
TN = (((0,), (0,)), ((), ()))


def struct(shape, dtype=F32):
    return jax.ShapeDtypeStruct(shape, dtype)


def call(kernel, outs, *operands, limit=12, specs=None, scratch=()):
    return pl.pallas_call(
        kernel,
        out_shape=outs,
        in_specs=specs or [VMEM] * len(operands),
        out_specs=jax.tree.map(lambda _: VMEM, outs),
        scratch_shapes=scratch,
        compiler_params=pltpu.CompilerParams(vmem_limit_bytes=limit * MIB),
    )(*operands)


def side_of():
    return lax.rem(lax.axis_index("aux"), 2)


def block_of():
    return lax.div(lax.axis_index("aux"), 2)


def masked_row(screen, densities, i, tiles):
    zero = jnp.zeros((), densities.dtype)
    return jnp.concatenate(
        [
            jnp.where(screen[i, t] != 0, densities[:, t * TILE : (t + 1) * TILE], zero)
            for t in tiles
        ],
        axis=1,
    )


def fit(
    screen_in, densities_in, integrals, left, right, out, screen, densities, total, arrived
):
    height, width = integrals.shape
    pieces = arrived.shape[0] - 2
    chunk = width // pieces
    small = [
        pltpu.make_async_copy(screen_in, screen, arrived.at[pieces]),
        pltpu.make_async_copy(densities_in, densities, arrived.at[pieces + 1]),
    ]
    copies = []
    held = []
    for j in range(pieces):
        ref = left if 2 * j < pieces else right
        start = j * chunk if ref is left else j * chunk - width // 2
        held.append(ref.at[:, start : start + chunk])
        copies.append(
            pltpu.make_async_copy(
                integrals.at[:, j * chunk : (j + 1) * chunk], held[j], arrived.at[j]
            )
        )
    for copy in small + copies:
        copy.start()
    total[...] = jnp.zeros_like(total)
    for copy in small:
        copy.wait()
    count = densities.shape[0]
    strips = height // TILE
    for j in range(pieces):
        tiles = range(j * chunk // TILE, (j + 1) * chunk // TILE)
        stacked = jnp.concatenate([masked_row(screen, densities, i, tiles) for i in range(strips)])
        copies[j].wait()
        total[...] += lax.dot_general(held[j][...], stacked, NT, preferred_element_type=F32)
    done = total[...].T
    for i in range(strips):
        out[:, i * TILE : (i + 1) * TILE] = done[
            i * count : (i + 1) * count, i * TILE : (i + 1) * TILE
        ]


def fit_partial(densities, integrals, screen):
    count = densities.shape[0]
    height, width = integrals.shape
    pieces = 8 if width % (8 * TILE) == 0 else width // TILE
    return call(
        fit,
        [struct((height, width // 2), BF16)] * 2 + [struct((count, height))],
        *(pltpu.with_memory_space_constraint(x, pltpu.HBM) for x in (screen, densities, integrals)),
        specs=[HBM] * 3,
        scratch=[
            pltpu.SMEM(screen.shape, jnp.int32),
            pltpu.VMEM(densities.shape, BF16),
            pltpu.VMEM((height, height // TILE * count), F32),
            pltpu.SemaphoreType.DMA((pieces + 2,)),
        ],
    )


def slab(screen, stacked, left, right, member, index):
    strips = left.shape[0] // TILE
    count = stacked.shape[0] // strips
    members, base = index
    chunk = 2 * left.shape[1] // members
    held = left if 2 * base < members else right
    offset = 0 if held is left else members // 2
    columns = pl.ds(pl.multiple_of((member - offset) * chunk, TILE), chunk)
    parts = jnp.dot(stacked, held[:, columns], preferred_element_type=F32)
    tiles = []
    for t in range(chunk // TILE):
        total = jnp.zeros((count, TILE), F32)
        for i in range(strips):
            part = parts[i * count : (i + 1) * count, t * TILE : (t + 1) * TILE]
            total += jnp.where(screen[i, member * (chunk // TILE) + t] != 0, part, 0.0)
        tiles.append(total)
    return jnp.concatenate(tiles, axis=1)


def by_strip(value, strips):
    strip_of = lax.broadcasted_iota(jnp.int32, value.shape, 1) // TILE
    return jnp.concatenate(
        [jnp.where(strip_of == i, value, jnp.zeros((), BF16)) for i in range(strips)]
    )


def coulomb(screen, rounded, left, right, out):
    members = out.shape[0]
    stacked = by_strip(rounded[...], left.shape[0] // TILE)
    for m in range(members):
        out[m] = slab(screen, stacked, left, right, m, (members, m)).astype(out.dtype)


def coulomb_side(side, screen, rounded, left, right, out):
    chips = out.shape[0]
    stacked = by_strip(rounded[...], left.shape[0] // TILE)
    for k in range(chips):
        part = slab(screen, stacked, left, right, 2 * k + side, (2 * chips, 2 * k))
        out[k] = part.astype(out.dtype)


def coulomb_mate(*refs):
    coulomb_side(1 - side_of(), *refs)


def coulomb_own(*refs):
    coulomb_side(side_of(), *refs)


def share(own, got, keep, one, two, three):
    block = block_of()
    keep[...] = own[block] + got[block].astype(F32)
    for distance, out in ((1, one), (2, two), (3, three)):
        chip = lax.bitwise_xor(block, distance)
        out[...] = (own[chip] + got[chip].astype(F32)).astype(out.dtype)


def gather_up(keep, one, two, three, out):
    out[...] = keep[...] + one[...].astype(F32) + two[...].astype(F32) + three[...].astype(F32)


def coulomb_partial(rounded, left, right, screen):
    members = lax.axis_size("aux")
    out = struct((members, rounded.shape[0], 2 * left.shape[1] // members), BF16)
    return call(coulomb, out, screen, rounded, left, right, specs=[SMEM, VMEM, VMEM, VMEM])


def chip_coulomb(rounded, left, right, screen):
    members = 2 * SOLVE_BLOCKS
    count = rounded.shape[0]
    chunk = 2 * left.shape[1] // members
    specs = [SMEM, VMEM, VMEM, VMEM]
    operands = (screen, rounded, left, right)
    given = call(coulomb_mate, struct((SOLVE_BLOCKS, count, chunk), BF16), *operands, specs=specs)

    def move(value, to):
        return lax.ppermute(value, "aux", [(i, to(i)) for i in range(members)])

    got = move(given, lambda i: i ^ 1)
    own = call(coulomb_own, struct((SOLVE_BLOCKS, count, chunk)), *operands, specs=specs)
    piece = struct((count, chunk), BF16)
    keep, one, two, three = call(share, [struct((count, chunk))] + [piece] * 3, own, got)
    three = move(three, lambda i: i ^ 6)
    one = move(one, lambda i: i ^ 2)
    two = move(two, lambda i: i ^ 4)
    return call(gather_up, struct((count, chunk)), keep, one, two, three)


def scatter_sum(slabs):
    arrived = lax.all_to_all(slabs, "aux", 0, 0, tiled=True)
    return jnp.sum(arrived.astype(F32), axis=0)


def high_low(value):
    high = value.astype(BF16)
    return high, (value - high.astype(F32)).astype(BF16)


def times(value, high, low, dims=NN):
    rows = value.shape[0]
    coarse = value.astype(BF16).astype(F32)
    pair = jnp.concatenate([coarse, value - coarse], axis=0).astype(BF16)
    both = lax.dot_general(pair, high, dims, preferred_element_type=F32)
    both += lax.dot_general(pair, low, dims, preferred_element_type=F32)
    return both[:rows] + both[rows:]


def prepare_first(*refs):
    here = (block_of() == 0) | (lax.axis_index("pair") > 0)
    prepare(here, *refs)


def prepare_later(*refs):
    prepare(lax.axis_index("pair") == 0, *refs)


def prepare(here, inv0, inv1, fac0, fac1, k_high, k_low, kt_high, kt_low, lhs, rhs):
    height = inv0.shape[0]

    @pl.when(here & (block_of() > 0) & (side_of() == 0))
    def _():
        for n, (inv, fac) in enumerate(((inv0, fac0), (inv1, fac1))):
            rows = [slice((3 * n + r) * height, (3 * n + r + 1) * height) for r in range(3)]
            high, low = high_low(inv[...])
            lhs[rows[0], :], lhs[rows[1], :], lhs[rows[2], :] = high, low, high
            high, low = high_low(fac[...])
            rhs[rows[0], :], rhs[rows[1], :], rhs[rows[2], :] = high, high, low
        depth = 3 * height
        halves = (
            (slice(0, height), slice(0, depth)),
            (slice(height, 2 * height), slice(0, 2 * depth)),
        )
        for part, used in halves:
            product = lax.dot_general(lhs[used, part], rhs[used, :], TN, preferred_element_type=F32)
            k_high[part, :], k_low[part, :] = high_low(product)
            kt_high[:, part], kt_low[:, part] = high_low(product.T)


def begin(f0, f1, f2, f3, inv, after, out):
    high, low = high_low(inv[...])
    out[...] = times(f0[...] + f1[...] + f2[...] + f3[...], high, low)


def both(own, mate, out):
    out[...] = own[...] + mate[...]


def lead_only(kernel):
    @functools.wraps(kernel)
    def guarded(*refs):
        pl.when(side_of() == 0)(lambda: kernel(*refs))

    return guarded


@lead_only
def after_zero(one, two, three, e, high, low, out):
    block = block_of()
    known = jnp.where(block == 1, one[...], jnp.where(block == 2, two[...], three[...]))
    term = times(known, high[...], low[...])
    out[...] = jnp.where(block == 0, e[...], jnp.where(block == 1, two[...] - term, term))


@lead_only
def after_one(first, second, e, high, low, out):
    block = block_of()
    known = jnp.where(block == 3, second[...], first[...])
    behind = jnp.where(block == 3, first[...], second[...])
    total = behind + times(known, high[...], low[...])
    out[...] = jnp.where(block == 0, e[...], jnp.where(block == 3, total, e[...] - total))


@lead_only
def turn(known, behind, e, kt_high, kt_low, high, low, settled, back):
    value = e[...] - behind[...] - times(known[...], kt_high[...], kt_low[...])
    settled[...] = value
    back[...] = times(value, high[...], low[...])


@lead_only
def back_two(into, near, far, t, s, high, low, high0, low0, settled, back, mixed):
    plane = lax.axis_index("pair")
    last = block_of() == 3
    passed = jnp.where(plane == 0, far[...], jnp.where(plane == 1, near[...], t[...]))
    value = jnp.where(last, passed, s[...] - into[...])
    settled[...] = value

    def multiply(high, low):
        product = times(value, high[...], low[...])
        back[...] = product
        mixed[...] = jnp.where(last, product, value)

    pl.when(plane == 0)(lambda: multiply(high0, low0))
    pl.when(plane > 0)(lambda: multiply(high, low))


@lead_only
def back_one(into, other, t, s, high, low, settled, back):
    plane = lax.axis_index("pair")
    block = block_of()
    passed = jnp.where(plane == 0, other[...], t[...])
    value = jnp.where(
        block == 1,
        s[...] - into[...] - other[...],
        jnp.where(block == 2, passed, t[...]),
    )
    settled[...] = value
    product = times(value, high[...], low[...])
    back[...] = jnp.where(block == 2, product + into[...], product)


def collect(z0, z1, z2, z3, i0, i1, i2, i3, t, p1, p2, p3, out):
    plane = lax.axis_index("pair")
    block = block_of()

    def by_plane(a, b, c, d):
        return jnp.where(
            plane == 0, a[...], jnp.where(plane == 1, b[...], jnp.where(plane == 2, c[...], d[...]))
        )

    start = by_plane(z0, z1, z2, z3)
    zero = start - by_plane(i0, i1, i2, i3) - by_plane(i3, i0, i1, i2)
    one = by_plane(t, p1, p2, p3)
    two = by_plane(t, t, p1, p2)
    three = by_plane(t, t, t, p1)
    out[...] = jnp.where(
        block == 0, zero, jnp.where(block == 1, one, jnp.where(block == 2, two, three))
    )


def finish(own, mate, inv, out):
    value = jnp.where(side_of() == 0, own[...], mate[...])
    high, low = high_low(inv[...])
    out[...] = times(value, high, low, NT).astype(out.dtype)


def mm(a, b):
    return jnp.dot(a, b, precision=HIGHEST, preferred_element_type=F32)


def mm_t(a, b):
    return lax.dot_general(a, b, NT, precision=HIGHEST, preferred_element_type=F32)


def chip_solve(partial_fit, factor, diag_inv):
    count, height = partial_fit.shape
    size = 2 * height
    planes = lax.axis_size("pair")
    chips = [(k, plane) for k in range(SOLVE_BLOCKS) for plane in range(planes)]

    def device(chip, c):
        return (2 * chip[0] + c) * planes + chip[1]

    def permute(value, to):
        for chip in chips:
            for c in range(2):
                to.setdefault(device(chip, c), device(chip, 1 - c))
        return lax.ppermute(value, AXES, sorted(to.items()))

    def send(value, *moves):
        to = {}
        for source, target, *via in moves:
            loop = [device(source, 0), device(target, 0), device(target, 1)]
            for chip in via:
                loop += [device(chip, 0), device(chip, 1)]
            loop.append(device(source, 1))
            to.update(zip(loop, loop[1:] + loop[:1]))
        return permute(value, to)

    def swap(value):
        return lax.ppermute(value, "aux", [(i, i ^ 1) for i in range(2 * SOLVE_BLOCKS)])

    panel = struct((count, size))
    square = struct((size, size), BF16)
    halves = (diag_inv, swap(diag_inv), factor, swap(factor))

    def prepared(kernel):
        scratch = [pltpu.VMEM((3 * size, size), BF16)] * 2
        return call(kernel, [square] * 4, *halves, limit=32, scratch=scratch)

    k_high, k_low, kt_high, kt_low = prepared(prepare_first)
    at_zero = prepared(prepare_later)
    home = [1, 1, 1, 2]
    gathered = []
    for route in ("far", "middle", "other"):
        to = {}
        for k in range(SOLVE_BLOCKS):
            turn_to = 1 if home[k] < 2 else -1
            middle, far, other = home[k] + turn_to, home[k] + 2 * turn_to, home[k] - turn_to
            ring = {"far": (far, home[k], middle), "middle": (middle, home[k]), "other": (other, home[k])}
            for c in range(2):
                loop = [device((k, plane), c) for plane in ring[route]]
                to.update(zip(loop, loop[1:] + loop[:1]))
        gathered.append(permute(partial_fit, to))
    e = call(begin, panel, partial_fit, *gathered, diag_inv, k_high)
    e = call(both, panel, e, swap(e))
    reach = [
        send(e, ((0, 1), (1, 0))),
        send(e, ((0, 1), (2, 0)), ((1, 1), (1, 0))),
        send(e, ((0, 1), (3, 0))),
    ]
    one = call(after_zero, panel, *reach, e, *at_zero[2:])
    first = send(one, ((1, 0), (2, 1)), ((3, 0), (3, 1)), ((0, 1), (0, 0)))
    second = send(one, ((1, 0), (3, 1)), ((2, 0), (2, 1)), ((0, 1), (0, 2)))
    two = call(after_one, panel, first, second, e, kt_high, kt_low)
    behind = send(two, ((3, 1), (3, 2)), ((0, 1), (0, 3)))
    known = send(two, ((2, 1), (3, 2), (2, 2)))
    t, back = call(turn, [panel] * 2, known, behind, e, kt_high, kt_low, k_high, k_low)
    into = send(back, ((3, 2), (2, 1)))
    near = send(t, ((3, 2), (3, 1)))
    far = send(t, ((3, 2), (3, 0)))
    t, back, mixed = call(back_two, [panel] * 3, into, near, far, t, two, k_high, k_low, *at_zero[:2])
    into = send(back, ((2, 1), (1, 0)), ((3, 0), (2, 0)))
    other = send(mixed, ((3, 1), (1, 0)), ((2, 1), (2, 0)))
    t, back = call(back_one, [panel] * 2, into, other, t, one, *at_zero[:2])
    near = {
        ((1, 0), (0, 3)): (3, 0),
        ((1, 0), (0, 2)): (1, 1),
        ((2, 0), (0, 3)): (2, 1),
        ((2, 0), (0, 2)): (3, 1),
    }
    into = [None] * planes
    spread = [None] * planes
    for plane in reversed(range(planes)):
        moves = [((1, 0), (0, plane)), ((2, 0), (0, (plane + 1) % planes))]
        into[plane] = send(
            back, *((*move, near[move]) if move in near else move for move in moves)
        )
    for step in reversed(range(1, planes)):
        moves = [((1, 0), (1, step))]
        if 1 + step < planes:
            moves.append(((2, 1), (2, 1 + step)))
        if 2 + step < planes:
            moves.append(((3, 2), (3, 2 + step)))
        spread[step] = send(t, *moves)
    t = call(collect, panel, first, e, second, behind, *into, t, *spread[1:])
    return call(finish, struct((count, height), BF16), t, swap(t), diag_inv)


def chain_solve(partial_fit, factor, diag_inv):
    count, height = partial_fit.shape
    breadth = factor.shape[1]
    block_size = diag_inv.shape[1]
    rows_aux = lax.axis_size("aux")
    total = height * rows_aux
    members = rows_aux // SOLVE_BLOCKS
    my_row = lax.axis_index("aux")
    my_column = lax.axis_index("pair")
    my_block = my_row // members
    column_block = (my_column * breadth + jnp.arange(breadth, dtype=jnp.int32)) // block_size
    factor_low = jnp.where((column_block < my_block)[None, :], factor, 0.0)

    def own_columns(whole):
        return lax.dynamic_slice_in_dim(whole, my_column * breadth, breadth, 1)

    zero_block = jnp.zeros((count, block_size), jnp.float32)
    solved = jnp.zeros((count, total), jnp.float32)
    for k in range(SOLVE_BLOCKS):

        def on_group(current):
            return mm(partial_fit - mm_t(own_columns(current), factor_low), diag_inv)

        def off_group(current):
            return zero_block

        summand = lax.cond(my_block == k, on_group, off_group, solved)
        arrived = lax.psum(summand, AXES)
        solved = lax.dynamic_update_slice_in_dim(solved, arrived, k * block_size, 1)
    own_coef = jnp.zeros((count, height), jnp.float32)
    contrib = jnp.zeros((count, total), jnp.float32)
    for target in reversed(range(SOLVE_BLOCKS)):
        settled = solved[:, target * block_size : (target + 1) * block_size]
        if target < SOLVE_BLOCKS - 1:
            portion = contrib[:, target * block_size : (target + 1) * block_size]
            settled = settled - lax.psum(portion, AXES)

        def on_group(state):
            coef = mm_t(settled, diag_inv)
            if target > 0:
                fresh = lax.dynamic_update_slice_in_dim(
                    jnp.zeros((count, total), jnp.float32),
                    mm(coef, factor_low),
                    my_column * breadth,
                    1,
                )
            else:
                fresh = state[1]
            return (coef, fresh)

        def keep_state(state):
            return state

        own_coef, contrib = lax.cond(my_block == target, on_group, keep_state, (own_coef, contrib))
    return own_coef.astype(jnp.bfloat16)


def shards(integrals, densities, screen, factor, diag_inv):
    block_size = diag_inv.shape[1]
    chip_blocks = (
        lax.axis_size("aux") == 2 * SOLVE_BLOCKS
        and factor.shape[1] == block_size
        and lax.axis_size("pair") == SOLVE_BLOCKS
    )
    solve = chip_solve if chip_blocks else chain_solve
    left, right, partial_fit = fit_partial(densities, integrals, screen)
    rounded = solve(partial_fit, factor, diag_inv)
    if chip_blocks:
        return chip_coulomb(rounded, left, right, screen)
    return scatter_sum(coulomb_partial(rounded, left, right, screen))


def solution(mesh):
    in_specs = (
        P("aux", "pair"),
        P(None, "pair"),
        P("aux", "pair"),
        P("aux", "pair"),
        P("aux", None),
    )
    out_specs = P(None, ("pair", "aux"))
    return jax.shard_map(shards, mesh=mesh, in_specs=in_specs, out_specs=out_specs, check_vma=False)
```

```python
import functools

import jax
import jax.numpy as jnp
from jax import lax
from jax.experimental import pallas as pl
from jax.experimental.pallas import tpu as pltpu
from jax.sharding import PartitionSpec as P

TILE = 128
SOLVE_BLOCKS = 4
AXES = ("aux", "pair")
HIGHEST = lax.Precision.HIGHEST
F32 = jnp.float32
BF16 = jnp.bfloat16
VMEM = pl.BlockSpec(memory_space=pltpu.VMEM)
SMEM = pl.BlockSpec(memory_space=pltpu.SMEM)
HBM = pl.BlockSpec(memory_space=pltpu.HBM)
MIB = 1024 * 1024
NN = (((1,), (0,)), ((), ()))
NT = (((1,), (1,)), ((), ()))
TN = (((0,), (0,)), ((), ()))


def struct(shape, dtype=F32):
    return jax.ShapeDtypeStruct(shape, dtype)


def call(kernel, outs, *operands, limit=12, specs=None, scratch=()):
    return pl.pallas_call(
        kernel,
        out_shape=outs,
        in_specs=specs or [VMEM] * len(operands),
        out_specs=jax.tree.map(lambda _: VMEM, outs),
        scratch_shapes=scratch,
        compiler_params=pltpu.CompilerParams(vmem_limit_bytes=limit * MIB),
    )(*operands)


def side_of():
    return lax.rem(lax.axis_index("aux"), 2)


def block_of():
    return lax.div(lax.axis_index("aux"), 2)


def masked_row(screen, densities, i, tiles):
    zero = jnp.zeros((), densities.dtype)
    return jnp.concatenate(
        [
            jnp.where(screen[i, t] != 0, densities[:, t * TILE : (t + 1) * TILE], zero)
            for t in tiles
        ],
        axis=1,
    )


def fit(
    screen_in, densities_in, integrals, left, right, out, screen, densities, total, arrived
):
    height, width = integrals.shape
    pieces = arrived.shape[0] - 2
    chunk = width // pieces
    small = [
        pltpu.make_async_copy(screen_in, screen, arrived.at[pieces]),
        pltpu.make_async_copy(densities_in, densities, arrived.at[pieces + 1]),
    ]
    copies = []
    held = []
    for j in range(pieces):
        ref = left if 2 * j < pieces else right
        start = j * chunk if ref is left else j * chunk - width // 2
        held.append(ref.at[:, start : start + chunk])
        copies.append(
            pltpu.make_async_copy(
                integrals.at[:, j * chunk : (j + 1) * chunk], held[j], arrived.at[j]
            )
        )
    for copy in small + copies:
        copy.start()
    total[...] = jnp.zeros_like(total)
    for copy in small:
        copy.wait()
    count = densities.shape[0]
    strips = height // TILE
    for j in range(pieces):
        tiles = range(j * chunk // TILE, (j + 1) * chunk // TILE)
        stacked = jnp.concatenate([masked_row(screen, densities, i, tiles) for i in range(strips)])
        copies[j].wait()
        total[...] += lax.dot_general(held[j][...], stacked, NT, preferred_element_type=F32)
    done = total[...].T
    for i in range(strips):
        out[:, i * TILE : (i + 1) * TILE] = done[
            i * count : (i + 1) * count, i * TILE : (i + 1) * TILE
        ]


def fit_partial(densities, integrals, screen):
    count = densities.shape[0]
    height, width = integrals.shape
    pieces = 4 if width % (4 * TILE) == 0 else width // TILE
    return call(
        fit,
        [struct((height, width // 2), BF16)] * 2 + [struct((count, height))],
        *(pltpu.with_memory_space_constraint(x, pltpu.HBM) for x in (screen, densities, integrals)),
        specs=[HBM] * 3,
        scratch=[
            pltpu.SMEM(screen.shape, jnp.int32),
            pltpu.VMEM(densities.shape, BF16),
            pltpu.VMEM((height, height // TILE * count), F32),
            pltpu.SemaphoreType.DMA((pieces + 2,)),
        ],
    )


def slab(screen, stacked, left, right, member, members):
    strips = left.shape[0] // TILE
    count = stacked.shape[0] // strips
    chunk = 2 * left.shape[1] // members
    held, first = (left, member) if 2 * member < members else (right, member - members // 2)
    columns = slice(first * chunk, (first + 1) * chunk)
    parts = jnp.dot(stacked, held[:, columns], preferred_element_type=F32)
    tiles = []
    for t in range(chunk // TILE):
        total = jnp.zeros((count, TILE), F32)
        for i in range(strips):
            part = parts[i * count : (i + 1) * count, t * TILE : (t + 1) * TILE]
            total += jnp.where(screen[i, member * (chunk // TILE) + t] != 0, part, 0.0)
        tiles.append(total)
    return jnp.concatenate(tiles, axis=1)


def by_strip(value, strips):
    strip_of = lax.broadcasted_iota(jnp.int32, value.shape, 1) // TILE
    return jnp.concatenate(
        [jnp.where(strip_of == i, value, jnp.zeros((), BF16)) for i in range(strips)]
    )


def coulomb(screen, rounded, left, right, out):
    members = out.shape[0]
    stacked = by_strip(rounded[...], left.shape[0] // TILE)
    for m in range(members):
        out[m] = slab(screen, stacked, left, right, m, members).astype(out.dtype)


def coulomb_side(wanted, screen, rounded, left, right, out):
    chips = out.shape[0]
    stacked = by_strip(rounded[...], left.shape[0] // TILE)

    def compute(side):
        for k in range(chips):
            part = slab(screen, stacked, left, right, 2 * k + side, 2 * chips)
            out[k] = part.astype(out.dtype)

    for side in range(2):
        pl.when(wanted == side)(functools.partial(compute, side))


def coulomb_mate(*refs):
    coulomb_side(1 - side_of(), *refs)


def coulomb_own(*refs):
    coulomb_side(side_of(), *refs)


def share(own, got, keep, one, two, three):
    block = block_of()
    keep[...] = own[block] + got[block].astype(F32)
    for distance, out in ((1, one), (2, two), (3, three)):
        chip = lax.bitwise_xor(block, distance)
        out[...] = (own[chip] + got[chip].astype(F32)).astype(out.dtype)


def gather_up(keep, one, two, three, out):
    out[...] = keep[...] + one[...].astype(F32) + two[...].astype(F32) + three[...].astype(F32)


def coulomb_partial(rounded, left, right, screen):
    members = lax.axis_size("aux")
    out = struct((members, rounded.shape[0], 2 * left.shape[1] // members), BF16)
    return call(coulomb, out, screen, rounded, left, right, specs=[SMEM, VMEM, VMEM, VMEM])


def chip_coulomb(rounded, left, right, screen):
    members = 2 * SOLVE_BLOCKS
    count = rounded.shape[0]
    chunk = 2 * left.shape[1] // members
    specs = [SMEM, VMEM, VMEM, VMEM]
    operands = (screen, rounded, left, right)
    given = call(coulomb_mate, struct((SOLVE_BLOCKS, count, chunk), BF16), *operands, specs=specs)

    def move(value, to):
        return lax.ppermute(value, "aux", [(i, to(i)) for i in range(members)])

    got = move(given, lambda i: i ^ 1)
    own = call(coulomb_own, struct((SOLVE_BLOCKS, count, chunk)), *operands, specs=specs)
    piece = struct((count, chunk), BF16)
    keep, one, two, three = call(share, [struct((count, chunk))] + [piece] * 3, own, got)
    three = move(three, lambda i: i ^ 6)
    one = move(one, lambda i: i ^ 2)
    two = move(two, lambda i: i ^ 4)
    return call(gather_up, struct((count, chunk)), keep, one, two, three)


def scatter_sum(slabs):
    arrived = lax.all_to_all(slabs, "aux", 0, 0, tiled=True)
    return jnp.sum(arrived.astype(F32), axis=0)


def high_low(value):
    high = value.astype(BF16)
    return high, (value - high.astype(F32)).astype(BF16)


def times(value, high, low, dims=NN):
    rows = value.shape[0]
    coarse = value.astype(BF16).astype(F32)
    pair = jnp.concatenate([coarse, value - coarse], axis=0).astype(BF16)
    both = lax.dot_general(pair, high, dims, preferred_element_type=F32)
    both += lax.dot_general(pair, low, dims, preferred_element_type=F32)
    return both[:rows] + both[rows:]


def prepare_first(*refs):
    here = (block_of() == 0) | (lax.axis_index("pair") > 0)
    prepare(here, *refs)


def prepare_later(*refs):
    prepare(lax.axis_index("pair") == 0, *refs)


def prepare(here, inv0, inv1, fac0, fac1, k_high, k_low, kt_high, kt_low, lhs, rhs):
    height = inv0.shape[0]

    @pl.when(here & (block_of() > 0) & (side_of() == 0))
    def _():
        for n, (inv, fac) in enumerate(((inv0, fac0), (inv1, fac1))):
            rows = [slice((3 * n + r) * height, (3 * n + r + 1) * height) for r in range(3)]
            high, low = high_low(inv[...])
            lhs[rows[0], :], lhs[rows[1], :], lhs[rows[2], :] = high, low, high
            high, low = high_low(fac[...])
            rhs[rows[0], :], rhs[rows[1], :], rhs[rows[2], :] = high, high, low
        depth = 3 * height
        halves = (
            (slice(0, height), slice(0, depth)),
            (slice(height, 2 * height), slice(0, 2 * depth)),
        )
        for part, used in halves:
            product = lax.dot_general(lhs[used, part], rhs[used, :], TN, preferred_element_type=F32)
            k_high[part, :], k_low[part, :] = high_low(product)
            kt_high[:, part], kt_low[:, part] = high_low(product.T)


def begin(f0, f1, f2, f3, inv, after, out):
    high, low = high_low(inv[...])
    out[...] = times(f0[...] + f1[...] + f2[...] + f3[...], high, low)


def both(own, mate, out):
    out[...] = own[...] + mate[...]


def lead_only(kernel):
    @functools.wraps(kernel)
    def guarded(*refs):
        pl.when(side_of() == 0)(lambda: kernel(*refs))

    return guarded


@lead_only
def after_zero(one, two, three, e, high, low, out):
    block = block_of()
    known = jnp.where(block == 1, one[...], jnp.where(block == 2, two[...], three[...]))
    term = times(known, high[...], low[...])
    out[...] = jnp.where(block == 0, e[...], jnp.where(block == 1, two[...] - term, term))


@lead_only
def after_one(first, second, e, high, low, out):
    block = block_of()
    known = jnp.where(block == 3, second[...], first[...])
    behind = jnp.where(block == 3, first[...], second[...])
    total = behind + times(known, high[...], low[...])
    out[...] = jnp.where(block == 0, e[...], jnp.where(block == 3, total, e[...] - total))


@lead_only
def turn(known, behind, e, kt_high, kt_low, high, low, settled, back):
    value = e[...] - behind[...] - times(known[...], kt_high[...], kt_low[...])
    settled[...] = value
    back[...] = times(value, high[...], low[...])


@lead_only
def back_two(into, near, far, t, s, high, low, high0, low0, settled, back, mixed):
    plane = lax.axis_index("pair")
    last = block_of() == 3
    passed = jnp.where(plane == 0, far[...], jnp.where(plane == 1, near[...], t[...]))
    value = jnp.where(last, passed, s[...] - into[...])
    settled[...] = value

    def multiply(high, low):
        product = times(value, high[...], low[...])
        back[...] = product
        mixed[...] = jnp.where(last, product, value)

    pl.when(plane == 0)(lambda: multiply(high0, low0))
    pl.when(plane > 0)(lambda: multiply(high, low))


@lead_only
def back_one(into, other, t, s, high, low, settled, back):
    plane = lax.axis_index("pair")
    block = block_of()
    passed = jnp.where(plane == 0, other[...], t[...])
    value = jnp.where(
        block == 1,
        s[...] - into[...] - other[...],
        jnp.where(block == 2, passed, t[...]),
    )
    settled[...] = value
    product = times(value, high[...], low[...])
    back[...] = jnp.where(block == 2, product + into[...], product)


def collect(z0, z1, z2, z3, i0, i1, i2, i3, t, p1, p2, p3, out):
    plane = lax.axis_index("pair")
    block = block_of()

    def by_plane(a, b, c, d):
        return jnp.where(
            plane == 0, a[...], jnp.where(plane == 1, b[...], jnp.where(plane == 2, c[...], d[...]))
        )

    start = by_plane(z0, z1, z2, z3)
    zero = start - by_plane(i0, i1, i2, i3) - by_plane(i3, i0, i1, i2)
    one = by_plane(t, p1, p2, p3)
    two = by_plane(t, t, p1, p2)
    three = by_plane(t, t, t, p1)
    out[...] = jnp.where(
        block == 0, zero, jnp.where(block == 1, one, jnp.where(block == 2, two, three))
    )


def finish(own, mate, inv, out):
    value = jnp.where(side_of() == 0, own[...], mate[...])
    high, low = high_low(inv[...])
    out[...] = times(value, high, low, NT).astype(out.dtype)


def mm(a, b):
    return jnp.dot(a, b, precision=HIGHEST, preferred_element_type=F32)


def mm_t(a, b):
    return lax.dot_general(a, b, NT, precision=HIGHEST, preferred_element_type=F32)


def chip_solve(partial_fit, factor, diag_inv):
    count, height = partial_fit.shape
    size = 2 * height
    planes = lax.axis_size("pair")
    chips = [(k, plane) for k in range(SOLVE_BLOCKS) for plane in range(planes)]

    def device(chip, c):
        return (2 * chip[0] + c) * planes + chip[1]

    def permute(value, to):
        for chip in chips:
            for c in range(2):
                to.setdefault(device(chip, c), device(chip, 1 - c))
        return lax.ppermute(value, AXES, sorted(to.items()))

    def send(value, *moves):
        to = {}
        for source, target, *via in moves:
            loop = [device(source, 0), device(target, 0), device(target, 1)]
            for chip in via:
                loop += [device(chip, 0), device(chip, 1)]
            loop.append(device(source, 1))
            to.update(zip(loop, loop[1:] + loop[:1]))
        return permute(value, to)

    def swap(value):
        return lax.ppermute(value, "aux", [(i, i ^ 1) for i in range(2 * SOLVE_BLOCKS)])

    panel = struct((count, size))
    square = struct((size, size), BF16)
    home = [1, 1, 1, 2]
    gathered = []
    for route in ("far", "other", "middle"):
        to = {}
        for k in range(SOLVE_BLOCKS):
            turn_to = 1 if home[k] < 2 else -1
            middle, far, other = home[k] + turn_to, home[k] + 2 * turn_to, home[k] - turn_to
            ring = {"far": (far, home[k], middle), "middle": (middle, home[k]), "other": (other, home[k])}
            for c in range(2):
                loop = [device((k, plane), c) for plane in ring[route]]
                to.update(zip(loop, loop[1:] + loop[:1]))
        gathered.append(permute(partial_fit, to))
    halves = (diag_inv, permute(diag_inv, {}), factor, permute(factor, {}))

    def prepared(kernel):
        scratch = [pltpu.VMEM((3 * size, size), BF16)] * 2
        return call(kernel, [square] * 4, *halves, limit=32, scratch=scratch)

    k_high, k_low, kt_high, kt_low = prepared(prepare_first)
    at_zero = prepared(prepare_later)
    e = call(begin, panel, partial_fit, *gathered, diag_inv, k_high)
    e = call(both, panel, e, swap(e))
    reach = [
        send(e, ((0, 1), (1, 0))),
        send(e, ((0, 1), (2, 0)), ((1, 1), (1, 0))),
        send(e, ((0, 1), (3, 0))),
    ]
    one = call(after_zero, panel, *reach, e, *at_zero[2:])
    first = send(one, ((1, 0), (2, 1)), ((3, 0), (3, 1)), ((0, 1), (0, 0)))
    second = send(one, ((1, 0), (3, 1)), ((2, 0), (2, 1)), ((0, 1), (0, 2)))
    two = call(after_one, panel, first, second, e, kt_high, kt_low)
    behind = send(two, ((3, 1), (3, 2)), ((0, 1), (0, 3)))
    known = send(two, ((2, 1), (3, 2), (2, 2)))
    t, back = call(turn, [panel] * 2, known, behind, e, kt_high, kt_low, k_high, k_low)
    into = send(back, ((3, 2), (2, 1)))
    near = send(t, ((3, 2), (3, 1)))
    far = send(t, ((3, 2), (3, 0)))
    t, back, mixed = call(back_two, [panel] * 3, into, near, far, t, two, k_high, k_low, *at_zero[:2])
    into = send(back, ((2, 1), (1, 0)), ((3, 0), (2, 0)))
    other = send(mixed, ((3, 1), (1, 0)), ((2, 1), (2, 0)))
    t, back = call(back_one, [panel] * 2, into, other, t, one, *at_zero[:2])
    near = {
        ((1, 0), (0, 3)): (3, 0),
        ((1, 0), (0, 2)): (1, 1),
        ((2, 0), (0, 3)): (2, 1),
        ((2, 0), (0, 2)): (3, 1),
        ((2, 0), (0, 0)): (2, 2),
    }
    into = [None] * planes
    spread = [None] * planes

    def spread_to(step):
        moves = [((1, 0), (1, step))]
        if 1 + step < planes:
            moves.append(((2, 1), (2, 1 + step)))
        if 2 + step < planes:
            moves.append(((3, 2), (3, 2 + step)))
        spread[step] = send(t, *moves)

    spread_to(planes - 1)
    for plane in reversed(range(planes)):
        moves = [((1, 0), (0, plane)), ((2, 0), (0, (plane + 1) % planes))]
        into[plane] = send(
            back, *((*move, near[move]) if move in near else move for move in moves)
        )
    for step in reversed(range(1, planes - 1)):
        spread_to(step)
    t = call(collect, panel, first, e, second, behind, *into, t, *spread[1:])
    return call(finish, struct((count, height), BF16), t, swap(t), diag_inv)


def chain_solve(partial_fit, factor, diag_inv):
    count, height = partial_fit.shape
    breadth = factor.shape[1]
    block_size = diag_inv.shape[1]
    rows_aux = lax.axis_size("aux")
    total = height * rows_aux
    members = rows_aux // SOLVE_BLOCKS
    my_row = lax.axis_index("aux")
    my_column = lax.axis_index("pair")
    my_block = my_row // members
    column_block = (my_column * breadth + jnp.arange(breadth, dtype=jnp.int32)) // block_size
    factor_low = jnp.where((column_block < my_block)[None, :], factor, 0.0)

    def own_columns(whole):
        return lax.dynamic_slice_in_dim(whole, my_column * breadth, breadth, 1)

    zero_block = jnp.zeros((count, block_size), jnp.float32)
    solved = jnp.zeros((count, total), jnp.float32)
    for k in range(SOLVE_BLOCKS):

        def on_group(current):
            return mm(partial_fit - mm_t(own_columns(current), factor_low), diag_inv)

        def off_group(current):
            return zero_block

        summand = lax.cond(my_block == k, on_group, off_group, solved)
        arrived = lax.psum(summand, AXES)
        solved = lax.dynamic_update_slice_in_dim(solved, arrived, k * block_size, 1)
    own_coef = jnp.zeros((count, height), jnp.float32)
    contrib = jnp.zeros((count, total), jnp.float32)
    for target in reversed(range(SOLVE_BLOCKS)):
        settled = solved[:, target * block_size : (target + 1) * block_size]
        if target < SOLVE_BLOCKS - 1:
            portion = contrib[:, target * block_size : (target + 1) * block_size]
            settled = settled - lax.psum(portion, AXES)

        def on_group(state):
            coef = mm_t(settled, diag_inv)
            if target > 0:
                fresh = lax.dynamic_update_slice_in_dim(
                    jnp.zeros((count, total), jnp.float32),
                    mm(coef, factor_low),
                    my_column * breadth,
                    1,
                )
            else:
                fresh = state[1]
            return (coef, fresh)

        def keep_state(state):
            return state

        own_coef, contrib = lax.cond(my_block == target, on_group, keep_state, (own_coef, contrib))
    return own_coef.astype(jnp.bfloat16)


def shards(integrals, densities, screen, factor, diag_inv):
    block_size = diag_inv.shape[1]
    chip_blocks = (
        lax.axis_size("aux") == 2 * SOLVE_BLOCKS
        and factor.shape[1] == block_size
        and lax.axis_size("pair") == SOLVE_BLOCKS
    )
    solve = chip_solve if chip_blocks else chain_solve
    left, right, partial_fit = fit_partial(densities, integrals, screen)
    rounded = solve(partial_fit, factor, diag_inv)
    if chip_blocks:
        return chip_coulomb(rounded, left, right, screen)
    return scatter_sum(coulomb_partial(rounded, left, right, screen))


def solution(mesh):
    in_specs = (
        P("aux", "pair"),
        P(None, "pair"),
        P("aux", "pair"),
        P("aux", "pair"),
        P("aux", None),
    )
    out_specs = P(None, ("pair", "aux"))
    return jax.shard_map(shards, mesh=mesh, in_specs=in_specs, out_specs=out_specs, check_vma=False)
```

```python
import functools

import jax
import jax.numpy as jnp
from jax import lax
from jax.experimental import pallas as pl
from jax.experimental.pallas import tpu as pltpu
from jax.sharding import PartitionSpec as P

TILE = 128
SOLVE_BLOCKS = 4
AXES = ("aux", "pair")
HIGHEST = lax.Precision.HIGHEST
F32 = jnp.float32
BF16 = jnp.bfloat16
VMEM = pl.BlockSpec(memory_space=pltpu.VMEM)
SMEM = pl.BlockSpec(memory_space=pltpu.SMEM)
HBM = pl.BlockSpec(memory_space=pltpu.HBM)
MIB = 1024 * 1024
NN = (((1,), (0,)), ((), ()))
NT = (((1,), (1,)), ((), ()))
TN = (((0,), (0,)), ((), ()))


def struct(shape, dtype=F32):
    return jax.ShapeDtypeStruct(shape, dtype)


def call(kernel, outs, *operands, limit=12, specs=None, scratch=()):
    return pl.pallas_call(
        kernel,
        out_shape=outs,
        in_specs=specs or [VMEM] * len(operands),
        out_specs=jax.tree.map(lambda _: VMEM, outs),
        scratch_shapes=scratch,
        compiler_params=pltpu.CompilerParams(vmem_limit_bytes=limit * MIB),
    )(*operands)


def side_of():
    return lax.rem(lax.axis_index("aux"), 2)


def block_of():
    return lax.div(lax.axis_index("aux"), 2)


def masked_row(screen, densities, i, tiles):
    zero = jnp.zeros((), densities.dtype)
    return jnp.concatenate(
        [
            jnp.where(screen[i, t] != 0, densities[:, t * TILE : (t + 1) * TILE], zero)
            for t in tiles
        ],
        axis=1,
    )


def fit(
    screen_in, densities_in, integrals, left, right, out, screen, densities, total, arrived
):
    height, width = integrals.shape
    pieces = arrived.shape[0] - 2
    chunk = width // pieces
    small = [
        pltpu.make_async_copy(screen_in, screen, arrived.at[pieces]),
        pltpu.make_async_copy(densities_in, densities, arrived.at[pieces + 1]),
    ]
    copies = []
    held = []
    for j in range(pieces):
        ref = left if 2 * j < pieces else right
        start = j * chunk if ref is left else j * chunk - width // 2
        held.append(ref.at[:, start : start + chunk])
        copies.append(
            pltpu.make_async_copy(
                integrals.at[:, j * chunk : (j + 1) * chunk], held[j], arrived.at[j]
            )
        )
    for copy in small + copies:
        copy.start()
    total[...] = jnp.zeros_like(total)
    for copy in small:
        copy.wait()
    count = densities.shape[0]
    strips = height // TILE
    for j in range(pieces):
        tiles = range(j * chunk // TILE, (j + 1) * chunk // TILE)
        stacked = jnp.concatenate([masked_row(screen, densities, i, tiles) for i in range(strips)])
        copies[j].wait()
        total[...] += lax.dot_general(held[j][...], stacked, NT, preferred_element_type=F32)
    done = total[...].T
    for i in range(strips):
        out[:, i * TILE : (i + 1) * TILE] = done[
            i * count : (i + 1) * count, i * TILE : (i + 1) * TILE
        ]


def fit_partial(densities, integrals, screen):
    count = densities.shape[0]
    height, width = integrals.shape
    pieces = 4 if width % (4 * TILE) == 0 else width // TILE
    return call(
        fit,
        [struct((height, width // 2), BF16)] * 2 + [struct((count, height))],
        *(pltpu.with_memory_space_constraint(x, pltpu.HBM) for x in (screen, densities, integrals)),
        specs=[HBM] * 3,
        scratch=[
            pltpu.SMEM(screen.shape, jnp.int32),
            pltpu.VMEM(densities.shape, BF16),
            pltpu.VMEM((height, height // TILE * count), F32),
            pltpu.SemaphoreType.DMA((pieces + 2,)),
        ],
    )


def slab(screen, stacked, left, right, member, members):
    strips = left.shape[0] // TILE
    count = stacked.shape[0] // strips
    chunk = 2 * left.shape[1] // members
    held, first = (left, member) if 2 * member < members else (right, member - members // 2)
    columns = slice(first * chunk, (first + 1) * chunk)
    parts = jnp.dot(stacked, held[:, columns], preferred_element_type=F32)
    tiles = []
    for t in range(chunk // TILE):
        total = jnp.zeros((count, TILE), F32)
        for i in range(strips):
            part = parts[i * count : (i + 1) * count, t * TILE : (t + 1) * TILE]
            total += jnp.where(screen[i, member * (chunk // TILE) + t] != 0, part, 0.0)
        tiles.append(total)
    return jnp.concatenate(tiles, axis=1)


def by_strip(value, strips):
    strip_of = lax.broadcasted_iota(jnp.int32, value.shape, 1) // TILE
    return jnp.concatenate(
        [jnp.where(strip_of == i, value, jnp.zeros((), BF16)) for i in range(strips)]
    )


def coulomb(screen, rounded, left, right, out):
    members = out.shape[0]
    stacked = by_strip(rounded[...], left.shape[0] // TILE)
    for m in range(members):
        out[m] = slab(screen, stacked, left, right, m, members).astype(out.dtype)


def coulomb_side(wanted, screen, rounded, left, right, out):
    chips = out.shape[0]
    stacked = by_strip(rounded[...], left.shape[0] // TILE)

    def compute(side):
        for k in range(chips):
            part = slab(screen, stacked, left, right, 2 * k + side, 2 * chips)
            out[k] = part.astype(out.dtype)

    for side in range(2):
        pl.when(wanted == side)(functools.partial(compute, side))


def coulomb_mate(*refs):
    coulomb_side(1 - side_of(), *refs)


def coulomb_own(*refs):
    coulomb_side(side_of(), *refs)


def share(own, got, keep, one, two, three):
    block = block_of()
    keep[...] = own[block] + got[block].astype(F32)
    for distance, out in ((1, one), (2, two), (3, three)):
        chip = lax.bitwise_xor(block, distance)
        out[...] = (own[chip] + got[chip].astype(F32)).astype(out.dtype)


def gather_up(keep, one, two, three, out):
    out[...] = keep[...] + one[...].astype(F32) + two[...].astype(F32) + three[...].astype(F32)


def coulomb_partial(rounded, left, right, screen):
    members = lax.axis_size("aux")
    out = struct((members, rounded.shape[0], 2 * left.shape[1] // members), BF16)
    return call(coulomb, out, screen, rounded, left, right, specs=[SMEM, VMEM, VMEM, VMEM])


def chip_coulomb(rounded, left, right, screen):
    members = 2 * SOLVE_BLOCKS
    count = rounded.shape[0]
    chunk = 2 * left.shape[1] // members
    specs = [SMEM, VMEM, VMEM, VMEM]
    operands = (screen, rounded, left, right)
    given = call(coulomb_mate, struct((SOLVE_BLOCKS, count, chunk), BF16), *operands, specs=specs)

    def move(value, to):
        return lax.ppermute(value, "aux", [(i, to(i)) for i in range(members)])

    got = move(given, lambda i: i ^ 1)
    own = call(coulomb_own, struct((SOLVE_BLOCKS, count, chunk)), *operands, specs=specs)
    piece = struct((count, chunk), BF16)
    keep, one, two, three = call(share, [struct((count, chunk))] + [piece] * 3, own, got)
    three = move(three, lambda i: i ^ 6)
    one = move(one, lambda i: i ^ 2)
    two = move(two, lambda i: i ^ 4)
    return call(gather_up, struct((count, chunk)), keep, one, two, three)


def scatter_sum(slabs):
    arrived = lax.all_to_all(slabs, "aux", 0, 0, tiled=True)
    return jnp.sum(arrived.astype(F32), axis=0)


def high_low(value):
    high = value.astype(BF16)
    return high, (value - high.astype(F32)).astype(BF16)


def times(value, high, low, dims=NN):
    rows = value.shape[0]
    coarse = value.astype(BF16).astype(F32)
    pair = jnp.concatenate([coarse, value - coarse], axis=0).astype(BF16)
    both = lax.dot_general(pair, high, dims, preferred_element_type=F32)
    both += lax.dot_general(pair, low, dims, preferred_element_type=F32)
    return both[:rows] + both[rows:]


def leads_block():
    return (block_of() > 0) & (side_of() == 0)


def prepare_first(inv0, inv1, fac0, fac1, k_high, k_low, kt_high, kt_low, lhs, rhs):
    height = inv0.shape[0]

    @pl.when(leads_block())
    def _():
        for n, (inv, fac) in enumerate(((inv0, fac0), (inv1, fac1))):
            rows = [slice((3 * n + r) * height, (3 * n + r + 1) * height) for r in range(3)]
            high, low = high_low(inv[...])
            lhs[rows[0], :], lhs[rows[1], :], lhs[rows[2], :] = high, low, high
            high, low = high_low(fac[...])
            rhs[rows[0], :], rhs[rows[1], :], rhs[rows[2], :] = high, high, low

    @pl.when(leads_block() & (lax.axis_index("pair") > 0))
    def _():
        multiply_up(lhs, rhs, k_high, k_low, kt_high, kt_low)


def prepare_later(*refs):
    pl.when(leads_block() & (lax.axis_index("pair") == 0))(lambda: multiply_up(*refs))


def multiply_up(lhs, rhs, k_high, k_low, kt_high, kt_low):
    depth, size = lhs.shape[0] // 2, lhs.shape[1]
    parts = (
        (slice(0, size // 2), slice(0, depth)),
        (slice(size // 2, size), slice(0, 2 * depth)),
    )
    for part, used in parts:
        product = lax.dot_general(lhs[used, part], rhs[used, :], TN, preferred_element_type=F32)
        k_high[part, :], k_low[part, :] = high_low(product)
        kt_high[:, part], kt_low[:, part] = high_low(product.T)


def begin(f0, f1, f2, f3, inv, after, out):
    high, low = high_low(inv[...])
    out[...] = times(f0[...] + f1[...] + f2[...] + f3[...], high, low)


def both(own, mate, out):
    out[...] = own[...] + mate[...]


def lead_only(kernel):
    @functools.wraps(kernel)
    def guarded(*refs):
        pl.when(side_of() == 0)(lambda: kernel(*refs))

    return guarded


@lead_only
def after_zero(one, two, three, e, high, low, out):
    block = block_of()
    known = jnp.where(block == 1, one[...], jnp.where(block == 2, two[...], three[...]))
    term = times(known, high[...], low[...])
    out[...] = jnp.where(block == 0, e[...], jnp.where(block == 1, two[...] - term, term))


@lead_only
def after_one(first, second, e, high, low, out):
    block = block_of()
    known = jnp.where(block == 3, second[...], first[...])
    behind = jnp.where(block == 3, first[...], second[...])
    total = behind + times(known, high[...], low[...])
    out[...] = jnp.where(block == 0, e[...], jnp.where(block == 3, total, e[...] - total))


@lead_only
def turn(known, behind, e, kt_high, kt_low, high, low, settled, back):
    value = e[...] - behind[...] - times(known[...], kt_high[...], kt_low[...])
    settled[...] = value
    back[...] = times(value, high[...], low[...])


@lead_only
def back_two(into, near, far, t, s, high, low, high0, low0, settled, back, mixed):
    plane = lax.axis_index("pair")
    last = block_of() == 3
    passed = jnp.where(plane == 0, far[...], jnp.where(plane == 1, near[...], t[...]))
    value = jnp.where(last, passed, s[...] - into[...])
    settled[...] = value

    def multiply(high, low):
        product = times(value, high[...], low[...])
        back[...] = product
        mixed[...] = jnp.where(last, product, value)

    pl.when(plane == 0)(lambda: multiply(high0, low0))
    pl.when(plane > 0)(lambda: multiply(high, low))


@lead_only
def back_one(into, other, t, s, high, low, settled, back):
    plane = lax.axis_index("pair")
    block = block_of()
    passed = jnp.where(plane == 0, other[...], t[...])
    value = jnp.where(
        block == 1,
        s[...] - into[...] - other[...],
        jnp.where(block == 2, passed, t[...]),
    )
    settled[...] = value
    product = times(value, high[...], low[...])
    back[...] = jnp.where(block == 2, product + into[...], product)


def collect(z0, z1, z2, z3, i0, i1, i2, i3, t, p1, p2, p3, out):
    plane = lax.axis_index("pair")
    block = block_of()

    def by_plane(a, b, c, d):
        return jnp.where(
            plane == 0, a[...], jnp.where(plane == 1, b[...], jnp.where(plane == 2, c[...], d[...]))
        )

    start = by_plane(z0, z1, z2, z3)
    zero = start - by_plane(i0, i1, i2, i3) - by_plane(i3, i0, i1, i2)
    one = by_plane(t, p1, p2, p3)
    two = by_plane(t, t, p1, p2)
    three = by_plane(t, t, t, p1)
    out[...] = jnp.where(
        block == 0, zero, jnp.where(block == 1, one, jnp.where(block == 2, two, three))
    )


def finish(own, mate, inv, out):
    value = jnp.where(side_of() == 0, own[...], mate[...])
    high, low = high_low(inv[...])
    out[...] = times(value, high, low, NT).astype(out.dtype)


def mm(a, b):
    return jnp.dot(a, b, precision=HIGHEST, preferred_element_type=F32)


def mm_t(a, b):
    return lax.dot_general(a, b, NT, precision=HIGHEST, preferred_element_type=F32)


def chip_solve(partial_fit, factor, diag_inv):
    count, height = partial_fit.shape
    size = 2 * height
    planes = lax.axis_size("pair")
    chips = [(k, plane) for k in range(SOLVE_BLOCKS) for plane in range(planes)]

    def device(chip, c):
        return (2 * chip[0] + c) * planes + chip[1]

    def permute(value, to):
        for chip in chips:
            for c in range(2):
                to.setdefault(device(chip, c), device(chip, 1 - c))
        return lax.ppermute(value, AXES, sorted(to.items()))

    def send(value, *moves):
        to = {}
        for source, target, *via in moves:
            loop = [device(source, 0), device(target, 0), device(target, 1)]
            for chip in via:
                loop += [device(chip, 0), device(chip, 1)]
            loop.append(device(source, 1))
            to.update(zip(loop, loop[1:] + loop[:1]))
        return permute(value, to)

    def swap(value):
        return lax.ppermute(value, "aux", [(i, i ^ 1) for i in range(2 * SOLVE_BLOCKS)])

    panel = struct((count, size))
    square = struct((size, size), BF16)
    halves = (diag_inv, swap(diag_inv), factor, swap(factor))

    stacked = struct((3 * size, size), BF16)
    k_high, k_low, kt_high, kt_low, *pairs = call(
        prepare_first, [square] * 4 + [stacked] * 2, *halves, limit=24
    )
    at_zero = call(prepare_later, [square] * 4, *pairs, limit=24)
    home = [1, 1, 1, 2]
    gathered = []
    for route in ("far", "other", "middle"):
        to = {}
        for k in range(SOLVE_BLOCKS):
            turn_to = 1 if home[k] < 2 else -1
            middle, far, other = home[k] + turn_to, home[k] + 2 * turn_to, home[k] - turn_to
            ring = {"far": (far, home[k], middle), "middle": (middle, home[k]), "other": (other, home[k])}
            for c in range(2):
                loop = [device((k, plane), c) for plane in ring[route]]
                to.update(zip(loop, loop[1:] + loop[:1]))
        gathered.append(permute(partial_fit, to))
    e = call(begin, panel, partial_fit, *gathered, diag_inv, k_high)
    e = call(both, panel, e, swap(e))
    reach = [
        send(e, ((0, 1), (1, 0))),
        send(e, ((0, 1), (2, 0)), ((1, 1), (1, 0))),
        send(e, ((0, 1), (3, 0))),
    ]
    one = call(after_zero, panel, *reach, e, *at_zero[2:])
    first = send(one, ((1, 0), (2, 1)), ((3, 0), (3, 1)), ((0, 1), (0, 0)))
    second = send(one, ((1, 0), (3, 1)), ((2, 0), (2, 1)), ((0, 1), (0, 2)))
    two = call(after_one, panel, first, second, e, kt_high, kt_low)
    behind = send(two, ((3, 1), (3, 2)), ((0, 1), (0, 3)))
    known = send(two, ((2, 1), (3, 2), (2, 2)))
    t, back = call(turn, [panel] * 2, known, behind, e, kt_high, kt_low, k_high, k_low)
    into = send(back, ((3, 2), (2, 1)))
    near = send(t, ((3, 2), (3, 1)))
    far = send(t, ((3, 2), (3, 0)))
    t, back, mixed = call(back_two, [panel] * 3, into, near, far, t, two, k_high, k_low, *at_zero[:2])
    into = send(back, ((2, 1), (1, 0)), ((3, 0), (2, 0)))
    other = send(mixed, ((3, 1), (1, 0)), ((2, 1), (2, 0)))
    t, back = call(back_one, [panel] * 2, into, other, t, one, *at_zero[:2])
    near = {
        ((1, 0), (0, 3)): (3, 0),
        ((1, 0), (0, 2)): (1, 1),
        ((2, 0), (0, 3)): (2, 1),
        ((2, 0), (0, 2)): (3, 1),
        ((2, 0), (0, 0)): (2, 2),
    }
    into = [None] * planes
    spread = [None] * planes

    def spread_to(step):
        moves = [((1, 0), (1, step))]
        if 1 + step < planes:
            moves.append(((2, 1), (2, 1 + step)))
        if 2 + step < planes:
            moves.append(((3, 2), (3, 2 + step)))
        spread[step] = send(t, *moves)

    spread_to(planes - 1)
    for plane in reversed(range(planes)):
        moves = [((1, 0), (0, plane)), ((2, 0), (0, (plane + 1) % planes))]
        into[plane] = send(
            back, *((*move, near[move]) if move in near else move for move in moves)
        )
    for step in reversed(range(1, planes - 1)):
        spread_to(step)
    t = call(collect, panel, first, e, second, behind, *into, t, *spread[1:])
    return call(finish, struct((count, height), BF16), t, swap(t), diag_inv)


def chain_solve(partial_fit, factor, diag_inv):
    count, height = partial_fit.shape
    breadth = factor.shape[1]
    block_size = diag_inv.shape[1]
    rows_aux = lax.axis_size("aux")
    total = height * rows_aux
    members = rows_aux // SOLVE_BLOCKS
    my_row = lax.axis_index("aux")
    my_column = lax.axis_index("pair")
    my_block = my_row // members
    column_block = (my_column * breadth + jnp.arange(breadth, dtype=jnp.int32)) // block_size
    factor_low = jnp.where((column_block < my_block)[None, :], factor, 0.0)

    def own_columns(whole):
        return lax.dynamic_slice_in_dim(whole, my_column * breadth, breadth, 1)

    zero_block = jnp.zeros((count, block_size), jnp.float32)
    solved = jnp.zeros((count, total), jnp.float32)
    for k in range(SOLVE_BLOCKS):

        def on_group(current):
            return mm(partial_fit - mm_t(own_columns(current), factor_low), diag_inv)

        def off_group(current):
            return zero_block

        summand = lax.cond(my_block == k, on_group, off_group, solved)
        arrived = lax.psum(summand, AXES)
        solved = lax.dynamic_update_slice_in_dim(solved, arrived, k * block_size, 1)
    own_coef = jnp.zeros((count, height), jnp.float32)
    contrib = jnp.zeros((count, total), jnp.float32)
    for target in reversed(range(SOLVE_BLOCKS)):
        settled = solved[:, target * block_size : (target + 1) * block_size]
        if target < SOLVE_BLOCKS - 1:
            portion = contrib[:, target * block_size : (target + 1) * block_size]
            settled = settled - lax.psum(portion, AXES)

        def on_group(state):
            coef = mm_t(settled, diag_inv)
            if target > 0:
                fresh = lax.dynamic_update_slice_in_dim(
                    jnp.zeros((count, total), jnp.float32),
                    mm(coef, factor_low),
                    my_column * breadth,
                    1,
                )
            else:
                fresh = state[1]
            return (coef, fresh)

        def keep_state(state):
            return state

        own_coef, contrib = lax.cond(my_block == target, on_group, keep_state, (own_coef, contrib))
    return own_coef.astype(jnp.bfloat16)


def shards(integrals, densities, screen, factor, diag_inv):
    block_size = diag_inv.shape[1]
    chip_blocks = (
        lax.axis_size("aux") == 2 * SOLVE_BLOCKS
        and factor.shape[1] == block_size
        and lax.axis_size("pair") == SOLVE_BLOCKS
    )
    solve = chip_solve if chip_blocks else chain_solve
    left, right, partial_fit = fit_partial(densities, integrals, screen)
    rounded = solve(partial_fit, factor, diag_inv)
    if chip_blocks:
        return chip_coulomb(rounded, left, right, screen)
    return scatter_sum(coulomb_partial(rounded, left, right, screen))


def solution(mesh):
    in_specs = (
        P("aux", "pair"),
        P(None, "pair"),
        P("aux", "pair"),
        P("aux", "pair"),
        P("aux", None),
    )
    out_specs = P(None, ("pair", "aux"))
    return jax.shard_map(shards, mesh=mesh, in_specs=in_specs, out_specs=out_specs, check_vma=False)
```

```python
import functools

import jax
import jax.numpy as jnp
from jax import lax
from jax.experimental import pallas as pl
from jax.experimental.pallas import tpu as pltpu
from jax.sharding import PartitionSpec as P

TILE = 128
SOLVE_BLOCKS = 4
AXES = ("aux", "pair")
HIGHEST = lax.Precision.HIGHEST
F32 = jnp.float32
BF16 = jnp.bfloat16
VMEM = pl.BlockSpec(memory_space=pltpu.VMEM)
SMEM = pl.BlockSpec(memory_space=pltpu.SMEM)
HBM = pl.BlockSpec(memory_space=pltpu.HBM)
MIB = 1024 * 1024
NN = (((1,), (0,)), ((), ()))
NT = (((1,), (1,)), ((), ()))
TN = (((0,), (0,)), ((), ()))


def struct(shape, dtype=F32):
    return jax.ShapeDtypeStruct(shape, dtype)


def call(kernel, outs, *operands, limit=12, specs=None, scratch=()):
    return pl.pallas_call(
        kernel,
        out_shape=outs,
        in_specs=specs or [VMEM] * len(operands),
        out_specs=jax.tree.map(lambda _: VMEM, outs),
        scratch_shapes=scratch,
        compiler_params=pltpu.CompilerParams(vmem_limit_bytes=limit * MIB),
    )(*operands)


def side_of():
    return lax.rem(lax.axis_index("aux"), 2)


def block_of():
    return lax.div(lax.axis_index("aux"), 2)


def masked_row(screen, densities, i, tiles):
    zero = jnp.zeros((), densities.dtype)
    return jnp.concatenate(
        [
            jnp.where(screen[i, t] != 0, densities[:, t * TILE : (t + 1) * TILE], zero)
            for t in tiles
        ],
        axis=1,
    )


def fit(
    screen_in, densities_in, integrals, left, right, out, screen, densities, total, arrived
):
    height, width = integrals.shape
    pieces = arrived.shape[0] - 2
    chunk = width // pieces
    small = [
        pltpu.make_async_copy(screen_in, screen, arrived.at[pieces]),
        pltpu.make_async_copy(densities_in, densities, arrived.at[pieces + 1]),
    ]
    copies = []
    held = []
    for j in range(pieces):
        ref = left if 2 * j < pieces else right
        start = j * chunk if ref is left else j * chunk - width // 2
        held.append(ref.at[:, start : start + chunk])
        copies.append(
            pltpu.make_async_copy(
                integrals.at[:, j * chunk : (j + 1) * chunk], held[j], arrived.at[j]
            )
        )
    for copy in small + copies:
        copy.start()
    total[...] = jnp.zeros_like(total)
    for copy in small:
        copy.wait()
    count = densities.shape[0]
    strips = height // TILE
    for j in range(pieces):
        tiles = range(j * chunk // TILE, (j + 1) * chunk // TILE)
        stacked = jnp.concatenate([masked_row(screen, densities, i, tiles) for i in range(strips)])
        copies[j].wait()
        total[...] += lax.dot_general(held[j][...], stacked, NT, preferred_element_type=F32)
    done = total[...].T
    for i in range(strips):
        out[:, i * TILE : (i + 1) * TILE] = done[
            i * count : (i + 1) * count, i * TILE : (i + 1) * TILE
        ]


def fit_partial(densities, integrals, screen):
    count = densities.shape[0]
    height, width = integrals.shape
    pieces = 4 if width % (4 * TILE) == 0 else width // TILE
    return call(
        fit,
        [struct((height, width // 2), BF16)] * 2 + [struct((count, height))],
        *(pltpu.with_memory_space_constraint(x, pltpu.HBM) for x in (screen, densities, integrals)),
        specs=[HBM] * 3,
        scratch=[
            pltpu.SMEM(screen.shape, jnp.int32),
            pltpu.VMEM(densities.shape, BF16),
            pltpu.VMEM((height, height // TILE * count), F32),
            pltpu.SemaphoreType.DMA((pieces + 2,)),
        ],
    )


def slab(screen, stacked, left, right, member, members):
    strips = left.shape[0] // TILE
    count = stacked.shape[0] // strips
    chunk = 2 * left.shape[1] // members
    held, first = (left, member) if 2 * member < members else (right, member - members // 2)
    columns = slice(first * chunk, (first + 1) * chunk)
    parts = jnp.dot(stacked, held[:, columns], preferred_element_type=F32)
    tiles = []
    for t in range(chunk // TILE):
        total = jnp.zeros((count, TILE), F32)
        for i in range(strips):
            part = parts[i * count : (i + 1) * count, t * TILE : (t + 1) * TILE]
            total += jnp.where(screen[i, member * (chunk // TILE) + t] != 0, part, 0.0)
        tiles.append(total)
    return jnp.concatenate(tiles, axis=1)


def by_strip(value, strips):
    strip_of = lax.broadcasted_iota(jnp.int32, value.shape, 1) // TILE
    return jnp.concatenate(
        [jnp.where(strip_of == i, value, jnp.zeros((), BF16)) for i in range(strips)]
    )


def coulomb(screen, rounded, left, right, out):
    members = out.shape[0]
    stacked = by_strip(rounded[...], left.shape[0] // TILE)
    for m in range(members):
        out[m] = slab(screen, stacked, left, right, m, members).astype(out.dtype)


def coulomb_side(wanted, screen, rounded, left, right, out):
    chips = out.shape[0]
    stacked = by_strip(rounded[...], left.shape[0] // TILE)

    def compute(side):
        for k in range(chips):
            part = slab(screen, stacked, left, right, 2 * k + side, 2 * chips)
            out[k] = part.astype(out.dtype)

    for side in range(2):
        pl.when(wanted == side)(functools.partial(compute, side))


def coulomb_mate(*refs):
    coulomb_side(1 - side_of(), *refs)


def coulomb_own(*refs):
    coulomb_side(side_of(), *refs)


def share(own, got, keep, one, two, three):
    block = block_of()
    keep[...] = own[block] + got[block].astype(F32)
    for distance, out in ((1, one), (2, two), (3, three)):
        chip = lax.bitwise_xor(block, distance)
        out[...] = (own[chip] + got[chip].astype(F32)).astype(out.dtype)


def gather_up(keep, one, two, three, out):
    out[...] = keep[...] + one[...].astype(F32) + two[...].astype(F32) + three[...].astype(F32)


def coulomb_partial(rounded, left, right, screen):
    members = lax.axis_size("aux")
    out = struct((members, rounded.shape[0], 2 * left.shape[1] // members), BF16)
    return call(coulomb, out, screen, rounded, left, right, specs=[SMEM, VMEM, VMEM, VMEM])


def chip_coulomb(rounded, left, right, screen):
    members = 2 * SOLVE_BLOCKS
    count = rounded.shape[0]
    chunk = 2 * left.shape[1] // members
    specs = [SMEM, VMEM, VMEM, VMEM]
    operands = (screen, rounded, left, right)
    given = call(coulomb_mate, struct((SOLVE_BLOCKS, count, chunk), BF16), *operands, specs=specs)

    def move(value, to):
        return lax.ppermute(value, "aux", [(i, to(i)) for i in range(members)])

    got = move(given, lambda i: i ^ 1)
    own = call(coulomb_own, struct((SOLVE_BLOCKS, count, chunk)), *operands, specs=specs)
    piece = struct((count, chunk), BF16)
    keep, one, two, three = call(share, [struct((count, chunk))] + [piece] * 3, own, got)
    three = move(three, lambda i: i ^ 6)
    one = move(one, lambda i: i ^ 2)
    two = move(two, lambda i: i ^ 4)
    return call(gather_up, struct((count, chunk)), keep, one, two, three)


def scatter_sum(slabs):
    arrived = lax.all_to_all(slabs, "aux", 0, 0, tiled=True)
    return jnp.sum(arrived.astype(F32), axis=0)


def high_low(value):
    high = value.astype(BF16)
    return high, (value - high.astype(F32)).astype(BF16)


def times(value, high, low, dims=NN):
    rows = value.shape[0]
    coarse = value.astype(BF16).astype(F32)
    pair = jnp.concatenate([coarse, value - coarse], axis=0).astype(BF16)
    both = lax.dot_general(pair, high, dims, preferred_element_type=F32)
    both += lax.dot_general(pair, low, dims, preferred_element_type=F32)
    return both[:rows] + both[rows:]


def prepare_first(*refs):
    prepare(lax.axis_index("pair") > 0, *refs)


def prepare_later(*refs):
    prepare(lax.axis_index("pair") == 0, *refs)


def prepare(here, inv0, inv1, fac0, fac1, k_high, k_low, kt_high, kt_low, lhs, rhs):
    height = inv0.shape[0]

    @pl.when(here & (lax.axis_index("pair") < block_of()) & (side_of() == 0))
    def _():
        for n, (inv, fac) in enumerate(((inv0, fac0), (inv1, fac1))):
            rows = [slice((3 * n + r) * height, (3 * n + r + 1) * height) for r in range(3)]
            high, low = high_low(inv[...])
            lhs[rows[0], :], lhs[rows[1], :], lhs[rows[2], :] = high, low, high
            high, low = high_low(fac[...])
            rhs[rows[0], :], rhs[rows[1], :], rhs[rows[2], :] = high, high, low
        depth = 3 * height
        halves = (
            (slice(0, height), slice(0, depth)),
            (slice(height, 2 * height), slice(0, 2 * depth)),
        )
        for part, used in halves:
            product = lax.dot_general(lhs[used, part], rhs[used, :], TN, preferred_element_type=F32)
            k_high[part, :], k_low[part, :] = high_low(product)
            kt_high[:, part], kt_low[:, part] = high_low(product.T)


def begin(f0, f1, f2, f3, inv, after, out):
    high, low = high_low(inv[...])
    out[...] = times(f0[...] + f1[...] + f2[...] + f3[...], high, low)


def both(own, mate, out):
    out[...] = own[...] + mate[...]


def lead_only(kernel):
    @functools.wraps(kernel)
    def guarded(*refs):
        pl.when(side_of() == 0)(lambda: kernel(*refs))

    return guarded


@lead_only
def after_zero(one, two, three, e, high, low, out):
    block = block_of()
    known = jnp.where(block == 1, one[...], jnp.where(block == 2, two[...], three[...]))
    term = times(known, high[...], low[...])
    out[...] = jnp.where(block == 0, e[...], jnp.where(block == 1, two[...] - term, term))


@lead_only
def after_one(first, second, e, high, low, out):
    block = block_of()
    known = jnp.where(block == 3, second[...], first[...])
    behind = jnp.where(block == 3, first[...], second[...])
    total = behind + times(known, high[...], low[...])
    out[...] = jnp.where(block == 0, e[...], jnp.where(block == 3, total, e[...] - total))


@lead_only
def turn(known, behind, e, kt_high, kt_low, high, low, settled, back):
    value = e[...] - behind[...] - times(known[...], kt_high[...], kt_low[...])
    settled[...] = value
    back[...] = times(value, high[...], low[...])


@lead_only
def back_two(into, near, far, t, s, high, low, high0, low0, settled, back, mixed):
    plane = lax.axis_index("pair")
    last = block_of() == 3
    passed = jnp.where(plane == 0, far[...], jnp.where(plane == 1, near[...], t[...]))
    value = jnp.where(last, passed, s[...] - into[...])
    settled[...] = value

    def multiply(high, low):
        product = times(value, high[...], low[...])
        back[...] = product
        mixed[...] = jnp.where(last, product, value)

    pl.when(plane == 0)(lambda: multiply(high0, low0))
    pl.when(plane > 0)(lambda: multiply(high, low))


@lead_only
def back_one(into, other, t, s, high, low, settled, back):
    plane = lax.axis_index("pair")
    block = block_of()
    passed = jnp.where(plane == 0, other[...], t[...])
    value = jnp.where(
        block == 1,
        s[...] - into[...] - other[...],
        jnp.where(block == 2, passed, t[...]),
    )
    settled[...] = value
    product = times(value, high[...], low[...])
    back[...] = jnp.where(block == 2, product + into[...], product)


def collect(z0, z1, z2, z3, i0, i1, i2, i3, t, p1, p2, p3, out):
    plane = lax.axis_index("pair")
    block = block_of()

    def by_plane(a, b, c, d):
        return jnp.where(
            plane == 0, a[...], jnp.where(plane == 1, b[...], jnp.where(plane == 2, c[...], d[...]))
        )

    start = by_plane(z0, z1, z2, z3)
    zero = start - by_plane(i0, i1, i2, i3) - by_plane(i3, i0, i1, i2)
    one = by_plane(t, p1, p2, p3)
    two = by_plane(t, t, p1, p2)
    three = by_plane(t, t, t, p1)
    out[...] = jnp.where(
        block == 0, zero, jnp.where(block == 1, one, jnp.where(block == 2, two, three))
    )


def finish(own, mate, inv, out):
    value = jnp.where(side_of() == 0, own[...], mate[...])
    high, low = high_low(inv[...])
    out[...] = times(value, high, low, NT).astype(out.dtype)


def mm(a, b):
    return jnp.dot(a, b, precision=HIGHEST, preferred_element_type=F32)


def mm_t(a, b):
    return lax.dot_general(a, b, NT, precision=HIGHEST, preferred_element_type=F32)


def chip_solve(partial_fit, factor, diag_inv):
    count, height = partial_fit.shape
    size = 2 * height
    planes = lax.axis_size("pair")
    chips = [(k, plane) for k in range(SOLVE_BLOCKS) for plane in range(planes)]

    def device(chip, c):
        return (2 * chip[0] + c) * planes + chip[1]

    def permute(value, to):
        for chip in chips:
            for c in range(2):
                to.setdefault(device(chip, c), device(chip, 1 - c))
        return lax.ppermute(value, AXES, sorted(to.items()))

    def send(value, *moves):
        to = {}
        for source, target, *via in moves:
            loop = [device(source, 0), device(target, 0), device(target, 1)]
            for chip in via:
                loop += [device(chip, 0), device(chip, 1)]
            loop.append(device(source, 1))
            to.update(zip(loop, loop[1:] + loop[:1]))
        return permute(value, to)

    def swap(value):
        return lax.ppermute(value, "aux", [(i, i ^ 1) for i in range(2 * SOLVE_BLOCKS)])

    panel = struct((count, size))
    square = struct((size, size), BF16)
    halves = (diag_inv, swap(diag_inv), factor, swap(factor))

    def prepared(kernel):
        scratch = [pltpu.VMEM((3 * size, size), BF16)] * 2
        return call(kernel, [square] * 4, *halves, limit=32, scratch=scratch)

    k_high, k_low, kt_high, kt_low = prepared(prepare_first)
    at_zero = prepared(prepare_later)
    home = [1, 1, 1, 2]
    gathered = []
    for route in ("far", "other", "middle"):
        to = {}
        for k in range(SOLVE_BLOCKS):
            turn_to = 1 if home[k] < 2 else -1
            middle, far, other = home[k] + turn_to, home[k] + 2 * turn_to, home[k] - turn_to
            ring = {"far": (far, home[k], middle), "middle": (middle, home[k]), "other": (other, home[k])}
            for c in range(2):
                loop = [device((k, plane), c) for plane in ring[route]]
                to.update(zip(loop, loop[1:] + loop[:1]))
        gathered.append(permute(partial_fit, to))
    e = call(begin, panel, partial_fit, *gathered, diag_inv, k_high)
    e = call(both, panel, e, swap(e))
    reach = [
        send(e, ((0, 1), (1, 0))),
        send(e, ((0, 1), (2, 0)), ((1, 1), (1, 0))),
        send(e, ((0, 1), (3, 0))),
    ]
    one = call(after_zero, panel, *reach, e, *at_zero[2:])
    first = send(one, ((1, 0), (2, 1)), ((3, 0), (3, 1)), ((0, 1), (0, 0)))
    second = send(one, ((1, 0), (3, 1)), ((2, 0), (2, 1)), ((0, 1), (0, 2)))
    two = call(after_one, panel, first, second, e, kt_high, kt_low)
    behind = send(two, ((3, 1), (3, 2)), ((0, 1), (0, 3)))
    known = send(two, ((2, 1), (3, 2), (2, 2)))
    t, back = call(turn, [panel] * 2, known, behind, e, kt_high, kt_low, k_high, k_low)
    into = send(back, ((3, 2), (2, 1)))
    near = send(t, ((3, 2), (3, 1)))
    far = send(t, ((3, 2), (3, 0)))
    t, back, mixed = call(back_two, [panel] * 3, into, near, far, t, two, k_high, k_low, *at_zero[:2])
    into = send(back, ((2, 1), (1, 0)), ((3, 0), (2, 0)))
    other = send(mixed, ((3, 1), (1, 0)), ((2, 1), (2, 0)))
    t, back = call(back_one, [panel] * 2, into, other, t, one, *at_zero[:2])
    near = {
        ((1, 0), (0, 3)): (3, 0),
        ((1, 0), (0, 2)): (1, 1),
        ((2, 0), (0, 3)): (2, 1),
        ((2, 0), (0, 2)): (3, 1),
        ((2, 0), (0, 0)): (2, 2),
    }
    into = [None] * planes
    spread = [None] * planes

    def spread_to(step):
        moves = [((1, 0), (1, step))]
        if 1 + step < planes:
            moves.append(((2, 1), (2, 1 + step)))
        if 2 + step < planes:
            moves.append(((3, 2), (3, 2 + step)))
        spread[step] = send(t, *moves)

    spread_to(planes - 1)
    for plane in reversed(range(planes)):
        moves = [((1, 0), (0, plane)), ((2, 0), (0, (plane + 1) % planes))]
        into[plane] = send(
            back, *((*move, near[move]) if move in near else move for move in moves)
        )
    for step in reversed(range(1, planes - 1)):
        spread_to(step)
    t = call(collect, panel, first, e, second, behind, *into, t, *spread[1:])
    return call(finish, struct((count, height), BF16), t, swap(t), diag_inv)


def chain_solve(partial_fit, factor, diag_inv):
    count, height = partial_fit.shape
    breadth = factor.shape[1]
    block_size = diag_inv.shape[1]
    rows_aux = lax.axis_size("aux")
    total = height * rows_aux
    members = rows_aux // SOLVE_BLOCKS
    my_row = lax.axis_index("aux")
    my_column = lax.axis_index("pair")
    my_block = my_row // members
    column_block = (my_column * breadth + jnp.arange(breadth, dtype=jnp.int32)) // block_size
    factor_low = jnp.where((column_block < my_block)[None, :], factor, 0.0)

    def own_columns(whole):
        return lax.dynamic_slice_in_dim(whole, my_column * breadth, breadth, 1)

    zero_block = jnp.zeros((count, block_size), jnp.float32)
    solved = jnp.zeros((count, total), jnp.float32)
    for k in range(SOLVE_BLOCKS):

        def on_group(current):
            return mm(partial_fit - mm_t(own_columns(current), factor_low), diag_inv)

        def off_group(current):
            return zero_block

        summand = lax.cond(my_block == k, on_group, off_group, solved)
        arrived = lax.psum(summand, AXES)
        solved = lax.dynamic_update_slice_in_dim(solved, arrived, k * block_size, 1)
    own_coef = jnp.zeros((count, height), jnp.float32)
    contrib = jnp.zeros((count, total), jnp.float32)
    for target in reversed(range(SOLVE_BLOCKS)):
        settled = solved[:, target * block_size : (target + 1) * block_size]
        if target < SOLVE_BLOCKS - 1:
            portion = contrib[:, target * block_size : (target + 1) * block_size]
            settled = settled - lax.psum(portion, AXES)

        def on_group(state):
            coef = mm_t(settled, diag_inv)
            if target > 0:
                fresh = lax.dynamic_update_slice_in_dim(
                    jnp.zeros((count, total), jnp.float32),
                    mm(coef, factor_low),
                    my_column * breadth,
                    1,
                )
            else:
                fresh = state[1]
            return (coef, fresh)

        def keep_state(state):
            return state

        own_coef, contrib = lax.cond(my_block == target, on_group, keep_state, (own_coef, contrib))
    return own_coef.astype(jnp.bfloat16)


def shards(integrals, densities, screen, factor, diag_inv):
    block_size = diag_inv.shape[1]
    chip_blocks = (
        lax.axis_size("aux") == 2 * SOLVE_BLOCKS
        and factor.shape[1] == block_size
        and lax.axis_size("pair") == SOLVE_BLOCKS
    )
    solve = chip_solve if chip_blocks else chain_solve
    left, right, partial_fit = fit_partial(densities, integrals, screen)
    rounded = solve(partial_fit, factor, diag_inv)
    if chip_blocks:
        return chip_coulomb(rounded, left, right, screen)
    return scatter_sum(coulomb_partial(rounded, left, right, screen))


def solution(mesh):
    in_specs = (
        P("aux", "pair"),
        P(None, "pair"),
        P("aux", "pair"),
        P("aux", "pair"),
        P("aux", None),
    )
    out_specs = P(None, ("pair", "aux"))
    return jax.shard_map(shards, mesh=mesh, in_specs=in_specs, out_specs=out_specs, check_vma=False)
```

```python
import functools

import jax
import jax.numpy as jnp
from jax import lax
from jax.experimental import pallas as pl
from jax.experimental.pallas import tpu as pltpu
from jax.sharding import PartitionSpec as P

TILE = 128
SOLVE_BLOCKS = 4
AXES = ("aux", "pair")
HIGHEST = lax.Precision.HIGHEST
F32 = jnp.float32
BF16 = jnp.bfloat16
VMEM = pl.BlockSpec(memory_space=pltpu.VMEM)
HBM = pl.BlockSpec(memory_space=pltpu.HBM)
MIB = 1024 * 1024
NN = (((1,), (0,)), ((), ()))
NT = (((1,), (1,)), ((), ()))
TN = (((0,), (0,)), ((), ()))


def struct(shape, dtype=F32):
    return jax.ShapeDtypeStruct(shape, dtype)


def call(kernel, outs, *operands, limit=12, specs=None, scratch=()):
    return pl.pallas_call(
        kernel,
        out_shape=outs,
        in_specs=specs or [VMEM] * len(operands),
        out_specs=jax.tree.map(lambda _: VMEM, outs),
        scratch_shapes=scratch,
        compiler_params=pltpu.CompilerParams(vmem_limit_bytes=limit * MIB),
    )(*operands)


def side_of():
    return lax.rem(lax.axis_index("aux"), 2)


def block_of():
    return lax.div(lax.axis_index("aux"), 2)


def masked_row(screen, densities, i, tiles):
    zero = jnp.zeros((), densities.dtype)
    return jnp.concatenate(
        [
            jnp.where(screen[i, t] != 0, densities[:, t * TILE : (t + 1) * TILE], zero)
            for t in tiles
        ],
        axis=1,
    )


def fit(
    screen_in, densities_in, integrals, left, right, out, masks, screen, densities, total, arrived
):
    height, width = integrals.shape
    pieces = arrived.shape[0] - 2
    chunk = width // pieces
    small = [
        pltpu.make_async_copy(screen_in, screen, arrived.at[pieces]),
        pltpu.make_async_copy(densities_in, densities, arrived.at[pieces + 1]),
    ]
    copies = []
    held = []
    for j in range(pieces):
        ref = left if 2 * j < pieces else right
        start = j * chunk if ref is left else j * chunk - width // 2
        held.append(ref.at[:, start : start + chunk])
        copies.append(
            pltpu.make_async_copy(
                integrals.at[:, j * chunk : (j + 1) * chunk], held[j], arrived.at[j]
            )
        )
    for copy in small + copies:
        copy.start()
    total[...] = jnp.zeros_like(total)
    for copy in small:
        copy.wait()
    count = densities.shape[0]
    strips = height // TILE
    for i in range(strips):
        for t in range(width // TILE):
            flag = jnp.where(screen[i, t] != 0, 1.0, 0.0)
            masks[i : i + 1, t * TILE : (t + 1) * TILE] = jnp.full((1, TILE), flag, F32)
    for j in range(pieces):
        tiles = range(j * chunk // TILE, (j + 1) * chunk // TILE)
        stacked = jnp.concatenate([masked_row(screen, densities, i, tiles) for i in range(strips)])
        copies[j].wait()
        total[...] += lax.dot_general(held[j][...], stacked, NT, preferred_element_type=F32)
    done = total[...].T
    for i in range(strips):
        out[:, i * TILE : (i + 1) * TILE] = done[
            i * count : (i + 1) * count, i * TILE : (i + 1) * TILE
        ]


def fit_partial(densities, integrals, screen):
    count = densities.shape[0]
    height, width = integrals.shape
    pieces = 4 if width % (4 * TILE) == 0 else width // TILE
    return call(
        fit,
        [struct((height, width // 2), BF16)] * 2
        + [struct((count, height)), struct((height // TILE, width))],
        *(pltpu.with_memory_space_constraint(x, pltpu.HBM) for x in (screen, densities, integrals)),
        specs=[HBM] * 3,
        scratch=[
            pltpu.SMEM(screen.shape, jnp.int32),
            pltpu.VMEM(densities.shape, BF16),
            pltpu.VMEM((height, height // TILE * count), F32),
            pltpu.SemaphoreType.DMA((pieces + 2,)),
        ],
    )


def slab(masks, stacked, left, right, member, members):
    strips = left.shape[0] // TILE
    count = stacked.shape[0] // strips
    chunk = 2 * left.shape[1] // members
    held, first = (left, member) if 2 * member < members else (right, member - members // 2)
    columns = slice(first * chunk, (first + 1) * chunk)
    parts = jnp.dot(stacked, held[:, columns], preferred_element_type=F32)
    total = jnp.zeros((count, chunk), F32)
    for i in range(strips):
        mask = masks[i : i + 1, member * chunk : (member + 1) * chunk]
        total += jnp.where(mask != 0, parts[i * count : (i + 1) * count], 0.0)
    return total


def by_strip(value, strips):
    strip_of = lax.broadcasted_iota(jnp.int32, value.shape, 1) // TILE
    return jnp.concatenate(
        [jnp.where(strip_of == i, value, jnp.zeros((), BF16)) for i in range(strips)]
    )


def coulomb(masks, rounded, left, right, out):
    members = out.shape[0]
    stacked = by_strip(rounded[...], left.shape[0] // TILE)
    for m in range(members):
        out[m] = slab(masks, stacked, left, right, m, members).astype(out.dtype)


def coulomb_side(wanted, masks, rounded, left, right, out):
    chips = out.shape[0]
    stacked = by_strip(rounded[...], left.shape[0] // TILE)

    def compute(side):
        for k in range(chips):
            part = slab(masks, stacked, left, right, 2 * k + side, 2 * chips)
            out[k] = part.astype(out.dtype)

    for side in range(2):
        pl.when(wanted == side)(functools.partial(compute, side))


def coulomb_mate(*refs):
    coulomb_side(1 - side_of(), *refs)


def coulomb_own(*refs):
    coulomb_side(side_of(), *refs)


def share(own, got, keep, one, two, three):
    block = block_of()
    keep[...] = own[block] + got[block].astype(F32)
    for distance, out in ((1, one), (2, two), (3, three)):
        chip = lax.bitwise_xor(block, distance)
        out[...] = (own[chip] + got[chip].astype(F32)).astype(out.dtype)


def gather_up(keep, one, two, three, out):
    out[...] = keep[...] + one[...].astype(F32) + two[...].astype(F32) + three[...].astype(F32)


def coulomb_partial(rounded, left, right, masks):
    members = lax.axis_size("aux")
    out = struct((members, rounded.shape[0], 2 * left.shape[1] // members), BF16)
    return call(coulomb, out, masks, rounded, left, right)


def chip_coulomb(rounded, left, right, masks):
    members = 2 * SOLVE_BLOCKS
    count = rounded.shape[0]
    chunk = 2 * left.shape[1] // members
    operands = (masks, rounded, left, right)
    given = call(coulomb_mate, struct((SOLVE_BLOCKS, count, chunk), BF16), *operands)

    def move(value, to):
        return lax.ppermute(value, "aux", [(i, to(i)) for i in range(members)])

    got = move(given, lambda i: i ^ 1)
    own = call(coulomb_own, struct((SOLVE_BLOCKS, count, chunk)), *operands)
    piece = struct((count, chunk), BF16)
    keep, one, two, three = call(share, [struct((count, chunk))] + [piece] * 3, own, got)
    three = move(three, lambda i: i ^ 6)
    one = move(one, lambda i: i ^ 2)
    two = move(two, lambda i: i ^ 4)
    return call(gather_up, struct((count, chunk)), keep, one, two, three)


def scatter_sum(slabs):
    arrived = lax.all_to_all(slabs, "aux", 0, 0, tiled=True)
    return jnp.sum(arrived.astype(F32), axis=0)


def high_low(value):
    high = value.astype(BF16)
    return high, (value - high.astype(F32)).astype(BF16)


def times(value, high, low, dims=NN):
    rows = value.shape[0]
    coarse = value.astype(BF16).astype(F32)
    pair = jnp.concatenate([coarse, value - coarse], axis=0).astype(BF16)
    both = lax.dot_general(pair, high, dims, preferred_element_type=F32)
    both += lax.dot_general(pair, low, dims, preferred_element_type=F32)
    return both[:rows] + both[rows:]


def prepare_first(*refs):
    prepare(lax.axis_index("pair") > 0, *refs)


def prepare_later(*refs):
    prepare(lax.axis_index("pair") == 0, *refs)


def prepare(here, inv0, inv1, fac0, fac1, k_high, k_low, kt_high, kt_low, lhs, rhs):
    height = inv0.shape[0]

    @pl.when(here & (lax.axis_index("pair") < block_of()) & (side_of() == 0))
    def _():
        for n, (inv, fac) in enumerate(((inv0, fac0), (inv1, fac1))):
            rows = [slice((3 * n + r) * height, (3 * n + r + 1) * height) for r in range(3)]
            high, low = high_low(inv[...])
            lhs[rows[0], :], lhs[rows[1], :], lhs[rows[2], :] = high, low, high
            high, low = high_low(fac[...])
            rhs[rows[0], :], rhs[rows[1], :], rhs[rows[2], :] = high, high, low
        depth = 3 * height
        halves = (
            (slice(0, height), slice(0, depth)),
            (slice(height, 2 * height), slice(0, 2 * depth)),
        )
        for part, used in halves:
            product = lax.dot_general(lhs[used, part], rhs[used, :], TN, preferred_element_type=F32)
            k_high[part, :], k_low[part, :] = high_low(product)
            kt_high[:, part], kt_low[:, part] = high_low(product.T)


def begin(f0, f1, f2, f3, inv, after, out):
    high, low = high_low(inv[...])
    out[...] = times(f0[...] + f1[...] + f2[...] + f3[...], high, low)


def both(own, mate, out):
    out[...] = own[...] + mate[...]


def lead_only(kernel):
    @functools.wraps(kernel)
    def guarded(*refs):
        pl.when(side_of() == 0)(lambda: kernel(*refs))

    return guarded


@lead_only
def after_zero(one, two, three, e, high, low, out):
    block = block_of()
    known = jnp.where(block == 1, one[...], jnp.where(block == 2, two[...], three[...]))
    term = times(known, high[...], low[...])
    out[...] = jnp.where(block == 0, e[...], jnp.where(block == 1, two[...] - term, term))


@lead_only
def after_one(first, second, e, high, low, out):
    block = block_of()
    known = jnp.where(block == 3, second[...], first[...])
    behind = jnp.where(block == 3, first[...], second[...])
    total = behind + times(known, high[...], low[...])
    out[...] = jnp.where(block == 0, e[...], jnp.where(block == 3, total, e[...] - total))


@lead_only
def turn(known, behind, e, kt_high, kt_low, high, low, settled, back):
    value = e[...] - behind[...] - times(known[...], kt_high[...], kt_low[...])
    settled[...] = value
    back[...] = times(value, high[...], low[...])


@lead_only
def back_two(into, near, far, t, s, high, low, high0, low0, settled, back, mixed):
    plane = lax.axis_index("pair")
    last = block_of() == 3
    passed = jnp.where(plane == 0, far[...], jnp.where(plane == 1, near[...], t[...]))
    value = jnp.where(last, passed, s[...] - into[...])
    settled[...] = value

    def multiply(high, low):
        product = times(value, high[...], low[...])
        back[...] = product
        mixed[...] = jnp.where(last, product, value)

    pl.when(plane == 0)(lambda: multiply(high0, low0))
    pl.when(plane > 0)(lambda: multiply(high, low))


@lead_only
def back_one(into, other, t, s, high, low, settled, back):
    plane = lax.axis_index("pair")
    block = block_of()
    passed = jnp.where(plane == 0, other[...], t[...])
    value = jnp.where(
        block == 1,
        s[...] - into[...] - other[...],
        jnp.where(block == 2, passed, t[...]),
    )
    settled[...] = value
    product = times(value, high[...], low[...])
    back[...] = jnp.where(block == 2, product + into[...], product)


def collect(z0, z1, z2, z3, i0, i1, i2, i3, t, p1, p2, p3, out):
    plane = lax.axis_index("pair")
    block = block_of()

    def by_plane(a, b, c, d):
        return jnp.where(
            plane == 0, a[...], jnp.where(plane == 1, b[...], jnp.where(plane == 2, c[...], d[...]))
        )

    start = by_plane(z0, z1, z2, z3)
    zero = start - by_plane(i0, i1, i2, i3) - by_plane(i3, i0, i1, i2)
    one = by_plane(t, p1, p2, p3)
    two = by_plane(t, t, p1, p2)
    three = by_plane(t, t, t, p1)
    out[...] = jnp.where(
        block == 0, zero, jnp.where(block == 1, one, jnp.where(block == 2, two, three))
    )


def finish(own, mate, inv, out):
    value = jnp.where(side_of() == 0, own[...], mate[...])
    high, low = high_low(inv[...])
    out[...] = times(value, high, low, NT).astype(out.dtype)


def mm(a, b):
    return jnp.dot(a, b, precision=HIGHEST, preferred_element_type=F32)


def mm_t(a, b):
    return lax.dot_general(a, b, NT, precision=HIGHEST, preferred_element_type=F32)


def chip_solve(partial_fit, factor, diag_inv):
    count, height = partial_fit.shape
    size = 2 * height
    planes = lax.axis_size("pair")
    chips = [(k, plane) for k in range(SOLVE_BLOCKS) for plane in range(planes)]

    def device(chip, c):
        return (2 * chip[0] + c) * planes + chip[1]

    def permute(value, to):
        for chip in chips:
            for c in range(2):
                to.setdefault(device(chip, c), device(chip, 1 - c))
        return lax.ppermute(value, AXES, sorted(to.items()))

    def send(value, *moves):
        to = {}
        for source, target, *via in moves:
            loop = [device(source, 0), device(target, 0), device(target, 1)]
            for chip in via:
                loop += [device(chip, 0), device(chip, 1)]
            loop.append(device(source, 1))
            to.update(zip(loop, loop[1:] + loop[:1]))
        return permute(value, to)

    def swap(value):
        return lax.ppermute(value, "aux", [(i, i ^ 1) for i in range(2 * SOLVE_BLOCKS)])

    panel = struct((count, size))
    square = struct((size, size), BF16)
    halves = (diag_inv, swap(diag_inv), factor, swap(factor))

    def prepared(kernel):
        scratch = [pltpu.VMEM((3 * size, size), BF16)] * 2
        return call(kernel, [square] * 4, *halves, limit=32, scratch=scratch)

    k_high, k_low, kt_high, kt_low = prepared(prepare_first)
    at_zero = prepared(prepare_later)
    home = [1, 1, 1, 2]
    gathered = []
    for route in ("far", "other", "middle"):
        to = {}
        for k in range(SOLVE_BLOCKS):
            turn_to = 1 if home[k] < 2 else -1
            middle, far, other = home[k] + turn_to, home[k] + 2 * turn_to, home[k] - turn_to
            ring = {"far": (far, home[k], middle), "middle": (middle, home[k]), "other": (other, home[k])}
            for c in range(2):
                loop = [device((k, plane), c) for plane in ring[route]]
                to.update(zip(loop, loop[1:] + loop[:1]))
        gathered.append(permute(partial_fit, to))
    e = call(begin, panel, partial_fit, *gathered, diag_inv, k_high)
    e = call(both, panel, e, swap(e))
    reach = [
        send(e, ((0, 1), (1, 0))),
        send(e, ((0, 1), (2, 0)), ((1, 1), (1, 0))),
        send(e, ((0, 1), (3, 0))),
    ]
    one = call(after_zero, panel, *reach, e, *at_zero[2:])
    first = send(one, ((1, 0), (2, 1)), ((3, 0), (3, 1)), ((0, 1), (0, 0)))
    second = send(one, ((1, 0), (3, 1)), ((2, 0), (2, 1)), ((0, 1), (0, 2)))
    two = call(after_one, panel, first, second, e, kt_high, kt_low)
    behind = send(two, ((3, 1), (3, 2)), ((0, 1), (0, 3)))
    known = send(two, ((2, 1), (3, 2), (2, 2)))
    t, back = call(turn, [panel] * 2, known, behind, e, kt_high, kt_low, k_high, k_low)
    into = send(back, ((3, 2), (2, 1)))
    near = send(t, ((3, 2), (3, 1)))
    far = send(t, ((3, 2), (3, 0)))
    t, back, mixed = call(back_two, [panel] * 3, into, near, far, t, two, k_high, k_low, *at_zero[:2])
    into = send(back, ((2, 1), (1, 0)), ((3, 0), (2, 0)))
    other = send(mixed, ((3, 1), (1, 0)), ((2, 1), (2, 0)))
    t, back = call(back_one, [panel] * 2, into, other, t, one, *at_zero[:2])
    near = {
        ((1, 0), (0, 3)): (3, 0),
        ((1, 0), (0, 2)): (1, 1),
        ((2, 0), (0, 3)): (2, 1),
        ((2, 0), (0, 2)): (3, 1),
        ((2, 0), (0, 0)): (2, 2),
    }
    into = [None] * planes
    spread = [None] * planes

    def spread_to(step):
        moves = [((1, 0), (1, step))]
        if 1 + step < planes:
            moves.append(((2, 1), (2, 1 + step)))
        if 2 + step < planes:
            moves.append(((3, 2), (3, 2 + step)))
        spread[step] = send(t, *moves)

    spread_to(planes - 1)
    for plane in reversed(range(planes)):
        moves = [((1, 0), (0, plane)), ((2, 0), (0, (plane + 1) % planes))]
        into[plane] = send(
            back, *((*move, near[move]) if move in near else move for move in moves)
        )
    for step in reversed(range(1, planes - 1)):
        spread_to(step)
    t = call(collect, panel, first, e, second, behind, *into, t, *spread[1:])
    return call(finish, struct((count, height), BF16), t, swap(t), diag_inv)


def chain_solve(partial_fit, factor, diag_inv):
    count, height = partial_fit.shape
    breadth = factor.shape[1]
    block_size = diag_inv.shape[1]
    rows_aux = lax.axis_size("aux")
    total = height * rows_aux
    members = rows_aux // SOLVE_BLOCKS
    my_row = lax.axis_index("aux")
    my_column = lax.axis_index("pair")
    my_block = my_row // members
    column_block = (my_column * breadth + jnp.arange(breadth, dtype=jnp.int32)) // block_size
    factor_low = jnp.where((column_block < my_block)[None, :], factor, 0.0)

    def own_columns(whole):
        return lax.dynamic_slice_in_dim(whole, my_column * breadth, breadth, 1)

    zero_block = jnp.zeros((count, block_size), jnp.float32)
    solved = jnp.zeros((count, total), jnp.float32)
    for k in range(SOLVE_BLOCKS):

        def on_group(current):
            return mm(partial_fit - mm_t(own_columns(current), factor_low), diag_inv)

        def off_group(current):
            return zero_block

        summand = lax.cond(my_block == k, on_group, off_group, solved)
        arrived = lax.psum(summand, AXES)
        solved = lax.dynamic_update_slice_in_dim(solved, arrived, k * block_size, 1)
    own_coef = jnp.zeros((count, height), jnp.float32)
    contrib = jnp.zeros((count, total), jnp.float32)
    for target in reversed(range(SOLVE_BLOCKS)):
        settled = solved[:, target * block_size : (target + 1) * block_size]
        if target < SOLVE_BLOCKS - 1:
            portion = contrib[:, target * block_size : (target + 1) * block_size]
            settled = settled - lax.psum(portion, AXES)

        def on_group(state):
            coef = mm_t(settled, diag_inv)
            if target > 0:
                fresh = lax.dynamic_update_slice_in_dim(
                    jnp.zeros((count, total), jnp.float32),
                    mm(coef, factor_low),
                    my_column * breadth,
                    1,
                )
            else:
                fresh = state[1]
            return (coef, fresh)

        def keep_state(state):
            return state

        own_coef, contrib = lax.cond(my_block == target, on_group, keep_state, (own_coef, contrib))
    return own_coef.astype(jnp.bfloat16)


def shards(integrals, densities, screen, factor, diag_inv):
    block_size = diag_inv.shape[1]
    chip_blocks = (
        lax.axis_size("aux") == 2 * SOLVE_BLOCKS
        and factor.shape[1] == block_size
        and lax.axis_size("pair") == SOLVE_BLOCKS
    )
    solve = chip_solve if chip_blocks else chain_solve
    left, right, partial_fit, masks = fit_partial(densities, integrals, screen)
    rounded = solve(partial_fit, factor, diag_inv)
    if chip_blocks:
        return chip_coulomb(rounded, left, right, masks)
    return scatter_sum(coulomb_partial(rounded, left, right, masks))


def solution(mesh):
    in_specs = (
        P("aux", "pair"),
        P(None, "pair"),
        P("aux", "pair"),
        P("aux", "pair"),
        P("aux", None),
    )
    out_specs = P(None, ("pair", "aux"))
    return jax.shard_map(shards, mesh=mesh, in_specs=in_specs, out_specs=out_specs, check_vma=False)
```
